32 devices in a mesh: col: 8 (over z, y), row: 4 (over x, core).
Axes of the slice: x: 2, y: 2, z: 4, core: 2. Of those that a mesh axis runs over, the one named last changes fastest.
Arguments:
- vel_x: float32 [36, 2, 96, 2048], P(None, None, 'row', 'col')
- vel_y: float32 [36, 2, 96, 2048], P(None, None, 'row', 'col')
- pot_temp: float32 [36, 2, 96, 2048], P(None, None, 'row', 'col')
- salinity: float32 [36, 2, 96, 2048], P(None, None, 'row', 'col')
- surf_eta: float32 [2, 96, 2048], P(None, 'row', 'col')
- trans_x: float32 [2, 96, 2048], P(None, 'row', 'col')
- trans_y: float32 [2, 96, 2048], P(None, 'row', 'col')
- col_depth: float32 [96, 2048], P('row', 'col')
- wet_levels: int32 [96, 2048], P('row', 'col')
- avg_weights: float32 [30], replicated
Outputs:
- output 1: float32 [2, 96, 2048], P(None, 'row', 'col')
- output 2: float32 [2, 96, 2048], P(None, 'row', 'col')
- output 3: float32 [2, 96, 2048], P(None, 'row', 'col')
- output 4: float32 [36, 2, 96, 2048], P(None, None, 'row', 'col')
- output 5: float32 [36, 2, 96, 2048], P(None, None, 'row', 'col')
- output 6: float32 [36, 2, 96, 2048], P(None, None, 'row', 'col')
- output 7: float32 [36, 2, 96, 2048], P(None, None, 'row', 'col')
All inputs are finite; a program needn't handle non-finite values.
Results may differ from the reference program's by a relative error of at most 0.001.
Values sent between devices are 32-bit elements.
A program may use at most 1 GiB of HBM per device.

```python
import jax
import jax.numpy as jnp
from jax import lax

MEMBERS = 2
LEVELS = 36
SUBCYCLES = 30
GRID_Y = 96
GRID_X = 2048

WAVE_COURANT = 0.4
THERM_EXP = 0.2
HALINE_CON = 0.15
PRESS_SCALE = 0.5
VISC_NUMBER = 1.0
DIFF_NUMBER = 0.5


def east_of(field_in):
    return jnp.roll(field_in, -1, axis=-1)


def west_of(field_in):
    return jnp.roll(field_in, 1, axis=-1)


def north_of(field_in):
    return jnp.concatenate([field_in[..., 1:, :], jnp.zeros_like(field_in[..., :1, :])], axis=-2)


def south_of(field_in):
    return jnp.concatenate([jnp.zeros_like(field_in[..., :1, :]), field_in[..., :-1, :]], axis=-2)


def wet_masks(wet_levels, level_total):
    levels = jnp.arange(level_total).reshape(level_total, 1, 1, 1)
    cell_mask = (levels < wet_levels).astype(jnp.float32)
    xface_mask = cell_mask * (levels < east_of(wet_levels)).astype(jnp.float32)
    yface_mask = cell_mask * (levels < north_of(wet_levels)).astype(jnp.float32)
    return cell_mask, xface_mask, yface_mask


def setup_inputs(seed: int = 0) -> dict:
    key_list = jax.random.split(jax.random.key(seed), 12)
    shape_3d = (LEVELS, MEMBERS, GRID_Y, GRID_X)
    shape_2d = (MEMBERS, GRID_Y, GRID_X)
    land_draw = jax.random.randint(key_list[0], (GRID_Y, GRID_X), 0, 10)
    depth_draw = jax.random.randint(key_list[1], (GRID_Y, GRID_X), 1, LEVELS + 1)
    wet_levels = jnp.where(land_draw == 0, 0, jnp.where(land_draw < 5, LEVELS, depth_draw)).astype(jnp.int32)
    cell_mask, xface_mask, yface_mask = wet_masks(wet_levels, LEVELS)
    profile = jnp.cos(jnp.pi * (jnp.arange(LEVELS) + 0.5) / LEVELS).reshape(LEVELS, 1, 1, 1)

    def tracer_field(key_pair):
        key_a, key_b, key_c = jax.random.split(key_pair, 3)
        base_field = jax.random.normal(key_a, shape_2d, jnp.float32)
        mode_field = jax.random.normal(key_b, shape_2d, jnp.float32)
        noise_3d = jax.random.normal(key_c, shape_3d, jnp.float32)
        return cell_mask * (base_field + mode_field * profile + 0.3 * noise_3d)

    vel_x = xface_mask * 0.3 * jax.random.normal(key_list[2], shape_3d, jnp.float32)
    vel_y = yface_mask * 0.3 * jax.random.normal(key_list[3], shape_3d, jnp.float32)
    pot_temp = tracer_field(key_list[4])
    salinity = tracer_field(key_list[5])
    surf_eta = cell_mask[0] * 0.3 * jax.random.normal(key_list[6], shape_2d, jnp.float32)
    trans_x = xface_mask[0] * 0.3 * jax.random.normal(key_list[7], shape_2d, jnp.float32)
    trans_y = yface_mask[0] * 0.3 * jax.random.normal(key_list[8], shape_2d, jnp.float32)
    col_depth = 0.5 + 1.5 * jax.random.uniform(key_list[9], (GRID_Y, GRID_X), jnp.float32)
    step_frac = (jnp.arange(SUBCYCLES) + 1.0) / SUBCYCLES
    raw_weights = step_frac * step_frac * (2.0 - step_frac * step_frac) * (0.3 + 1.4 * jax.random.uniform(key_list[10], (SUBCYCLES,), jnp.float32))
    avg_weights = raw_weights / jnp.sum(raw_weights)
    return {"vel_x": vel_x, "vel_y": vel_y, "pot_temp": pot_temp, "salinity": salinity, "surf_eta": surf_eta, "trans_x": trans_x, "trans_y": trans_y, "col_depth": col_depth, "wet_levels": wet_levels, "avg_weights": avg_weights}


def vertical_solve(right_side, face_mask, strength):
    mask_below = jnp.concatenate([face_mask[1:], jnp.zeros_like(face_mask[:1])], axis=0)
    face_up = face_mask * mask_below
    face_down = jnp.concatenate([jnp.zeros_like(face_up[:1]), face_up[:-1]], axis=0)
    lower_diag = -strength * face_down
    upper_diag = -strength * face_up
    main_diag = 1.0 + strength * (face_down + face_up)

    def forward(state_prev, level_row):
        upper_prev, side_prev = state_prev
        low_k, diag_k, up_k, side_k = level_row
        divisor = diag_k - low_k * upper_prev
        upper_new = up_k / divisor
        side_new = (side_k - low_k * side_prev) / divisor
        return (upper_new, side_new), (upper_new, side_new)

    zero_level = jnp.zeros_like(right_side[0])
    upper_all, side_all = lax.scan(forward, (zero_level, zero_level), (lower_diag, main_diag, upper_diag, right_side))[1]

    def backward(sol_next, level_row):
        up_k, side_k = level_row
        sol_k = side_k - up_k * sol_next
        return sol_k, sol_k

    return lax.scan(backward, zero_level, (upper_all, side_all), reverse=True)[1]


def tracer_step(tracer, vel_x, vel_y, cell_mask):
    flux_x = vel_x * 0.5 * (tracer + east_of(tracer))
    flux_y = vel_y * 0.5 * (tracer + north_of(tracer))
    advected = cell_mask * (tracer - (flux_x - west_of(flux_x) + flux_y - south_of(flux_y)))
    return vertical_solve(advected, cell_mask, DIFF_NUMBER)


def barotropic(surf_eta, trans_x, trans_y, force_x, force_y, depth_x, depth_y, wet_top, xface_top, yface_top, avg_weights):
    sub_count = avg_weights.shape[0]
    step_x = force_x / sub_count
    step_y = force_y / sub_count

    def subcycle(sub_state, weight):
        eta_now, tx_now, ty_now, eta_avg, tx_avg, ty_avg = sub_state
        eta_now = wet_top * (eta_now - WAVE_COURANT * (tx_now - west_of(tx_now) + ty_now - south_of(ty_now)))
        tx_now = xface_top * (tx_now + step_x - WAVE_COURANT * depth_x * (east_of(eta_now) - eta_now))
        ty_now = yface_top * (ty_now + step_y - WAVE_COURANT * depth_y * (north_of(eta_now) - eta_now))
        return (eta_now, tx_now, ty_now, eta_avg + weight * eta_now, tx_avg + weight * tx_now, ty_avg + weight * ty_now), None

    zero_field = jnp.zeros_like(surf_eta)
    end_state = lax.scan(subcycle, (surf_eta, trans_x, trans_y, zero_field, zero_field, zero_field), avg_weights)[0]
    return end_state[3], end_state[4], end_state[5]


def reference(vel_x, vel_y, pot_temp, salinity, surf_eta, trans_x, trans_y, col_depth, wet_levels, avg_weights):
    level_count = vel_x.shape[0]
    cell_mask, xface_mask, yface_mask = wet_masks(wet_levels, level_count)
    density = HALINE_CON * salinity - THERM_EXP * pot_temp
    pressure = (PRESS_SCALE / level_count) * (jnp.cumsum(density, axis=0) - 0.5 * density)
    vy_south = south_of(vel_y)
    vx_north = north_of(vel_x)
    vy_at_x = 0.25 * (vel_y + vy_south + east_of(vel_y) + east_of(vy_south))
    vx_at_y = 0.25 * (vel_x + west_of(vel_x) + vx_north + west_of(vx_north))
    tend_x = xface_mask * (pressure - east_of(pressure) - 0.5 * vel_x * (east_of(vel_x) - west_of(vel_x)) - 0.5 * vy_at_x * (vx_north - south_of(vel_x)))
    tend_y = yface_mask * (pressure - north_of(pressure) - 0.5 * vx_at_y * (east_of(vel_y) - west_of(vel_y)) - 0.5 * vel_y * (north_of(vel_y) - vy_south))
    count_x = jnp.maximum(jnp.sum(xface_mask, axis=0), 1.0)
    count_y = jnp.maximum(jnp.sum(yface_mask, axis=0), 1.0)
    depth_x = 0.5 * (col_depth + east_of(col_depth)) * xface_mask[0]
    depth_y = 0.5 * (col_depth + north_of(col_depth)) * yface_mask[0]
    force_x = depth_x * jnp.sum(tend_x, axis=0) / count_x
    force_y = depth_y * jnp.sum(tend_y, axis=0) / count_y
    pred_x = vertical_solve(vel_x + tend_x, xface_mask, VISC_NUMBER)
    pred_y = vertical_solve(vel_y + tend_y, yface_mask, VISC_NUMBER)
    temp_new = tracer_step(pot_temp, vel_x, vel_y, cell_mask)
    salt_new = tracer_step(salinity, vel_x, vel_y, cell_mask)
    eta_new, trans_x_new, trans_y_new = barotropic(surf_eta, trans_x, trans_y, force_x, force_y, depth_x, depth_y, cell_mask[0], xface_mask[0], yface_mask[0], avg_weights)
    vel_x_new = xface_mask * (pred_x - jnp.sum(pred_x, axis=0) / count_x + trans_x_new / (depth_x + 1.0 - xface_mask[0]))
    vel_y_new = yface_mask * (pred_y - jnp.sum(pred_y, axis=0) / count_y + trans_y_new / (depth_y + 1.0 - yface_mask[0]))
    return eta_new, trans_x_new, trans_y_new, vel_x_new, vel_y_new, temp_new, salt_new
```

```python
import functools

import jax
import jax.numpy as jnp
from jax import lax
from jax.experimental import pallas as pl
from jax.experimental.pallas import tpu as pltpu
from jax.sharding import PartitionSpec as P

WAVE_COURANT = 0.4
THERM_EXP = 0.2
HALINE_CON = 0.15
PRESS_SCALE = 0.5
VISC_NUMBER = 1.0
DIFF_NUMBER = 0.5

MESH = pl.DeviceIdType.MESH
F32 = jnp.float32
ROWS = 24
PAD = 8
XR = ROWS + 2 * PAD
LEVEL_BLOCK = 4
LANES = 128
TILE = (8, LANES)
RING = 3
M = 2
FRAME = 4 * ROWS + 2 * PAD
HALO = 32


def sweep_constants(level_count, strength):
    inverse, ratio = [], []
    for k in range(level_count):
        pivot = 1.0 + strength if k == 0 else 1.0 + 2.0 * strength - strength * ratio[-1]
        inverse.append(1.0 / pivot)
        ratio.append(strength / pivot)
    return inverse, ratio


def iota(shape, axis):
    return lax.broadcasted_iota(jnp.int32, shape, axis)


def lanes(*lead):
    return iota((*lead, 8, 128), len(lead) + 1)


def turn(x, shift):
    return pltpu.roll(x, shift, x.ndim - 1)


def east(x, keep=3):
    rolled = turn(x, 127)
    following = rolled[1:] if keep == 2 else jnp.concatenate([rolled[1:], rolled[:1]], axis=0)
    return jnp.where(lanes(keep) == 127, following, rolled[:keep])


def west(x, keep=3):
    rolled = turn(x, 1)
    return jnp.where(lanes(keep) == 0, jnp.concatenate([rolled[2:], rolled[:keep - 1]], axis=0), rolled[:keep])


def step_kernel(
    col_count, level_count, sub_count,
    u_hbm, v_hbm, t_hbm, s_hbm, eta_in, tx_in, ty_in, depth_in, wet_in, weights, table,
    xu_hbm, xv_hbm, ct_hbm, cs_hbm, qu_out, qv_out, nuv_out, eta_out, tx_out, ty_out,
    cube, sol,
    col_w, col_e, rcv_e, rcv_w, row_s, row_n, rcv_n, rcv_s, rcv_se, rcv_nw,
    kmt, nuv, sums, stage, stage_w, stage_e, pk_e, pk_w, fstage, fstage_w, fstage_e, fpk_e, fpk_w,
    frame, coef, acc, result, result_in,
    load_sem, store_sem, send_sem, edge_sem, row_sem, e_sem, w_sem, frow_sem, fe_sem, fw_sem, swap_sem,
):
    L = level_count
    U, V, T, S = range(4)
    ETA, TX, TY, DEPTH, FX, FY = range(6)
    OWN = slice(0, 2)
    col = lax.axis_index("col")
    row = lax.axis_index("row")
    chip = row // 2
    core = row % 2
    east_col = lax.rem(col + 1, col_count)
    west_col = lax.rem(col + col_count - 1, col_count)
    peers = [lax.rem(row + d, 4) for d in (1, 2, 3)]
    lane = lanes()
    zero = jnp.zeros(TILE, F32)

    def aligned(start, size=8):
        return pl.ds(pl.multiple_of(start, 8), size)

    barrier = pltpu.get_barrier_semaphore()
    for r in peers:
        pl.semaphore_signal(barrier, inc=1, device_id={"row": r, "col": col}, device_id_type=MESH)
    for other in (east_col, west_col):
        for r in range(4):
            pl.semaphore_signal(barrier, inc=1, device_id={"row": r, "col": other}, device_id_type=MESH)

    loads = []
    for f, src in enumerate((u_hbm, v_hbm, t_hbm, s_hbm)):
        for lt in range(2):
            loads.append(pltpu.make_async_copy(
                src.at[:, :, :, pl.ds(LANES * lt, LANES)], cube.at[f, :, :, lt, pl.ds(PAD, ROWS), :], load_sem.at[2 * f + lt]))
            loads[-1].start()

    def pack_2d(get, count, out_w, out_e):
        for i in range(3):
            rs = pl.ds(8 * i, 8)
            for m in range(2):
                pack_w = pack_e = zero
                for j in range(count):
                    here = lane // HALO == j
                    pack_w = jnp.where(here, turn(get[m, j, 0, rs, :], HALO * j), pack_w)
                    pack_e = jnp.where(here, turn(get[m, j, 1, rs, :], (HALO * j + HALO) % 128), pack_e)
                out_w[m, rs, :] = pack_w
                out_e[m, rs, :] = pack_e

    for lt in range(2):
        ls = pl.ds(LANES * lt, LANES)
        wet = wet_in[:, ls].astype(F32)
        kmt[lt, pl.ds(0, ROWS), :] = wet
        masked = jnp.where(wet > 0.0, depth_in[:, ls], 0.0)
        for m in range(2):
            stage[m, ETA, lt] = eta_in[m, :, ls]
            stage[m, TX, lt] = tx_in[m, :, ls]
            stage[m, TY, lt] = ty_in[m, :, ls]
            stage[m, DEPTH, lt] = masked
    pack_2d(stage, 4, stage_w, stage_e)

    has_s, has_n = row > 0, row < 3

    @pl.when(row == 0)
    def _():
        rcv_s[...] = jnp.zeros(rcv_s.shape, F32)
        rcv_se[...] = jnp.zeros(rcv_se.shape, F32)

    @pl.when(row == 3)
    def _():
        rcv_n[...] = jnp.zeros(rcv_n.shape, F32)
        rcv_nw[...] = jnp.zeros(rcv_nw.shape, F32)

    frame[:, :, pl.ds(0, PAD), :] = jnp.zeros((6, 3, PAD, 128), F32)
    frame[:, :, pl.ds(PAD + 4 * ROWS, PAD), :] = jnp.zeros((6, 3, PAD, 128), F32)

    for copy in loads:
        copy.wait()

    lane42 = lanes(4, 2)

    def pack(k, carry):
        west_pack, east_pack = carry
        for i in range(3):
            slot = L * i + k
            rs = pl.ds(PAD + 8 * i, 8)
            west_pack = jnp.where(lane42 == slot, turn(cube[:, k, :, 0, rs, :], slot), west_pack)
            east_pack = jnp.where(lane42 == slot, turn(cube[:, k, :, 1, rs, :], slot + 1), east_pack)
        return west_pack, east_pack

    empty = jnp.zeros((4, 2, 8, 128), F32)
    west_pack, east_pack = lax.fori_loop(0, L, pack, (empty, empty))
    col_w[...] = west_pack
    col_e[...] = east_pack
    for i in range(3):
        slot = 3 * L + i
        col_w[0, 0] = jnp.where(lane == slot, turn(kmt[0, pl.ds(8 * i, 8), :], slot), col_w[0, 0])

    sub42 = iota((4, 2, 8, 128), 2)

    def pack_rows(g, carry):
        low = high = empty
        for j in range(8):
            k, m = 4 * g + j // 2, j % 2
            low = jnp.where(sub42 == j, cube[:, k, m, OWN, pl.ds(PAD - j, 8), :], low)
            high = jnp.where(sub42 == j, cube[:, k, m, OWN, pl.ds(PAD + ROWS - 1 - j, 8), :], high)
        row_s[:, :, aligned(8 * g), :] = low
        row_n[:, :, aligned(8 * g), :] = high
        return carry

    lax.fori_loop(0, L // 4, pack_rows, 0)
    for f in range(4):
        row_s[f, :, pl.ds(2 * L, 8), :] = kmt[:, pl.ds(0, 8), :]
        row_n[f, :, pl.ds(2 * L, 8), :] = kmt[:, pl.ds(0, 8), :]

    pl.semaphore_wait(barrier, 11)

    def send(src, dst, ssem, rsem, r, c):
        return pltpu.make_async_remote_copy(
            src_ref=src, dst_ref=dst, send_sem=send_sem.at[ssem], recv_sem=rsem, device_id={"row": r, "col": c}, device_id_type=MESH)

    own_rows = aligned(PAD + ROWS * row, ROWS)
    south, north = jnp.maximum(row - 1, 0), jnp.minimum(row + 1, 3)
    to_w = send(col_w, rcv_e, 0, edge_sem.at[0], row, west_col)
    to_e = send(col_e, rcv_w, 1, edge_sem.at[1], row, east_col)
    to_s = send(row_s, rcv_n, 2, edge_sem.at[2], south, col)
    to_n = send(row_n, rcv_s, 3, edge_sem.at[3], north, col)
    to_nw = send(col_w.at[V], rcv_se, 4, edge_sem.at[4], north, west_col)
    to_se = send(col_e.at[U], rcv_nw, 5, edge_sem.at[5], south, east_col)
    to_w.start()
    to_e.start()

    @pl.when(has_s)
    def _():
        to_s.start()
        to_se.start()

    @pl.when(has_n)
    def _():
        to_n.start()
        to_nw.start()

    def exchange(stg, stg_w, stg_e, first, count, base, rsem, esem, wsem, pe, pw):
        out = []
        for d, r in enumerate(peers):
            out.append(send(stg.at[r % 2], frame.at[pl.ds(first, count), OWN, own_rows, :], base + d, rsem.at[row], r, col))
        for r in range(4):
            out.append(send(stg_w.at[r % 2], pe.at[row], base + 3 + 2 * r, esem.at[row], r, west_col))
            out.append(send(stg_e.at[r % 2], pw.at[row], base + 4 + 2 * r, wsem.at[row], r, east_col))
        for copy in out:
            copy.start()
        frame[pl.ds(first, count), OWN, own_rows, :] = stg[core]
        return out

    def collect(stg, stg_w, first, count, rsem, esem, wsem, pe, pw):
        for r in peers:
            rows = aligned(PAD + ROWS * r, ROWS)
            send(stg.at[0], frame.at[pl.ds(first, count), OWN, rows, :], 0, rsem.at[r], r, col).wait_recv()
        for r in range(4):
            send(stg_w.at[0], pe.at[r], 0, esem.at[r], r, east_col).wait_recv()
            send(stg_w.at[0], pw.at[r], 0, wsem.at[r], r, west_col).wait_recv()
        side = lax.broadcasted_iota(jnp.int32, (ROWS, 128), 1) // HALO
        for r in range(4):
            for j in range(count):
                frame[first + j, 2, pl.ds(PAD + ROWS * r, ROWS), :] = jnp.where(
                    side == 0, turn(pe[r], (128 - HALO * j) % 128), jnp.where(side == 3, turn(pw[r], (128 - HALO * j - HALO) % 128), 0.0))

    sent = exchange(stage, stage_w, stage_e, ETA, 4, 6, row_sem, e_sem, w_sem, pk_e, pk_w)

    to_w.wait_recv()
    to_e.wait_recv()

    @pl.when(has_n)
    def _():
        to_s.wait_recv()
        to_se.wait_recv()

    @pl.when(has_s)
    def _():
        to_n.wait_recv()
        to_nw.wait_recv()

    def unpack_rows(g, carry):
        below, above = rcv_s[:, :, aligned(8 * g), :], rcv_n[:, :, aligned(8 * g), :]
        for j in range(8):
            k, m = 4 * g + j // 2, j % 2
            cube[:, k, m, OWN, pl.ds(PAD - 1, 1), :] = below[:, :, j:j + 1, :]
            cube[:, k, m, OWN, pl.ds(PAD + ROWS, 1), :] = above[:, :, j:j + 1, :]
        return carry

    lax.fori_loop(0, L // 4, unpack_rows, 0)
    kmt[:, pl.ds(ROWS, 8), :] = rcv_n[0, :, pl.ds(2 * L, 8), :]
    for i in range(3):
        rs = pl.ds(8 * i, 8)
        wet = kmt[:, rs, :]
        halo = turn(rcv_e[0, 0], 128 - (3 * L + i))
        nuv[0, :, rs, :] = jnp.minimum(wet, east(jnp.concatenate([wet, halo[None]], axis=0), 2))
        nuv[1, :, rs, :] = jnp.minimum(wet, kmt[:, pl.ds(8 * i + 1, 8), :])

    def unpack(k, carry):
        for i in range(3):
            slot = L * i + k
            cube[:, k, :, 2, pl.ds(PAD + 8 * i, 8), :] = jnp.where(
                lane42 < 64, turn(rcv_e[...], lax.rem(128 - slot, 128)), turn(rcv_w[...], 127 - slot))
        cube[V, k, :, 2, pl.ds(0, PAD), :] = turn(rcv_se[...], 128 - 2 * L - k)
        cube[U, k, :, 2, pl.ds(PAD + ROWS, PAD), :] = turn(rcv_nw[...], 127 - k)
        return carry

    lax.fori_loop(0, L, unpack, 0)

    press = PRESS_SCALE / L
    pair = jnp.zeros((2, 8, 128), F32)

    def for_strips(body, init, reverse=False):
        def strip(s, carry):
            m = s // 3
            i = s - 3 * m
            rs = aligned(8 * i)

            def get(f, k, part, d=0):
                start = PAD + 8 * i + d
                return cube[f, k, m, part, pl.ds(start if d else pl.multiple_of(start, 8), 8), :]

            state, finish = init(m, rs)

            def block(b, state):
                for j in range(LEVEL_BLOCK):
                    k = b * LEVEL_BLOCK + j
                    state = body(L - 1 - k if reverse else k, m, rs, get, state)
                return state

            finish(m, rs, lax.fori_loop(0, L // LEVEL_BLOCK, block, state))
            return carry

        lax.fori_loop(0, 6, strip, 0)

    def momentum_init(m, rs):
        return (pair,) * 6, momentum_finish

    def momentum_finish(m, rs, state):
        sums[0, m, :, rs, :] = state[4]
        sums[1, m, :, rs, :] = state[5]

    def momentum(k, m, rs, get, state):
        cx, cy, eu, ev, gu_sum, gv_sum = state
        level = k.astype(F32)
        both = slice(0, 3)
        u, v, un, vs = get(U, k, both), get(V, k, both), get(U, k, both, 1), get(V, k, both, -1)
        rho = HALINE_CON * get(S, k, both) - THERM_EXP * get(T, k, both)
        dx = rho[OWN] - east(rho, 2)
        dy = rho[OWN] - (HALINE_CON * get(S, k, OWN, 1) - THERM_EXP * get(T, k, OWN, 1))
        vsum, usum = v + vs, u + un
        cx, cy = cx + dx, cy + dy
        gu = press * (cx - 0.5 * dx) - 0.5 * (u[OWN] * (east(u, 2) - west(u, 2))) - 0.125 * (
            (vsum[OWN] + east(vsum, 2)) * (un[OWN] - get(U, k, OWN, -1)))
        gv = press * (cy - 0.5 * dy) - 0.125 * ((usum[OWN] + west(usum, 2)) * (east(v, 2) - west(v, 2))) - 0.5 * (
            v[OWN] * (get(V, k, OWN, 1) - vs[OWN]))
        gu = jnp.where(nuv[0, :, rs, :] > level, gu, 0.0)
        gv = jnp.where(nuv[1, :, rs, :] > level, gv, 0.0)
        inverse = table[0, k]
        eu = (u[OWN] + gu + VISC_NUMBER * eu) * inverse
        ev = (v[OWN] + gv + VISC_NUMBER * ev) * inverse
        sol[U, k, m, :, rs, :] = eu
        sol[V, k, m, :, rs, :] = ev
        return cx, cy, eu, ev, gu_sum + gu, gv_sum + gv

    for_strips(momentum, momentum_init)

    collect(stage, stage_w, ETA, 4, row_sem, e_sem, w_sem, pk_e, pk_w)

    def coefficients(i, carry):
        rs = aligned(PAD + 8 * i)
        depth = frame[DEPTH, :, rs, :]
        depth_e = east(depth)
        depth_n = frame[DEPTH, :, pl.ds(PAD + 8 * i + 1, 8), :]
        wet = depth > 0.0
        coef[0, :, rs, :] = jnp.where(wet, WAVE_COURANT, 0.0)
        coef[1, :, rs, :] = jnp.where(wet & (depth_e > 0.0), 0.5 * (depth + depth_e), 0.0)
        coef[2, :, rs, :] = jnp.where(wet & (depth_n > 0.0), 0.5 * (depth + depth_n), 0.0)
        return carry

    lax.fori_loop(0, 12, coefficients, 0)

    for d in range(2):
        scale = coef[1 + d, OWN, own_rows, :] / (jnp.maximum(nuv[d], 1.0) * float(sub_count))
        for m in range(2):
            fstage[m, d] = scale * sums[d, m]
    pack_2d(fstage, 2, fstage_w, fstage_e)
    sent += exchange(fstage, fstage_w, fstage_e, FX, 2, 17, frow_sem, fe_sem, fw_sem, fpk_e, fpk_w)

    def back_init(m, rs):
        return (pair,) * 4, back_finish

    def back_finish(m, rs, state):
        for d in range(2):
            sums[d, m, :, rs, :] = state[2 + d] / jnp.maximum(nuv[d, :, rs, :], 1.0)

    def back(k, m, rs, get, state):
        x, total = list(state[:2]), list(state[2:])
        level = k.astype(F32)
        for d in range(2):
            e, n = sol[d, k, m, :, rs, :], nuv[d, :, rs, :]
            x[d] = e + table[1, k] * jnp.where(n > level + 1.0, x[d], e * table[2, k])
            sol[d, k, m, :, rs, :] = x[d]
            total[d] = total[d] + jnp.where(n > level, x[d], 0.0)
        return (*x, *total)

    for_strips(back, back_init, reverse=True)

    stores = []

    def store(f, dst):
        for lt in range(2):
            stores.append(pltpu.make_async_copy(sol.at[f, :, :, lt], dst.at[:, :, :, pl.ds(LANES * lt, LANES)], store_sem.at[2 * f + lt]))
            stores[-1].start()

    store(U, xu_hbm)
    store(V, xv_hbm)

    def tracer_init(m, rs):
        return (pair,) * 2, lambda *a: None

    def tracers(k, m, rs, get, state):
        level = k.astype(F32)
        u, v, vs = 0.5 * get(U, k, slice(0, 3)), 0.5 * get(V, k, OWN), 0.5 * get(V, k, OWN, -1)
        out = []
        for f, e in zip((T, S), state):
            t = get(f, k, slice(0, 3))
            fx = u * (t + east(t))
            t = t[OWN]
            b = t - fx[OWN] + west(fx, 2) - v * (t + get(f, k, OWN, 1)) + vs * (t + get(f, k, OWN, -1))
            b = jnp.where(kmt[:, rs, :] > level, b, 0.0)
            out.append((b + DIFF_NUMBER * e) * table[3, k])
            sol[f, k, m, :, rs, :] = out[-1]
        return tuple(out)

    for_strips(tracers, tracer_init)
    store(T, ct_hbm)
    store(S, cs_hbm)
    acc[...] = jnp.zeros(acc.shape, F32)

    collect(fstage, fstage_w, FX, 2, frow_sem, fe_sem, fw_sem, fpk_e, fpk_w)

    def subcycles(first, last, tiles):
        base = PAD + chip * (8 * (12 - tiles))

        def body(n, carry):
            def rows_of(t):
                return aligned(base + 8 * t)

            def eta_tile(t):
                rs = rows_of(t)
                u, v = frame[TX, :, rs, :], frame[TY, :, rs, :]
                div = (u - west(u)) + (v - frame[TY, :, pl.ds(base + 8 * t - 1, 8), :])
                eta = frame[ETA, :, rs, :] - coef[0, :, rs, :] * div
                frame[ETA, :, rs, :] = eta
                return u, v, WAVE_COURANT * eta

            last_row = iota((3, 8, 128), 1) == 7
            following = eta_tile(0)
            for t in range(tiles):
                u, v, e = following
                if t + 1 < tiles:
                    following = eta_tile(t + 1)
                else:
                    following = (None, None, WAVE_COURANT * frame[ETA, :, rows_of(tiles), :])
                e_n = jnp.where(last_row, pltpu.roll(following[2], 7, 1), pltpu.roll(e, 7, 1))
                rs = rows_of(t)
                frame[TX, :, rs, :] = u + frame[FX, :, rs, :] - coef[1, :, rs, :] * (east(e) - e)
                frame[TY, :, rs, :] = v + frame[FY, :, rs, :] - coef[2, :, rs, :] * (e_n - e)
            chip_rows = aligned(PAD + 2 * ROWS * chip, 2 * ROWS)
            acc[...] += weights[n] * frame[pl.ds(0, 3), OWN, chip_rows, :]
            return carry

        lax.fori_loop(first, last, body, 0)

    def tiles_at(n):
        return min(-(-(2 * ROWS + sub_count - n) // 16) * 2, 12)

    n = 0
    while n < sub_count:
        last = n
        while last < sub_count and tiles_at(last) == tiles_at(n):
            last += 1
        subcycles(n, last, tiles_at(n))
        n = last

    mine = aligned(ROWS * core, ROWS)
    theirs = aligned(ROWS * (1 - core), ROWS)
    result[...] = acc[:, :, theirs, :]
    swap = send(result, result_in, 28, swap_sem, row + 1 - 2 * core, col)
    swap.start()
    swap.wait_recv()
    for m in range(2):
        whole = jnp.where(core == m, acc[:, :, mine, :], result_in[...])
        for lt in range(2):
            ls = pl.ds(LANES * lt, LANES)
            eta_out[m, :, ls] = whole[ETA, lt]
            tx_out[m, :, ls] = whole[TX, lt]
            ty_out[m, :, ls] = whole[TY, lt]
            for d, out in enumerate((qu_out, qv_out)):
                depth = coef[1 + d, lt, own_rows, :]
                out[m, :, ls] = whole[TX + d, lt] / jnp.where(depth > 0.0, depth, 1.0) - sums[d, m, lt]
                nuv_out[d, :, ls] = nuv[d, lt]

    for copy in stores:
        copy.wait()
    to_w.wait_send()
    to_e.wait_send()

    @pl.when(has_s)
    def _():
        to_s.wait_send()
        to_se.wait_send()

    @pl.when(has_n)
    def _():
        to_n.wait_send()
        to_nw.wait_send()

    for copy in sent:
        copy.wait_send()
    swap.wait_send()


def final_kernel(level_count, xu, xv, ct, cs, qu, qv, nuv, wet, eta_in, tx_in, ty_in,
                 eta_out, tx_out, ty_out, u_out, v_out, t_out, s_out):
    ratio = sweep_constants(level_count, DIFF_NUMBER)[1]
    eta_out[...] = eta_in[...]
    tx_out[...] = tx_in[...]
    ty_out[...] = ty_in[...]
    for lt in range(2):
        ls = pl.ds(LANES * lt, LANES)
        n_wet = wet[:, ls]
        for src, out in ((ct, t_out), (cs, s_out)):
            x = jnp.zeros(TILE, F32)
            for k in reversed(range(level_count)):
                e = src[k, 0, :, ls]
                x = e + ratio[k] * jnp.where(n_wet > k + 1, x, e * (1.0 / (1.0 - ratio[k])))
                out[k, 0, :, ls] = jnp.where(n_wet > k, x, 0.0)
        for d, (src, q, out) in enumerate(((xu, qu, u_out), (xv, qv, v_out))):
            n, mean = nuv[d, :, ls], q[0, :, ls]
            for k in range(level_count):
                out[k, 0, :, ls] = jnp.where(n > float(k), src[k, 0, :, ls] + mean, 0.0)


def solution(mesh):
    col_count = mesh.shape["col"]

    def local_step(vel_x, vel_y, pot_temp, salinity, surf_eta, trans_x, trans_y, col_depth, wet_levels, avg_weights):
        L = vel_x.shape[0]
        N = avg_weights.shape[0]
        any_spec = pl.BlockSpec(memory_space=pl.ANY)
        vmem_spec = pl.BlockSpec(memory_space=pltpu.VMEM)
        cube = jax.ShapeDtypeStruct(vel_x.shape, F32)
        flat = jax.ShapeDtypeStruct(surf_eta.shape, F32)
        vm = lambda *shape: pltpu.VMEM(shape, F32)
        dma = lambda n: pltpu.SemaphoreType.DMA((n,))
        inverse, ratio = sweep_constants(L, VISC_NUMBER)
        table = jnp.array([inverse, ratio, [1.0 / (1.0 - r) for r in ratio], sweep_constants(L, DIFF_NUMBER)[0]], F32)
        xu, xv, ct, cs, qu, qv, nuv, eta_o, tx_o, ty_o = pl.pallas_call(
            functools.partial(step_kernel, col_count, L, N),
            out_shape=[cube] * 4 + [flat] * 3 + [flat] * 3,
            in_specs=[any_spec] * 4 + [vmem_spec] * 5 + [pl.BlockSpec(memory_space=pltpu.SMEM)] * 2,
            out_specs=[any_spec] * 4 + [vmem_spec] * 6,
            scratch_shapes=[
                vm(4, L, M, RING, XR, LANES), vm(4, L, M, M, ROWS, LANES), *[vm(4, M, 8, LANES)] * 4, *[vm(4, M, M * L + 8, LANES)] * 4,
                *[vm(M, 8, LANES)] * 2, vm(M, ROWS + 8, LANES), vm(M, M, ROWS, LANES), vm(M, M, M, ROWS, LANES),
                vm(M, 4, M, ROWS, LANES), *[vm(M, ROWS, LANES)] * M, *[vm(4, ROWS, LANES)] * M,
                vm(M, M, M, ROWS, LANES), *[vm(M, ROWS, LANES)] * M, *[vm(4, ROWS, LANES)] * M,
                vm(6, RING, FRAME, LANES), vm(RING, RING, FRAME, LANES), vm(RING, M, M * ROWS, LANES), *[vm(RING, M, ROWS, LANES)] * M,
                dma(8), dma(8), dma(29), dma(6), *[dma(4)] * 6, pltpu.SemaphoreType.DMA],
            compiler_params=pltpu.CompilerParams(collective_id=0, has_side_effects=True),
            name="ocean_step",
        )(vel_x, vel_y, pot_temp, salinity, surf_eta, trans_x, trans_y, col_depth, wet_levels, avg_weights, table)
        cube_spec = pl.BlockSpec((L, 1, 8, 256), lambda m, i: (0, m, i, 0))
        flat_spec = pl.BlockSpec((1, 8, 256), lambda m, i: (m, i, 0))
        outs = pl.pallas_call(
            functools.partial(final_kernel, L),
            grid=(2, 3),
            out_shape=[flat] * 3 + [cube] * 4,
            in_specs=[cube_spec] * 4 + [flat_spec] * 2
            + [pl.BlockSpec((2, 8, 256), lambda m, i: (0, i, 0)), pl.BlockSpec((8, 256), lambda m, i: (i, 0))] + [flat_spec] * 3,
            out_specs=[flat_spec] * 3 + [cube_spec] * 4,
            name="ocean_final",
        )(xu, xv, ct, cs, qu, qv, nuv, wet_levels, eta_o, tx_o, ty_o)
        return tuple(outs)

    spec_3d = P(None, None, "row", "col")
    spec_2d = P(None, "row", "col")
    spec_map = P("row", "col")
    return jax.shard_map(local_step, mesh=mesh, in_specs=(spec_3d,) * 4 + (spec_2d,) * 3 + (spec_map,) * 2 + (P(),),
                         out_specs=(spec_2d,) * 3 + (spec_3d,) * 4, check_vma=False)
```

```python
import functools

import jax
import jax.numpy as jnp
from jax import lax
from jax.experimental import pallas as pl
from jax.experimental.pallas import tpu as pltpu
from jax.sharding import PartitionSpec as P

WAVE_COURANT = 0.4
THERM_EXP = 0.2
HALINE_CON = 0.15
PRESS_SCALE = 0.5
VISC_NUMBER = 1.0
DIFF_NUMBER = 0.5

MESH = pl.DeviceIdType.MESH
F32 = jnp.float32
ROWS = 24
PAD = 8
XR = ROWS + 2 * PAD
EDGE_BLOCK = 4
LEVEL_BLOCK = 12
LANES = 128
TILE = (8, LANES)
RING = 3
M = 2
FRAME = 4 * ROWS + 2 * PAD
HALO = 32


def sweep_constants(level_count, strength):
    inverse, ratio = [], []
    for k in range(level_count):
        pivot = 1.0 + strength if k == 0 else 1.0 + 2.0 * strength - strength * ratio[-1]
        inverse.append(1.0 / pivot)
        ratio.append(strength / pivot)
    return inverse, ratio


def iota(shape, axis):
    return lax.broadcasted_iota(jnp.int32, shape, axis)


def lanes(*lead):
    return iota((*lead, 8, 128), len(lead) + 1)


def turn(x, shift):
    return pltpu.roll(x, shift, x.ndim - 1)


def east(x, keep=3):
    rolled = turn(x, 127)
    following = rolled[1:] if keep == 2 else jnp.concatenate([rolled[1:], rolled[:1]], axis=0)
    return jnp.where(lanes(keep) == 127, following, rolled[:keep])


def west(x, keep=3):
    rolled = turn(x, 1)
    return jnp.where(lanes(keep) == 0, jnp.concatenate([rolled[2:], rolled[:keep - 1]], axis=0), rolled[:keep])


def step_kernel(
    col_count, level_count, sub_count,
    u_hbm, v_hbm, t_hbm, s_hbm, eta_in, tx_in, ty_in, depth_in, wet_in, weights, table,
    xu_hbm, xv_hbm, ct_hbm, cs_hbm, qu_out, qv_out, nuv_out, eta_out, tx_out, ty_out,
    cube, sol,
    col_w, col_e, rcv_e, rcv_w, row_s, row_n, rcv_n, rcv_s, rcv_se, rcv_nw,
    kmt, nuv, sums, stage, stage_w, stage_e, pk_e, pk_w, fstage, fstage_w, fstage_e, fpk_e, fpk_w,
    frame, coef, acc, result, result_in,
    load_sem, store_sem, send_sem, edge_sem, row_sem, e_sem, w_sem, frow_sem, fe_sem, fw_sem, swap_sem,
):
    L = level_count
    U, V, T, S = range(4)
    ETA, TX, TY, DEPTH, FX, FY = range(6)
    OWN = slice(0, 2)
    col = lax.axis_index("col")
    row = lax.axis_index("row")
    chip = row // 2
    core = row % 2
    east_col = lax.rem(col + 1, col_count)
    west_col = lax.rem(col + col_count - 1, col_count)
    peers = [lax.rem(row + d, 4) for d in (1, 2, 3)]
    lane = lanes()
    zero = jnp.zeros(TILE, F32)

    def aligned(start, size=8):
        return pl.ds(pl.multiple_of(start, 8), size)

    barrier = pltpu.get_barrier_semaphore()
    for r in peers:
        pl.semaphore_signal(barrier, inc=1, device_id={"row": r, "col": col}, device_id_type=MESH)
    for other in (east_col, west_col):
        for r in range(4):
            pl.semaphore_signal(barrier, inc=1, device_id={"row": r, "col": other}, device_id_type=MESH)

    loads = []
    for f, src in enumerate((u_hbm, v_hbm, t_hbm, s_hbm)):
        for lt in range(2):
            loads.append(pltpu.make_async_copy(
                src.at[:, :, :, pl.ds(LANES * lt, LANES)], cube.at[f, :, :, lt, pl.ds(PAD, ROWS), :], load_sem.at[2 * f + lt]))
            loads[-1].start()

    def pack_2d(get, count, out_w, out_e):
        for i in range(3):
            rs = pl.ds(8 * i, 8)
            for m in range(2):
                pack_w = pack_e = zero
                for j in range(count):
                    here = lane // HALO == j
                    pack_w = jnp.where(here, turn(get[m, j, 0, rs, :], HALO * j), pack_w)
                    pack_e = jnp.where(here, turn(get[m, j, 1, rs, :], (HALO * j + HALO) % 128), pack_e)
                out_w[m, rs, :] = pack_w
                out_e[m, rs, :] = pack_e

    for lt in range(2):
        ls = pl.ds(LANES * lt, LANES)
        wet = wet_in[:, ls].astype(F32)
        kmt[lt, pl.ds(0, ROWS), :] = wet
        masked = jnp.where(wet > 0.0, depth_in[:, ls], 0.0)
        for m in range(2):
            stage[m, ETA, lt] = eta_in[m, :, ls]
            stage[m, TX, lt] = tx_in[m, :, ls]
            stage[m, TY, lt] = ty_in[m, :, ls]
            stage[m, DEPTH, lt] = masked
    pack_2d(stage, 4, stage_w, stage_e)

    has_s, has_n = row > 0, row < 3

    @pl.when(row == 0)
    def _():
        rcv_s[...] = jnp.zeros(rcv_s.shape, F32)
        rcv_se[...] = jnp.zeros(rcv_se.shape, F32)

    @pl.when(row == 3)
    def _():
        rcv_n[...] = jnp.zeros(rcv_n.shape, F32)
        rcv_nw[...] = jnp.zeros(rcv_nw.shape, F32)

    frame[:, :, pl.ds(0, PAD), :] = jnp.zeros((6, 3, PAD, 128), F32)
    frame[:, :, pl.ds(PAD + 4 * ROWS, PAD), :] = jnp.zeros((6, 3, PAD, 128), F32)

    for copy in loads:
        copy.wait()

    lane42 = lanes(4, 2)

    def pack(g, carry):
        west_pack, east_pack = carry
        for k, i in [(EDGE_BLOCK * g + j, i) for j in range(EDGE_BLOCK) for i in range(3)]:
            slot = L * i + k
            rs = pl.ds(PAD + 8 * i, 8)
            west_pack = jnp.where(lane42 == slot, turn(cube[:, k, :, 0, rs, :], slot), west_pack)
            east_pack = jnp.where(lane42 == slot, turn(cube[:, k, :, 1, rs, :], slot + 1), east_pack)
        return west_pack, east_pack

    empty = jnp.zeros((4, 2, 8, 128), F32)
    west_pack, east_pack = lax.fori_loop(0, L // EDGE_BLOCK, pack, (empty, empty))
    col_w[...] = west_pack
    col_e[...] = east_pack
    for i in range(3):
        slot = 3 * L + i
        col_w[0, 0] = jnp.where(lane == slot, turn(kmt[0, pl.ds(8 * i, 8), :], slot), col_w[0, 0])

    sub42 = iota((4, 2, 8, 128), 2)

    def pack_rows(g, carry):
        low = high = empty
        for j in range(8):
            k, m = 4 * g + j // 2, j % 2
            low = jnp.where(sub42 == j, cube[:, k, m, OWN, pl.ds(PAD - j, 8), :], low)
            high = jnp.where(sub42 == j, cube[:, k, m, OWN, pl.ds(PAD + ROWS - 1 - j, 8), :], high)
        row_s[:, :, aligned(8 * g), :] = low
        row_n[:, :, aligned(8 * g), :] = high
        return carry

    lax.fori_loop(0, L // 4, pack_rows, 0)
    for f in range(4):
        row_s[f, :, pl.ds(2 * L, 8), :] = kmt[:, pl.ds(0, 8), :]
        row_n[f, :, pl.ds(2 * L, 8), :] = kmt[:, pl.ds(0, 8), :]

    pl.semaphore_wait(barrier, 11)

    def send(src, dst, ssem, rsem, r, c):
        return pltpu.make_async_remote_copy(
            src_ref=src, dst_ref=dst, send_sem=send_sem.at[ssem], recv_sem=rsem, device_id={"row": r, "col": c}, device_id_type=MESH)

    own_rows = aligned(PAD + ROWS * row, ROWS)
    south, north = jnp.maximum(row - 1, 0), jnp.minimum(row + 1, 3)
    to_w = send(col_w, rcv_e, 0, edge_sem.at[0], row, west_col)
    to_e = send(col_e, rcv_w, 1, edge_sem.at[1], row, east_col)
    to_s = send(row_s, rcv_n, 2, edge_sem.at[2], south, col)
    to_n = send(row_n, rcv_s, 3, edge_sem.at[3], north, col)
    to_nw = send(col_w.at[V], rcv_se, 4, edge_sem.at[4], north, west_col)
    to_se = send(col_e.at[U], rcv_nw, 5, edge_sem.at[5], south, east_col)
    to_w.start()
    to_e.start()

    @pl.when(has_s)
    def _():
        to_s.start()
        to_se.start()

    @pl.when(has_n)
    def _():
        to_n.start()
        to_nw.start()

    def exchange(stg, stg_w, stg_e, first, count, base, rsem, esem, wsem, pe, pw):
        out = []
        for d, r in enumerate(peers):
            out.append(send(stg.at[r % 2], frame.at[pl.ds(first, count), OWN, own_rows, :], base + d, rsem.at[row], r, col))
        for r in range(4):
            out.append(send(stg_w.at[r % 2], pe.at[row], base + 3 + 2 * r, esem.at[row], r, west_col))
            out.append(send(stg_e.at[r % 2], pw.at[row], base + 4 + 2 * r, wsem.at[row], r, east_col))
        for copy in out:
            copy.start()
        frame[pl.ds(first, count), OWN, own_rows, :] = stg[core]
        return out

    def collect(stg, stg_w, first, count, rsem, esem, wsem, pe, pw):
        for r in peers:
            rows = aligned(PAD + ROWS * r, ROWS)
            send(stg.at[0], frame.at[pl.ds(first, count), OWN, rows, :], 0, rsem.at[r], r, col).wait_recv()
        for r in range(4):
            send(stg_w.at[0], pe.at[r], 0, esem.at[r], r, east_col).wait_recv()
            send(stg_w.at[0], pw.at[r], 0, wsem.at[r], r, west_col).wait_recv()
        side = lax.broadcasted_iota(jnp.int32, (ROWS, 128), 1) // HALO
        for r in range(4):
            for j in range(count):
                frame[first + j, 2, pl.ds(PAD + ROWS * r, ROWS), :] = jnp.where(
                    side == 0, turn(pe[r], (128 - HALO * j) % 128), jnp.where(side == 3, turn(pw[r], (128 - HALO * j - HALO) % 128), 0.0))

    sent = exchange(stage, stage_w, stage_e, ETA, 4, 6, row_sem, e_sem, w_sem, pk_e, pk_w)

    to_w.wait_recv()
    to_e.wait_recv()

    @pl.when(has_n)
    def _():
        to_s.wait_recv()
        to_se.wait_recv()

    @pl.when(has_s)
    def _():
        to_n.wait_recv()
        to_nw.wait_recv()

    def unpack_rows(g, carry):
        below, above = rcv_s[:, :, aligned(8 * g), :], rcv_n[:, :, aligned(8 * g), :]
        for j in range(8):
            k, m = 4 * g + j // 2, j % 2
            cube[:, k, m, OWN, pl.ds(PAD - 1, 1), :] = below[:, :, j:j + 1, :]
            cube[:, k, m, OWN, pl.ds(PAD + ROWS, 1), :] = above[:, :, j:j + 1, :]
        return carry

    lax.fori_loop(0, L // 4, unpack_rows, 0)
    kmt[:, pl.ds(ROWS, 8), :] = rcv_n[0, :, pl.ds(2 * L, 8), :]
    for i in range(3):
        rs = pl.ds(8 * i, 8)
        wet = kmt[:, rs, :]
        halo = turn(rcv_e[0, 0], 128 - (3 * L + i))
        nuv[0, :, rs, :] = jnp.minimum(wet, east(jnp.concatenate([wet, halo[None]], axis=0), 2))
        nuv[1, :, rs, :] = jnp.minimum(wet, kmt[:, pl.ds(8 * i + 1, 8), :])

    def unpack(g, carry):
        from_e, from_w = rcv_e[...], rcv_w[...]
        for k in [EDGE_BLOCK * g + j for j in range(EDGE_BLOCK)]:
            for i in range(3):
                slot = L * i + k
                cube[:, k, :, 2, pl.ds(PAD + 8 * i, 8), :] = jnp.where(
                    lane42 < 64, turn(from_e, lax.rem(128 - slot, 128)), turn(from_w, 127 - slot))
            cube[V, k, :, 2, pl.ds(0, PAD), :] = turn(rcv_se[...], 128 - 2 * L - k)
            cube[U, k, :, 2, pl.ds(PAD + ROWS, PAD), :] = turn(rcv_nw[...], 127 - k)
        return carry

    lax.fori_loop(0, L // EDGE_BLOCK, unpack, 0)

    press = PRESS_SCALE / L
    pair = jnp.zeros((2, 8, 128), F32)

    def for_strips(body, init, reverse=False):
        def strip(s, carry):
            m = s // 3
            i = s - 3 * m
            rs = aligned(8 * i)

            def get(f, k, part, d=0):
                start = PAD + 8 * i + d
                return cube[f, k, m, part, pl.ds(start if d else pl.multiple_of(start, 8), 8), :]

            state, finish = init(m, rs)

            def block(b, state):
                for j in range(LEVEL_BLOCK):
                    k = b * LEVEL_BLOCK + j
                    state = body(L - 1 - k if reverse else k, m, rs, get, state)
                return state

            finish(m, rs, lax.fori_loop(0, L // LEVEL_BLOCK, block, state))
            return carry

        lax.fori_loop(0, 6, strip, 0)

    def momentum_init(m, rs):
        return (pair,) * 6, momentum_finish

    def momentum_finish(m, rs, state):
        sums[0, m, :, rs, :] = state[4]
        sums[1, m, :, rs, :] = state[5]

    def momentum(k, m, rs, get, state):
        cx, cy, eu, ev, gu_sum, gv_sum = state
        level = k.astype(F32)
        both = slice(0, 3)
        u, v, un, vs = get(U, k, both), get(V, k, both), get(U, k, both, 1), get(V, k, both, -1)
        rho = HALINE_CON * get(S, k, both) - THERM_EXP * get(T, k, both)
        dx = rho[OWN] - east(rho, 2)
        dy = rho[OWN] - (HALINE_CON * get(S, k, OWN, 1) - THERM_EXP * get(T, k, OWN, 1))
        vsum, usum = v + vs, u + un
        cx, cy = cx + dx, cy + dy
        gu = press * (cx - 0.5 * dx) - 0.5 * (u[OWN] * (east(u, 2) - west(u, 2))) - 0.125 * (
            (vsum[OWN] + east(vsum, 2)) * (un[OWN] - get(U, k, OWN, -1)))
        gv = press * (cy - 0.5 * dy) - 0.125 * ((usum[OWN] + west(usum, 2)) * (east(v, 2) - west(v, 2))) - 0.5 * (
            v[OWN] * (get(V, k, OWN, 1) - vs[OWN]))
        gu = jnp.where(nuv[0, :, rs, :] > level, gu, 0.0)
        gv = jnp.where(nuv[1, :, rs, :] > level, gv, 0.0)
        inverse = table[0, k]
        eu = (u[OWN] + gu + VISC_NUMBER * eu) * inverse
        ev = (v[OWN] + gv + VISC_NUMBER * ev) * inverse
        sol[U, k, m, :, rs, :] = eu
        sol[V, k, m, :, rs, :] = ev
        return cx, cy, eu, ev, gu_sum + gu, gv_sum + gv

    for_strips(momentum, momentum_init)

    collect(stage, stage_w, ETA, 4, row_sem, e_sem, w_sem, pk_e, pk_w)

    def coefficients(i, carry):
        rs = aligned(PAD + 8 * i)
        depth = frame[DEPTH, :, rs, :]
        depth_e = east(depth)
        depth_n = frame[DEPTH, :, pl.ds(PAD + 8 * i + 1, 8), :]
        wet = depth > 0.0
        coef[0, :, rs, :] = jnp.where(wet, WAVE_COURANT, 0.0)
        coef[1, :, rs, :] = jnp.where(wet & (depth_e > 0.0), 0.5 * (depth + depth_e), 0.0)
        coef[2, :, rs, :] = jnp.where(wet & (depth_n > 0.0), 0.5 * (depth + depth_n), 0.0)
        return carry

    lax.fori_loop(0, 12, coefficients, 0)

    for d in range(2):
        scale = coef[1 + d, OWN, own_rows, :] / (jnp.maximum(nuv[d], 1.0) * float(sub_count))
        for m in range(2):
            fstage[m, d] = scale * sums[d, m]
    pack_2d(fstage, 2, fstage_w, fstage_e)
    sent += exchange(fstage, fstage_w, fstage_e, FX, 2, 17, frow_sem, fe_sem, fw_sem, fpk_e, fpk_w)

    def back_init(m, rs):
        return (pair,) * 4, back_finish

    def back_finish(m, rs, state):
        for d in range(2):
            sums[d, m, :, rs, :] = state[2 + d] / jnp.maximum(nuv[d, :, rs, :], 1.0)

    def back(k, m, rs, get, state):
        x, total = list(state[:2]), list(state[2:])
        level = k.astype(F32)
        for d in range(2):
            e, n = sol[d, k, m, :, rs, :], nuv[d, :, rs, :]
            x[d] = e + table[1, k] * jnp.where(n > level + 1.0, x[d], e * table[2, k])
            sol[d, k, m, :, rs, :] = x[d]
            total[d] = total[d] + jnp.where(n > level, x[d], 0.0)
        return (*x, *total)

    for_strips(back, back_init, reverse=True)

    stores = []

    def store(f, dst):
        for lt in range(2):
            stores.append(pltpu.make_async_copy(sol.at[f, :, :, lt], dst.at[:, :, :, pl.ds(LANES * lt, LANES)], store_sem.at[2 * f + lt]))
            stores[-1].start()

    store(U, xu_hbm)
    store(V, xv_hbm)

    def tracer_init(m, rs):
        return (pair,) * 2, lambda *a: None

    def tracers(k, m, rs, get, state):
        level = k.astype(F32)
        u, v, vs = 0.5 * get(U, k, slice(0, 3)), 0.5 * get(V, k, OWN), 0.5 * get(V, k, OWN, -1)
        out = []
        for f, e in zip((T, S), state):
            t = get(f, k, slice(0, 3))
            fx = u * (t + east(t))
            t = t[OWN]
            b = t - fx[OWN] + west(fx, 2) - v * (t + get(f, k, OWN, 1)) + vs * (t + get(f, k, OWN, -1))
            b = jnp.where(kmt[:, rs, :] > level, b, 0.0)
            out.append((b + DIFF_NUMBER * e) * table[3, k])
            sol[f, k, m, :, rs, :] = out[-1]
        return tuple(out)

    for_strips(tracers, tracer_init)
    store(T, ct_hbm)
    store(S, cs_hbm)
    acc[...] = jnp.zeros(acc.shape, F32)

    collect(fstage, fstage_w, FX, 2, frow_sem, fe_sem, fw_sem, fpk_e, fpk_w)

    def subcycles(first, last, tiles):
        base = PAD + chip * (8 * (12 - tiles))

        def body(n, carry):
            def rows_of(t):
                return aligned(base + 8 * t)

            def eta_tile(t):
                rs = rows_of(t)
                u, v = frame[TX, :, rs, :], frame[TY, :, rs, :]
                div = (u - west(u)) + (v - frame[TY, :, pl.ds(base + 8 * t - 1, 8), :])
                eta = frame[ETA, :, rs, :] - coef[0, :, rs, :] * div
                frame[ETA, :, rs, :] = eta
                return u, v, WAVE_COURANT * eta

            last_row = iota((3, 8, 128), 1) == 7
            following = eta_tile(0)
            for t in range(tiles):
                u, v, e = following
                if t + 1 < tiles:
                    following = eta_tile(t + 1)
                else:
                    following = (None, None, WAVE_COURANT * frame[ETA, :, rows_of(tiles), :])
                e_n = jnp.where(last_row, pltpu.roll(following[2], 7, 1), pltpu.roll(e, 7, 1))
                rs = rows_of(t)
                frame[TX, :, rs, :] = u + frame[FX, :, rs, :] - coef[1, :, rs, :] * (east(e) - e)
                frame[TY, :, rs, :] = v + frame[FY, :, rs, :] - coef[2, :, rs, :] * (e_n - e)
            chip_rows = aligned(PAD + 2 * ROWS * chip, 2 * ROWS)
            acc[...] += weights[n] * frame[pl.ds(0, 3), OWN, chip_rows, :]
            return carry

        lax.fori_loop(first, last, body, 0)

    def tiles_at(n):
        return min(-(-(2 * ROWS + sub_count - n) // 16) * 2, 12)

    n = 0
    while n < sub_count:
        last = n
        while last < sub_count and tiles_at(last) == tiles_at(n):
            last += 1
        subcycles(n, last, tiles_at(n))
        n = last

    mine = aligned(ROWS * core, ROWS)
    theirs = aligned(ROWS * (1 - core), ROWS)
    result[...] = acc[:, :, theirs, :]
    swap = send(result, result_in, 28, swap_sem, row + 1 - 2 * core, col)
    swap.start()
    swap.wait_recv()
    for m in range(2):
        whole = jnp.where(core == m, acc[:, :, mine, :], result_in[...])
        for lt in range(2):
            ls = pl.ds(LANES * lt, LANES)
            eta_out[m, :, ls] = whole[ETA, lt]
            tx_out[m, :, ls] = whole[TX, lt]
            ty_out[m, :, ls] = whole[TY, lt]
            for d, out in enumerate((qu_out, qv_out)):
                depth = coef[1 + d, lt, own_rows, :]
                out[m, :, ls] = whole[TX + d, lt] / jnp.where(depth > 0.0, depth, 1.0) - sums[d, m, lt]
                nuv_out[d, :, ls] = nuv[d, lt]

    for copy in stores:
        copy.wait()
    to_w.wait_send()
    to_e.wait_send()

    @pl.when(has_s)
    def _():
        to_s.wait_send()
        to_se.wait_send()

    @pl.when(has_n)
    def _():
        to_n.wait_send()
        to_nw.wait_send()

    for copy in sent:
        copy.wait_send()
    swap.wait_send()


def final_kernel(level_count, xu, xv, ct, cs, qu, qv, nuv, wet, eta_in, tx_in, ty_in,
                 eta_out, tx_out, ty_out, u_out, v_out, t_out, s_out):
    ratio = sweep_constants(level_count, DIFF_NUMBER)[1]
    eta_out[...] = eta_in[...]
    tx_out[...] = tx_in[...]
    ty_out[...] = ty_in[...]
    for lt in range(2):
        ls = pl.ds(LANES * lt, LANES)
        n_wet = wet[:, ls]
        for src, out in ((ct, t_out), (cs, s_out)):
            x = jnp.zeros(TILE, F32)
            for k in reversed(range(level_count)):
                e = src[k, 0, :, ls]
                x = e + ratio[k] * jnp.where(n_wet > k + 1, x, e * (1.0 / (1.0 - ratio[k])))
                out[k, 0, :, ls] = jnp.where(n_wet > k, x, 0.0)
        for d, (src, q, out) in enumerate(((xu, qu, u_out), (xv, qv, v_out))):
            n, mean = nuv[d, :, ls], q[0, :, ls]
            for k in range(level_count):
                out[k, 0, :, ls] = jnp.where(n > float(k), src[k, 0, :, ls] + mean, 0.0)


def solution(mesh):
    col_count = mesh.shape["col"]

    def local_step(vel_x, vel_y, pot_temp, salinity, surf_eta, trans_x, trans_y, col_depth, wet_levels, avg_weights):
        L = vel_x.shape[0]
        N = avg_weights.shape[0]
        any_spec = pl.BlockSpec(memory_space=pl.ANY)
        vmem_spec = pl.BlockSpec(memory_space=pltpu.VMEM)
        cube = jax.ShapeDtypeStruct(vel_x.shape, F32)
        flat = jax.ShapeDtypeStruct(surf_eta.shape, F32)
        vm = lambda *shape: pltpu.VMEM(shape, F32)
        dma = lambda n: pltpu.SemaphoreType.DMA((n,))
        inverse, ratio = sweep_constants(L, VISC_NUMBER)
        table = jnp.array([inverse, ratio, [1.0 / (1.0 - r) for r in ratio], sweep_constants(L, DIFF_NUMBER)[0]], F32)
        xu, xv, ct, cs, qu, qv, nuv, eta_o, tx_o, ty_o = pl.pallas_call(
            functools.partial(step_kernel, col_count, L, N),
            out_shape=[cube] * 4 + [flat] * 3 + [flat] * 3,
            in_specs=[any_spec] * 4 + [vmem_spec] * 5 + [pl.BlockSpec(memory_space=pltpu.SMEM)] * 2,
            out_specs=[any_spec] * 4 + [vmem_spec] * 6,
            scratch_shapes=[
                vm(4, L, M, RING, XR, LANES), vm(4, L, M, M, ROWS, LANES), *[vm(4, M, 8, LANES)] * 4, *[vm(4, M, M * L + 8, LANES)] * 4,
                *[vm(M, 8, LANES)] * 2, vm(M, ROWS + 8, LANES), vm(M, M, ROWS, LANES), vm(M, M, M, ROWS, LANES),
                vm(M, 4, M, ROWS, LANES), *[vm(M, ROWS, LANES)] * M, *[vm(4, ROWS, LANES)] * M,
                vm(M, M, M, ROWS, LANES), *[vm(M, ROWS, LANES)] * M, *[vm(4, ROWS, LANES)] * M,
                vm(6, RING, FRAME, LANES), vm(RING, RING, FRAME, LANES), vm(RING, M, M * ROWS, LANES), *[vm(RING, M, ROWS, LANES)] * M,
                dma(8), dma(8), dma(29), dma(6), *[dma(4)] * 6, pltpu.SemaphoreType.DMA],
            compiler_params=pltpu.CompilerParams(collective_id=0, has_side_effects=True),
            name="ocean_step",
        )(vel_x, vel_y, pot_temp, salinity, surf_eta, trans_x, trans_y, col_depth, wet_levels, avg_weights, table)
        cube_spec = pl.BlockSpec((L, 1, 8, 256), lambda m, i: (0, m, i, 0))
        flat_spec = pl.BlockSpec((1, 8, 256), lambda m, i: (m, i, 0))
        outs = pl.pallas_call(
            functools.partial(final_kernel, L),
            grid=(2, 3),
            out_shape=[flat] * 3 + [cube] * 4,
            in_specs=[cube_spec] * 4 + [flat_spec] * 2
            + [pl.BlockSpec((2, 8, 256), lambda m, i: (0, i, 0)), pl.BlockSpec((8, 256), lambda m, i: (i, 0))] + [flat_spec] * 3,
            out_specs=[flat_spec] * 3 + [cube_spec] * 4,
            name="ocean_final",
        )(xu, xv, ct, cs, qu, qv, nuv, wet_levels, eta_o, tx_o, ty_o)
        return tuple(outs)

    spec_3d = P(None, None, "row", "col")
    spec_2d = P(None, "row", "col")
    spec_map = P("row", "col")
    return jax.shard_map(local_step, mesh=mesh, in_specs=(spec_3d,) * 4 + (spec_2d,) * 3 + (spec_map,) * 2 + (P(),),
                         out_specs=(spec_2d,) * 3 + (spec_3d,) * 4, check_vma=False)
```

```python
import functools

import jax
import jax.numpy as jnp
from jax import lax
from jax.experimental import pallas as pl
from jax.experimental.pallas import tpu as pltpu
from jax.sharding import PartitionSpec as P

WAVE_COURANT = 0.4
THERM_EXP = 0.2
HALINE_CON = 0.15
PRESS_SCALE = 0.5
VISC_NUMBER = 1.0
DIFF_NUMBER = 0.5

MESH = pl.DeviceIdType.MESH
F32 = jnp.float32
ROWS = 24
PAD = 8
XR = ROWS + 2 * PAD
EDGE_BLOCK = 4
LEVEL_BLOCK = 12
LANES = 128
TILE = (8, LANES)
RING = 3
M = 2
STEP_VMEM, FINAL_VMEM = 46 << 20, 8 << 20
FRAME = 4 * ROWS + 2 * PAD
HALO = 32


def sweep_constants(level_count, strength):
    inverse, ratio = [], []
    for k in range(level_count):
        pivot = 1.0 + strength if k == 0 else 1.0 + 2.0 * strength - strength * ratio[-1]
        inverse.append(1.0 / pivot)
        ratio.append(strength / pivot)
    return inverse, ratio


def iota(shape, axis):
    return lax.broadcasted_iota(jnp.int32, shape, axis)


def lanes(*lead):
    return iota((*lead, 8, 128), len(lead) + 1)


def turn(x, shift):
    return pltpu.roll(x, shift, x.ndim - 1)


def east(x, keep=3):
    rolled = turn(x, 127)
    following = rolled[1:] if keep == 2 else jnp.concatenate([rolled[1:], rolled[:1]], axis=0)
    return jnp.where(lanes(keep) == 127, following, rolled[:keep])


def west(x, keep=3):
    rolled = turn(x, 1)
    return jnp.where(lanes(keep) == 0, jnp.concatenate([rolled[2:], rolled[:keep - 1]], axis=0), rolled[:keep])


def step_kernel(
    col_count, level_count, sub_count,
    u_hbm, v_hbm, t_hbm, s_hbm, eta_in, tx_in, ty_in, depth_in, wet_in, weights, table,
    sol_u, sol_v, sol_t, sol_s, qu_out, qv_out, nuv_out, eta_out, tx_out, ty_out,
    cube,
    col_w, col_e, rcv_e, rcv_w, row_s, row_n, rcv_n, rcv_s, rcv_se, rcv_nw,
    kmt, nuv, sums, stage, stage_w, stage_e, pk_e, pk_w, fstage, fstage_w, fstage_e, fpk_e, fpk_w,
    frame, coef, acc, result, result_in,
    load_sem, send_sem, edge_sem, row_sem, e_sem, w_sem, frow_sem, fe_sem, fw_sem, swap_sem,
):
    L = level_count
    U, V, T, S = range(4)
    sol = (sol_u, sol_v, sol_t, sol_s)
    ETA, TX, TY, DEPTH, FX, FY = range(6)
    OWN = slice(0, 2)
    col = lax.axis_index("col")
    row = lax.axis_index("row")
    chip = row // 2
    core = row % 2
    east_col = lax.rem(col + 1, col_count)
    west_col = lax.rem(col + col_count - 1, col_count)
    peers = [lax.rem(row + d, 4) for d in (1, 2, 3)]
    lane = lanes()
    zero = jnp.zeros(TILE, F32)

    def aligned(start, size=8):
        return pl.ds(pl.multiple_of(start, 8), size)

    barrier = pltpu.get_barrier_semaphore()
    for r in peers:
        pl.semaphore_signal(barrier, inc=1, device_id={"row": r, "col": col}, device_id_type=MESH)
    for other in (east_col, west_col):
        for r in range(4):
            pl.semaphore_signal(barrier, inc=1, device_id={"row": r, "col": other}, device_id_type=MESH)

    loads = []
    for f, src in enumerate((u_hbm, v_hbm, t_hbm, s_hbm)):
        for lt in range(2):
            loads.append(pltpu.make_async_copy(
                src.at[:, :, :, pl.ds(LANES * lt, LANES)], cube.at[f, :, :, lt, pl.ds(PAD, ROWS), :], load_sem.at[2 * f + lt]))
            loads[-1].start()

    def pack_2d(get, count, out_w, out_e):
        for i in range(3):
            rs = pl.ds(8 * i, 8)
            for m in range(2):
                pack_w = pack_e = zero
                for j in range(count):
                    here = lane // HALO == j
                    pack_w = jnp.where(here, turn(get[m, j, 0, rs, :], HALO * j), pack_w)
                    pack_e = jnp.where(here, turn(get[m, j, 1, rs, :], (HALO * j + HALO) % 128), pack_e)
                out_w[m, rs, :] = pack_w
                out_e[m, rs, :] = pack_e

    for lt in range(2):
        ls = pl.ds(LANES * lt, LANES)
        wet = wet_in[:, ls].astype(F32)
        kmt[lt, pl.ds(0, ROWS), :] = wet
        masked = jnp.where(wet > 0.0, depth_in[:, ls], 0.0)
        for m in range(2):
            stage[m, ETA, lt] = eta_in[m, :, ls]
            stage[m, TX, lt] = tx_in[m, :, ls]
            stage[m, TY, lt] = ty_in[m, :, ls]
            stage[m, DEPTH, lt] = masked
    pack_2d(stage, 4, stage_w, stage_e)

    has_s, has_n = row > 0, row < 3

    @pl.when(row == 0)
    def _():
        rcv_s[...] = jnp.zeros(rcv_s.shape, F32)
        rcv_se[...] = jnp.zeros(rcv_se.shape, F32)

    @pl.when(row == 3)
    def _():
        rcv_n[...] = jnp.zeros(rcv_n.shape, F32)
        rcv_nw[...] = jnp.zeros(rcv_nw.shape, F32)

    frame[:, :, pl.ds(0, PAD), :] = jnp.zeros((6, 3, PAD, 128), F32)
    frame[:, :, pl.ds(PAD + 4 * ROWS, PAD), :] = jnp.zeros((6, 3, PAD, 128), F32)

    for copy in loads:
        copy.wait()

    lane42 = lanes(4, 2)

    def pack(g, carry):
        west_pack, east_pack = carry
        for k, i in [(EDGE_BLOCK * g + j, i) for j in range(EDGE_BLOCK) for i in range(3)]:
            slot = L * i + k
            rs = pl.ds(PAD + 8 * i, 8)
            west_pack = jnp.where(lane42 == slot, turn(cube[:, k, :, 0, rs, :], slot), west_pack)
            east_pack = jnp.where(lane42 == slot, turn(cube[:, k, :, 1, rs, :], slot + 1), east_pack)
        return west_pack, east_pack

    empty = jnp.zeros((4, 2, 8, 128), F32)
    west_pack, east_pack = lax.fori_loop(0, L // EDGE_BLOCK, pack, (empty, empty))
    col_w[...] = west_pack
    col_e[...] = east_pack
    for i in range(3):
        slot = 3 * L + i
        col_w[0, 0] = jnp.where(lane == slot, turn(kmt[0, pl.ds(8 * i, 8), :], slot), col_w[0, 0])

    sub42 = iota((4, 2, 8, 128), 2)

    def pack_rows(g, carry):
        low = high = empty
        for j in range(8):
            k, m = 4 * g + j // 2, j % 2
            low = jnp.where(sub42 == j, cube[:, k, m, OWN, pl.ds(PAD - j, 8), :], low)
            high = jnp.where(sub42 == j, cube[:, k, m, OWN, pl.ds(PAD + ROWS - 1 - j, 8), :], high)
        row_s[:, :, aligned(8 * g), :] = low
        row_n[:, :, aligned(8 * g), :] = high
        return carry

    lax.fori_loop(0, L // 4, pack_rows, 0)
    for f in range(4):
        row_s[f, :, pl.ds(2 * L, 8), :] = kmt[:, pl.ds(0, 8), :]
        row_n[f, :, pl.ds(2 * L, 8), :] = kmt[:, pl.ds(0, 8), :]

    pl.semaphore_wait(barrier, 11)

    def send(src, dst, ssem, rsem, r, c):
        return pltpu.make_async_remote_copy(
            src_ref=src, dst_ref=dst, send_sem=send_sem.at[ssem], recv_sem=rsem, device_id={"row": r, "col": c}, device_id_type=MESH)

    own_rows = aligned(PAD + ROWS * row, ROWS)
    south, north = jnp.maximum(row - 1, 0), jnp.minimum(row + 1, 3)
    to_w = send(col_w, rcv_e, 0, edge_sem.at[0], row, west_col)
    to_e = send(col_e, rcv_w, 1, edge_sem.at[1], row, east_col)
    to_s = send(row_s, rcv_n, 2, edge_sem.at[2], south, col)
    to_n = send(row_n, rcv_s, 3, edge_sem.at[3], north, col)
    to_nw = send(col_w.at[V], rcv_se, 4, edge_sem.at[4], north, west_col)
    to_se = send(col_e.at[U], rcv_nw, 5, edge_sem.at[5], south, east_col)
    to_w.start()
    to_e.start()

    @pl.when(has_s)
    def _():
        to_s.start()
        to_se.start()

    @pl.when(has_n)
    def _():
        to_n.start()
        to_nw.start()

    def exchange(stg, stg_w, stg_e, first, count, base, rsem, esem, wsem, pe, pw):
        out = []
        for d, r in enumerate(peers):
            out.append(send(stg.at[r % 2], frame.at[pl.ds(first, count), OWN, own_rows, :], base + d, rsem.at[row], r, col))
        for r in range(4):
            out.append(send(stg_w.at[r % 2], pe.at[row], base + 3 + 2 * r, esem.at[row], r, west_col))
            out.append(send(stg_e.at[r % 2], pw.at[row], base + 4 + 2 * r, wsem.at[row], r, east_col))
        for copy in out:
            copy.start()
        frame[pl.ds(first, count), OWN, own_rows, :] = stg[core]
        return out

    def collect(stg, stg_w, first, count, rsem, esem, wsem, pe, pw):
        for r in peers:
            rows = aligned(PAD + ROWS * r, ROWS)
            send(stg.at[0], frame.at[pl.ds(first, count), OWN, rows, :], 0, rsem.at[r], r, col).wait_recv()
        for r in range(4):
            send(stg_w.at[0], pe.at[r], 0, esem.at[r], r, east_col).wait_recv()
            send(stg_w.at[0], pw.at[r], 0, wsem.at[r], r, west_col).wait_recv()
        side = lax.broadcasted_iota(jnp.int32, (ROWS, 128), 1) // HALO
        for r in range(4):
            for j in range(count):
                frame[first + j, 2, pl.ds(PAD + ROWS * r, ROWS), :] = jnp.where(
                    side == 0, turn(pe[r], (128 - HALO * j) % 128), jnp.where(side == 3, turn(pw[r], (128 - HALO * j - HALO) % 128), 0.0))

    to_w.wait_recv()
    to_e.wait_recv()

    @pl.when(has_n)
    def _():
        to_s.wait_recv()
        to_se.wait_recv()

    @pl.when(has_s)
    def _():
        to_n.wait_recv()
        to_nw.wait_recv()

    sent = exchange(stage, stage_w, stage_e, ETA, 4, 6, row_sem, e_sem, w_sem, pk_e, pk_w)

    def unpack_rows(g, carry):
        below, above = rcv_s[:, :, aligned(8 * g), :], rcv_n[:, :, aligned(8 * g), :]
        for j in range(8):
            k, m = 4 * g + j // 2, j % 2
            cube[:, k, m, OWN, pl.ds(PAD - 1, 1), :] = below[:, :, j:j + 1, :]
            cube[:, k, m, OWN, pl.ds(PAD + ROWS, 1), :] = above[:, :, j:j + 1, :]
        return carry

    lax.fori_loop(0, L // 4, unpack_rows, 0)
    kmt[:, pl.ds(ROWS, 8), :] = rcv_n[0, :, pl.ds(2 * L, 8), :]
    for i in range(3):
        rs = pl.ds(8 * i, 8)
        wet = kmt[:, rs, :]
        halo = turn(rcv_e[0, 0], 128 - (3 * L + i))
        nuv[0, :, rs, :] = jnp.minimum(wet, east(jnp.concatenate([wet, halo[None]], axis=0), 2))
        nuv[1, :, rs, :] = jnp.minimum(wet, kmt[:, pl.ds(8 * i + 1, 8), :])

    def unpack(g, carry):
        from_e, from_w = rcv_e[...], rcv_w[...]
        for k in [EDGE_BLOCK * g + j for j in range(EDGE_BLOCK)]:
            for i in range(3):
                slot = L * i + k
                cube[:, k, :, 2, pl.ds(PAD + 8 * i, 8), :] = jnp.where(
                    lane42 < 64, turn(from_e, lax.rem(128 - slot, 128)), turn(from_w, 127 - slot))
            cube[V, k, :, 2, pl.ds(0, PAD), :] = turn(rcv_se[...], 128 - 2 * L - k)
            cube[U, k, :, 2, pl.ds(PAD + ROWS, PAD), :] = turn(rcv_nw[...], 127 - k)
        return carry

    lax.fori_loop(0, L // EDGE_BLOCK, unpack, 0)

    press = PRESS_SCALE / L
    pair = jnp.zeros((2, 8, 128), F32)

    def for_strips(body, init, reverse=False):
        def strip(s, carry):
            m = s // 3
            i = s - 3 * m
            rs = aligned(8 * i)

            def get(f, k, part, d=0):
                start = PAD + 8 * i + d
                return cube[f, k, m, part, pl.ds(start if d else pl.multiple_of(start, 8), 8), :]

            state, finish = init(m, rs)

            def block(b, state):
                for j in range(LEVEL_BLOCK):
                    k = b * LEVEL_BLOCK + j
                    state = body(L - 1 - k if reverse else k, m, rs, get, state)
                return state

            finish(m, rs, lax.fori_loop(0, L // LEVEL_BLOCK, block, state))
            return carry

        lax.fori_loop(0, 6, strip, 0)

    def momentum_init(m, rs):
        return (pair,) * 6, momentum_finish

    def momentum_finish(m, rs, state):
        sums[0, m, :, rs, :] = state[4]
        sums[1, m, :, rs, :] = state[5]

    def momentum(k, m, rs, get, state):
        cx, cy, eu, ev, gu_sum, gv_sum = state
        level = k.astype(F32)
        both = slice(0, 3)
        u, v, un, vs = get(U, k, both), get(V, k, both), get(U, k, both, 1), get(V, k, both, -1)
        rho = HALINE_CON * get(S, k, both) - THERM_EXP * get(T, k, both)
        dx = rho[OWN] - east(rho, 2)
        dy = rho[OWN] - (HALINE_CON * get(S, k, OWN, 1) - THERM_EXP * get(T, k, OWN, 1))
        vsum, usum = v + vs, u + un
        cx, cy = cx + dx, cy + dy
        gu = press * (cx - 0.5 * dx) - 0.5 * (u[OWN] * (east(u, 2) - west(u, 2))) - 0.125 * (
            (vsum[OWN] + east(vsum, 2)) * (un[OWN] - get(U, k, OWN, -1)))
        gv = press * (cy - 0.5 * dy) - 0.125 * ((usum[OWN] + west(usum, 2)) * (east(v, 2) - west(v, 2))) - 0.5 * (
            v[OWN] * (get(V, k, OWN, 1) - vs[OWN]))
        gu = jnp.where(nuv[0, :, rs, :] > level, gu, 0.0)
        gv = jnp.where(nuv[1, :, rs, :] > level, gv, 0.0)
        inverse = table[0, k]
        eu = (u[OWN] + gu + VISC_NUMBER * eu) * inverse
        ev = (v[OWN] + gv + VISC_NUMBER * ev) * inverse
        sol[U][k, m, :, rs, :] = eu
        sol[V][k, m, :, rs, :] = ev
        return cx, cy, eu, ev, gu_sum + gu, gv_sum + gv

    for_strips(momentum, momentum_init)

    collect(stage, stage_w, ETA, 4, row_sem, e_sem, w_sem, pk_e, pk_w)

    def coefficients(i, carry):
        rs = aligned(PAD + 8 * i)
        depth = frame[DEPTH, :, rs, :]
        depth_e = east(depth)
        depth_n = frame[DEPTH, :, pl.ds(PAD + 8 * i + 1, 8), :]
        wet = depth > 0.0
        coef[0, :, rs, :] = jnp.where(wet, WAVE_COURANT, 0.0)
        coef[1, :, rs, :] = jnp.where(wet & (depth_e > 0.0), 0.5 * (depth + depth_e), 0.0)
        coef[2, :, rs, :] = jnp.where(wet & (depth_n > 0.0), 0.5 * (depth + depth_n), 0.0)
        return carry

    lax.fori_loop(0, 12, coefficients, 0)

    for d in range(2):
        scale = coef[1 + d, OWN, own_rows, :] / (jnp.maximum(nuv[d], 1.0) * float(sub_count))
        for m in range(2):
            fstage[m, d] = scale * sums[d, m]
    pack_2d(fstage, 2, fstage_w, fstage_e)
    sent += exchange(fstage, fstage_w, fstage_e, FX, 2, 17, frow_sem, fe_sem, fw_sem, fpk_e, fpk_w)

    def back_init(m, rs):
        return (pair,) * 4, back_finish

    def back_finish(m, rs, state):
        for d in range(2):
            sums[d, m, :, rs, :] = state[2 + d] / jnp.maximum(nuv[d, :, rs, :], 1.0)

    def back(k, m, rs, get, state):
        x, total = list(state[:2]), list(state[2:])
        level = k.astype(F32)
        for d in range(2):
            e, n = sol[d][k, m, :, rs, :], nuv[d, :, rs, :]
            x[d] = e + table[1, k] * jnp.where(n > level + 1.0, x[d], e * table[2, k])
            sol[d][k, m, :, rs, :] = x[d]
            total[d] = total[d] + jnp.where(n > level, x[d], 0.0)
        return (*x, *total)

    for_strips(back, back_init, reverse=True)

    def tracer_init(m, rs):
        return (pair,) * 2, lambda *a: None

    def tracers(k, m, rs, get, state):
        level = k.astype(F32)
        u, v, vs = 0.5 * get(U, k, slice(0, 3)), 0.5 * get(V, k, OWN), 0.5 * get(V, k, OWN, -1)
        out = []
        for f, e in zip((T, S), state):
            t = get(f, k, slice(0, 3))
            fx = u * (t + east(t))
            t = t[OWN]
            b = t - fx[OWN] + west(fx, 2) - v * (t + get(f, k, OWN, 1)) + vs * (t + get(f, k, OWN, -1))
            b = jnp.where(kmt[:, rs, :] > level, b, 0.0)
            out.append((b + DIFF_NUMBER * e) * table[3, k])
            sol[f][k, m, :, rs, :] = out[-1]
        return tuple(out)

    for_strips(tracers, tracer_init)
    acc[...] = jnp.zeros(acc.shape, F32)

    collect(fstage, fstage_w, FX, 2, frow_sem, fe_sem, fw_sem, fpk_e, fpk_w)

    def subcycles(first, last, tiles):
        base = PAD + chip * (8 * (12 - tiles))

        def body(n, carry):
            def rows_of(t):
                return aligned(base + 8 * t)

            def eta_tile(t):
                rs = rows_of(t)
                u, v = frame[TX, :, rs, :], frame[TY, :, rs, :]
                div = (u - west(u)) + (v - frame[TY, :, pl.ds(base + 8 * t - 1, 8), :])
                eta = frame[ETA, :, rs, :] - coef[0, :, rs, :] * div
                frame[ETA, :, rs, :] = eta
                return u, v, WAVE_COURANT * eta

            last_row = iota((3, 8, 128), 1) == 7
            following = eta_tile(0)
            for t in range(tiles):
                u, v, e = following
                if t + 1 < tiles:
                    following = eta_tile(t + 1)
                else:
                    following = (None, None, WAVE_COURANT * frame[ETA, :, rows_of(tiles), :])
                e_n = jnp.where(last_row, pltpu.roll(following[2], 7, 1), pltpu.roll(e, 7, 1))
                rs = rows_of(t)
                frame[TX, :, rs, :] = u + frame[FX, :, rs, :] - coef[1, :, rs, :] * (east(e) - e)
                frame[TY, :, rs, :] = v + frame[FY, :, rs, :] - coef[2, :, rs, :] * (e_n - e)
            chip_rows = aligned(PAD + 2 * ROWS * chip, 2 * ROWS)
            acc[...] += weights[n] * frame[pl.ds(0, 3), OWN, chip_rows, :]
            return carry

        lax.fori_loop(first, last, body, 0)

    def tiles_at(n):
        return min(-(-(2 * ROWS + sub_count - n) // 16) * 2, 12)

    n = 0
    while n < sub_count:
        last = n
        while last < sub_count and tiles_at(last) == tiles_at(n):
            last += 1
        subcycles(n, last, tiles_at(n))
        n = last

    mine = aligned(ROWS * core, ROWS)
    theirs = aligned(ROWS * (1 - core), ROWS)
    result[...] = acc[:, :, theirs, :]
    swap = send(result, result_in, 28, swap_sem, row + 1 - 2 * core, col)
    swap.start()
    swap.wait_recv()
    for m in range(2):
        whole = jnp.where(core == m, acc[:, :, mine, :], result_in[...])
        for lt in range(2):
            ls = pl.ds(LANES * lt, LANES)
            eta_out[m, :, ls] = whole[ETA, lt]
            tx_out[m, :, ls] = whole[TX, lt]
            ty_out[m, :, ls] = whole[TY, lt]
            for d, out in enumerate((qu_out, qv_out)):
                depth = coef[1 + d, lt, own_rows, :]
                out[m, :, ls] = whole[TX + d, lt] / jnp.where(depth > 0.0, depth, 1.0) - sums[d, m, lt]
                nuv_out[d, :, ls] = nuv[d, lt]

    to_w.wait_send()
    to_e.wait_send()

    @pl.when(has_s)
    def _():
        to_s.wait_send()
        to_se.wait_send()

    @pl.when(has_n)
    def _():
        to_n.wait_send()
        to_nw.wait_send()

    for copy in sent:
        copy.wait_send()
    swap.wait_send()


def final_kernel(level_count, sol_u, sol_v, sol_t, sol_s, qu, qv, nuv, wet, eta_in, tx_in, ty_in, eta_out, tx_out, ty_out, u_out, v_out, t_out, s_out):
    ratio = sweep_constants(level_count, DIFF_NUMBER)[1]
    m = pl.program_id(0)
    rs = pl.ds(pl.multiple_of(pl.program_id(1) * 8, 8), 8)
    eta_out[...] = eta_in[...]
    tx_out[...] = tx_in[...]
    ty_out[...] = ty_in[...]
    for lt in range(2):
        ls = pl.ds(LANES * lt, LANES)
        n_wet = wet[:, ls]
        for src, out in ((sol_t, t_out), (sol_s, s_out)):
            x = jnp.zeros(TILE, F32)
            for k in reversed(range(level_count)):
                e = src[k, m, lt, rs, :]
                x = e + ratio[k] * jnp.where(n_wet > k + 1, x, e * (1.0 / (1.0 - ratio[k])))
                out[k, 0, :, ls] = jnp.where(n_wet > k, x, 0.0)
        for d, (src, q, out) in enumerate(((sol_u, qu, u_out), (sol_v, qv, v_out))):
            n, mean = nuv[d, :, ls], q[0, :, ls]
            for k in range(level_count):
                out[k, 0, :, ls] = jnp.where(n > float(k), src[k, m, lt, rs, :] + mean, 0.0)


def solution(mesh):
    col_count = mesh.shape["col"]

    def local_step(vel_x, vel_y, pot_temp, salinity, surf_eta, trans_x, trans_y, col_depth, wet_levels, avg_weights):
        L = vel_x.shape[0]
        N = avg_weights.shape[0]
        hbm_spec = pl.BlockSpec(memory_space=pltpu.HBM)
        vmem_spec = pl.BlockSpec(memory_space=pltpu.VMEM)
        cube = jax.ShapeDtypeStruct(vel_x.shape, F32)
        flat = jax.ShapeDtypeStruct(surf_eta.shape, F32)
        vm = lambda *shape: pltpu.VMEM(shape, F32)
        dma = lambda n: pltpu.SemaphoreType.DMA((n,))
        inverse, ratio = sweep_constants(L, VISC_NUMBER)
        table = jnp.array([inverse, ratio, [1.0 / (1.0 - r) for r in ratio], sweep_constants(L, DIFF_NUMBER)[0]], F32)
        *sol, qu, qv, nuv, eta_o, tx_o, ty_o = pl.pallas_call(
            functools.partial(step_kernel, col_count, L, N),
            out_shape=[jax.ShapeDtypeStruct((L, M, M, ROWS, LANES), F32)] * 4 + [flat] * 6,
            in_specs=[hbm_spec] * 4 + [vmem_spec] * 5 + [pl.BlockSpec(memory_space=pltpu.SMEM)] * 2,
            out_specs=[vmem_spec] * 10,
            scratch_shapes=[
                vm(4, L, M, RING, XR, LANES), *[vm(4, M, 8, LANES)] * 4, *[vm(4, M, M * L + 8, LANES)] * 4,
                *[vm(M, 8, LANES)] * 2, vm(M, ROWS + 8, LANES), vm(M, M, ROWS, LANES), vm(M, M, M, ROWS, LANES),
                vm(M, 4, M, ROWS, LANES), *[vm(M, ROWS, LANES)] * M, *[vm(4, ROWS, LANES)] * M,
                vm(M, M, M, ROWS, LANES), *[vm(M, ROWS, LANES)] * M, *[vm(4, ROWS, LANES)] * M,
                vm(6, RING, FRAME, LANES), vm(RING, RING, FRAME, LANES), vm(RING, M, M * ROWS, LANES), *[vm(RING, M, ROWS, LANES)] * M,
                dma(8), dma(29), dma(6), *[dma(4)] * 6, pltpu.SemaphoreType.DMA],
            compiler_params=pltpu.CompilerParams(collective_id=0, has_side_effects=True, vmem_limit_bytes=STEP_VMEM),
            name="ocean_step",
        )(vel_x, vel_y, pot_temp, salinity, surf_eta, trans_x, trans_y, col_depth, wet_levels, avg_weights, table)
        cube_spec = pl.BlockSpec((L, 1, 8, 256), lambda m, i: (0, m, i, 0))
        flat_spec = pl.BlockSpec((1, 8, 256), lambda m, i: (m, i, 0))
        outs = pl.pallas_call(
            functools.partial(final_kernel, L),
            grid=(2, 3),
            out_shape=[flat] * 3 + [cube] * 4,
            in_specs=[vmem_spec] * 4 + [flat_spec] * 2
            + [pl.BlockSpec((2, 8, 256), lambda m, i: (0, i, 0)), pl.BlockSpec((8, 256), lambda m, i: (i, 0))] + [flat_spec] * 3,
            out_specs=[flat_spec] * 3 + [cube_spec] * 4,
            name="ocean_final",
            compiler_params=pltpu.CompilerParams(vmem_limit_bytes=FINAL_VMEM),
        )(*sol, qu, qv, nuv, wet_levels, eta_o, tx_o, ty_o)
        return tuple(outs)

    spec_3d = P(None, None, "row", "col")
    spec_2d = P(None, "row", "col")
    spec_map = P("row", "col")
    return jax.shard_map(local_step, mesh=mesh, in_specs=(spec_3d,) * 4 + (spec_2d,) * 3 + (spec_map,) * 2 + (P(),),
                         out_specs=(spec_2d,) * 3 + (spec_3d,) * 4, check_vma=False)
```

```python
import functools

import jax
import jax.numpy as jnp
from jax import lax
from jax.experimental import pallas as pl
from jax.experimental.pallas import tpu as pltpu
from jax.sharding import PartitionSpec as P

WAVE_COURANT = 0.4
THERM_EXP = 0.2
HALINE_CON = 0.15
PRESS_SCALE = 0.5
VISC_NUMBER = 1.0
DIFF_NUMBER = 0.5

MESH = pl.DeviceIdType.MESH
F32 = jnp.float32
ROWS = 24
PAD = 8
XR = ROWS + 2 * PAD
EDGE_BLOCK = 4
LEVEL_BLOCK = 12
LANES = 128
SUB = 8
TILE = (SUB, LANES)
PAIR, STRIPS, QUAD, OCTET = range(2), range(3), range(4), range(SUB)
RING = 3
M = 2
STEP_VMEM, FINAL_VMEM = 46 << 20, 8 << 20
FRAME = 4 * ROWS + 2 * PAD
HALO = 32


def sweep_constants(level_count, strength):
    inverse, ratio = [], []
    for k in range(level_count):
        pivot = 1.0 + strength if k == 0 else 1.0 + 2.0 * strength - strength * ratio[-1]
        inverse.append(1.0 / pivot)
        ratio.append(strength / pivot)
    return inverse, ratio


def iota(shape, axis):
    return lax.broadcasted_iota(jnp.int32, shape, axis)


def lanes(*lead):
    return iota((*lead, 8, 128), len(lead) + 1)


def turn(x, shift):
    return pltpu.roll(x, shift, x.ndim - 1)


def east(x):
    rolled = turn(x, 127)
    return jnp.where(lanes(3) == 127, jnp.concatenate([rolled[1:], rolled[:1]], axis=0), rolled)


def west(x):
    rolled = turn(x, 1)
    return jnp.where(lanes(3) == 0, jnp.concatenate([rolled[2:], rolled[:2]], axis=0), rolled)


def east_block(x):
    rolled = turn(x[:2], 127)
    return jnp.where(lanes(2) == 127, jnp.concatenate([rolled[1:], x[2:]], axis=0), rolled)


def west_block(x):
    rolled = turn(x[:2], 1)
    return jnp.where(lanes(2) == 0, jnp.concatenate([x[2:], rolled[:1]], axis=0), rolled)


ETA, TX, TY, DEPTH, PACK, KMT = range(6)


def pack_2d(stage, count, put):
    lane = lanes()
    for i in STRIPS:
        rs = pl.ds(SUB * i, SUB)
        for m in PAIR:
            pack_w = pack_e = jnp.zeros(TILE, F32)
            for j in range(count):
                here = lane // HALO == j
                pack_w = jnp.where(here, turn(stage[m, j, 0, rs, :], HALO * j), pack_w)
                pack_e = jnp.where(here, turn(stage[m, j, 1, rs, :], (HALO * j + HALO) % LANES), pack_e)
            put(m, rs, pack_w, pack_e)


def stage_kernel(sub_count, eta, tx, ty, depth, wet_in, weights, stage):
    for lt in PAIR:
        ls = pl.ds(LANES * lt, LANES)
        wet = wet_in[:, ls].astype(F32)
        masked = jnp.where(wet > 0.0, depth[:, ls], 0.0)
        stage[0, KMT, lt] = wet
        for m in PAIR:
            for j, field in ((ETA, eta), (TX, tx), (TY, ty)):
                stage[m, j, lt] = field[m, :, ls]
            stage[m, DEPTH, lt] = masked
    for n in range(sub_count):
        stage[1, KMT, n // ROWS, pl.ds(n % ROWS, 1), :] = jnp.full((1, LANES), weights[n], F32)

    def put(m, rs, pack_w, pack_e):
        stage[m, PACK, 0, rs, :] = pack_w
        stage[m, PACK, 1, rs, :] = pack_e

    pack_2d(stage, 4, put)


def step_kernel(
    col_count, level_count, sub_count,
    u_hbm, v_hbm, t_hbm, s_hbm, stage,
    sol_u, sol_v, sol_t, sol_s, qu_out, qv_out, nuv_out, eta_out, tx_out, ty_out,
    cube,
    col_w, col_e, rcv_e, rcv_w, row_s, row_n, rcv_n, rcv_s, rcv_se, rcv_nw,
    kmt, nuv, sums, pk_e, pk_w, fstage, fstage_w, fstage_e, fpk_e, fpk_w,
    frame, coef, acc, result, result_in,
    table, load_sem, send_sem, edge_sem, row_sem, e_sem, w_sem, frow_sem, fe_sem, fw_sem, swap_sem,
):
    L = level_count
    U, V, T, S = range(4)
    sol = (sol_u, sol_v, sol_t, sol_s)
    FX, FY = 4, 5
    OWN = slice(0, 2)
    col = lax.axis_index("col")
    row = lax.axis_index("row")
    chip = row // 2
    core = row % 2
    east_col = lax.rem(col + 1, col_count)
    west_col = lax.rem(col + col_count - 1, col_count)
    peers = [lax.rem(row + d, 4) for d in (1, 2, 3)]
    lane = lanes()
    zero = jnp.zeros(TILE, F32)

    def aligned(start, size=8):
        return pl.ds(pl.multiple_of(start, 8), size)

    barrier = pltpu.get_barrier_semaphore()
    for r in peers:
        pl.semaphore_signal(barrier, inc=1, device_id={"row": r, "col": col}, device_id_type=MESH)
    for other in (east_col, west_col):
        for r in QUAD:
            pl.semaphore_signal(barrier, inc=1, device_id={"row": r, "col": other}, device_id_type=MESH)

    loads = []
    for f, src in enumerate((u_hbm, v_hbm, t_hbm, s_hbm)):
        for lt in PAIR:
            loads.append(pltpu.make_async_copy(
                src.at[:, :, :, pl.ds(LANES * lt, LANES)], cube.at[f, :, :, lt, pl.ds(PAD, ROWS), :], load_sem.at[2 * f + lt]))
            loads[-1].start()

    inv_v, ratio_v = sweep_constants(L, VISC_NUMBER)
    for n, line in enumerate((inv_v, ratio_v, [1.0 / (1.0 - r) for r in ratio_v], sweep_constants(L, DIFF_NUMBER)[0])):
        for k in range(L):
            table[n, k] = line[k]

    kmt[:, pl.ds(0, ROWS), :] = stage[0, KMT]

    has_s, has_n = row > 0, row < 3

    @pl.when(row == 0)
    def _():
        rcv_s[...] = jnp.zeros(rcv_s.shape, F32)
        rcv_se[...] = jnp.zeros(rcv_se.shape, F32)

    @pl.when(row == 3)
    def _():
        rcv_n[...] = jnp.zeros(rcv_n.shape, F32)
        rcv_nw[...] = jnp.zeros(rcv_nw.shape, F32)

    frame[:, :, pl.ds(0, PAD), :] = jnp.zeros((6, 3, PAD, 128), F32)
    frame[:, :, pl.ds(PAD + 4 * ROWS, PAD), :] = jnp.zeros((6, 3, PAD, 128), F32)

    for copy in loads:
        copy.wait()

    lane42 = lanes(4, 2)

    def pack(g, carry):
        west_pack, east_pack = carry
        for k, i in [(EDGE_BLOCK * g + j, i) for j in range(EDGE_BLOCK) for i in STRIPS]:
            slot = L * i + k
            rs = pl.ds(PAD + SUB * i, SUB)
            west_pack = jnp.where(lane42 == slot, turn(cube[:, k, :, 0, rs, :], slot), west_pack)
            east_pack = jnp.where(lane42 == slot, turn(cube[:, k, :, 1, rs, :], slot + 1), east_pack)
        return west_pack, east_pack

    empty = jnp.zeros((4, M, SUB, LANES), F32)
    west_pack, east_pack = lax.fori_loop(0, L // EDGE_BLOCK, pack, (empty, empty))
    col_w[...] = west_pack
    col_e[...] = east_pack
    for i in STRIPS:
        slot = 3 * L + i
        col_w[0, 0] = jnp.where(lane == slot, turn(kmt[0, pl.ds(SUB * i, SUB), :], slot), col_w[0, 0])

    sub42 = iota((4, M, SUB, LANES), 2)

    def pack_rows(g, carry):
        low = high = empty
        for j in OCTET:
            k, m = 4 * g + j // 2, j % 2
            low = jnp.where(sub42 == j, cube[:, k, m, OWN, pl.ds(PAD - j, 8), :], low)
            high = jnp.where(sub42 == j, cube[:, k, m, OWN, pl.ds(PAD + ROWS - 1 - j, 8), :], high)
        rows = aligned(SUB * g)
        row_s[:V + 1, :, rows, :] = low[:T]
        row_s[T, :, rows, :] = low[T] - (HALINE_CON / THERM_EXP) * low[S]
        row_s[S:, :, rows, :] = low[T:]
        row_n[:, :, rows, :] = high
        return carry

    lax.fori_loop(0, L // 4, pack_rows, 0)
    row_s[U, :, pl.ds(M * L, SUB), :] = kmt[:, pl.ds(0, SUB), :]

    pl.semaphore_wait(barrier, 11)

    def send(src, dst, ssem, rsem, r, c):
        return pltpu.make_async_remote_copy(
            src_ref=src, dst_ref=dst, send_sem=send_sem.at[ssem], recv_sem=rsem, device_id={"row": r, "col": c}, device_id_type=MESH)

    own_rows = aligned(PAD + ROWS * row, ROWS)
    south, north = jnp.maximum(row - 1, 0), jnp.minimum(row + 1, 3)
    to_w = send(col_w, rcv_e, 0, edge_sem.at[0], row, west_col)
    to_e = send(col_e, rcv_w, 1, edge_sem.at[1], row, east_col)
    first_s, first_n = pl.ds(0, 3), pl.ds(0, 2)
    later_s, later_n = pl.ds(3, 2), pl.ds(2, 2)
    to_s = send(row_s.at[first_s], rcv_n.at[first_s], 2, edge_sem.at[2], south, col)
    to_n = send(row_n.at[first_n], rcv_s.at[first_n], 3, edge_sem.at[3], north, col)
    to_s_later = send(row_s.at[later_s], rcv_n.at[later_s], 6, edge_sem.at[6], south, col)
    to_n_later = send(row_n.at[later_n], rcv_s.at[later_n], 7, edge_sem.at[7], north, col)
    to_nw = send(col_w.at[V], rcv_se, 4, edge_sem.at[4], north, west_col)
    to_se = send(col_e.at[U], rcv_nw, 5, edge_sem.at[5], south, east_col)
    to_w.start()
    to_e.start()

    @pl.when(has_s)
    def _():
        to_s.start()
        to_se.start()
        to_s_later.start()

    @pl.when(has_n)
    def _():
        to_n.start()
        to_nw.start()
        to_n_later.start()

    def exchange(block, pack_w, pack_e, first, count, base, rsem, esem, wsem, pe, pw):
        out = []
        for d, r in enumerate(peers):
            out.append(send(block(r % 2), frame.at[pl.ds(first, count), OWN, own_rows, :], base + d, rsem.at[row], r, col))
        for r in QUAD:
            out.append(send(pack_w(r % 2), pe.at[row], base + 3 + 2 * r, esem.at[row], r, west_col))
            out.append(send(pack_e(r % 2), pw.at[row], base + 4 + 2 * r, wsem.at[row], r, east_col))
        for copy in out:
            copy.start()
        frame[pl.ds(first, count), OWN, own_rows, :] = block(core)[...]
        return out

    def collect(block, pack_w, first, count, rsem, esem, wsem, pe, pw):
        for r in peers:
            rows = aligned(PAD + ROWS * r, ROWS)
            send(block(0), frame.at[pl.ds(first, count), OWN, rows, :], 0, rsem.at[r], r, col).wait_recv()
        for r in QUAD:
            send(pack_w(0), pe.at[r], 0, esem.at[r], r, east_col).wait_recv()
            send(pack_w(0), pw.at[r], 0, wsem.at[r], r, west_col).wait_recv()
        side = lax.broadcasted_iota(jnp.int32, (ROWS, 128), 1) // HALO
        for r in QUAD:
            for j in range(count):
                frame[first + j, 2, pl.ds(PAD + ROWS * r, ROWS), :] = jnp.where(
                    side == 0, turn(pe[r], (128 - HALO * j) % 128), jnp.where(side == 3, turn(pw[r], (128 - HALO * j - HALO) % 128), 0.0))

    def stage_block(m):
        return stage.at[m, pl.ds(0, PACK)]

    def stage_w(m):
        return stage.at[m, PACK, 0]

    def stage_e(m):
        return stage.at[m, PACK, 1]

    to_w.wait_recv()
    to_e.wait_recv()

    def unpack(g, carry):
        from_e, from_w = rcv_e[...], rcv_w[...]
        for k in [EDGE_BLOCK * g + j for j in range(EDGE_BLOCK)]:
            for i in STRIPS:
                slot = L * i + k
                cube[:, k, :, 2, pl.ds(PAD + SUB * i, SUB), :] = jnp.where(
                    lane42 < 64, turn(from_w, lax.rem(128 - slot, 128)), turn(from_e, 127 - slot))
        return carry

    lax.fori_loop(0, L // EDGE_BLOCK, unpack, 0)

    def masks(i):
        rs = pl.ds(SUB * i, SUB)
        wet = kmt[:, rs, :]
        halo = turn(rcv_e[0, 0], 127 - (3 * L + i))
        nuv[0, :, rs, :] = jnp.minimum(wet, east_block(jnp.concatenate([wet, halo[None]], axis=0)))
        nuv[1, :, rs, :] = jnp.minimum(wet, kmt[:, pl.ds(8 * i + 1, 8), :])

    masks(0)
    masks(1)

    press = PRESS_SCALE / L
    pair = jnp.zeros((M, SUB, LANES), F32)

    def for_strips(body, init, reverse=False, strips=(0, 1, 3)):
        start, step, count = strips

        def strip(s, carry):
            m = s // count
            i = start + step * (s - count * m)
            rs = aligned(SUB * i)

            def get(f, k, part, d=0):
                start = PAD + 8 * i + d
                return cube[f, k, m, part, pl.ds(start if d else pl.multiple_of(start, 8), 8), :]

            state, finish = init(m, rs)

            def block(b, state):
                for j in range(LEVEL_BLOCK):
                    k = b * LEVEL_BLOCK + j
                    state = body(L - 1 - k if reverse else k, m, rs, get, state)
                return state

            finish(m, rs, lax.fori_loop(0, L // LEVEL_BLOCK, block, state))
            return carry

        lax.fori_loop(0, M * count, strip, 0)

    def momentum_init(m, rs):
        return (pair,) * 6, momentum_finish

    def momentum_finish(m, rs, state):
        sums[0, m, :, rs, :] = state[4]
        sums[1, m, :, rs, :] = state[5]

    def momentum(k, m, rs, get, state):
        cx, cy, eu, ev, gu_sum, gv_sum = state
        level = k.astype(F32)
        both = slice(0, 3)
        u, v, un, vs = get(U, k, both), get(V, k, both), get(U, k, both, 1), get(V, k, both, -1)
        rho = HALINE_CON * get(S, k, both) - THERM_EXP * get(T, k, both)
        dx = rho[OWN] - east_block(rho)
        dy = rho[OWN] - (HALINE_CON * get(S, k, OWN, 1) - THERM_EXP * get(T, k, OWN, 1))
        vsum, usum = v + vs, u + un
        cx, cy = cx + dx, cy + dy
        gu = press * (cx - 0.5 * dx) - 0.5 * (u[OWN] * (east_block(u) - west_block(u))) - 0.125 * (
            (vsum[OWN] + east_block(vsum)) * (un[OWN] - get(U, k, OWN, -1)))
        gv = press * (cy - 0.5 * dy) - 0.125 * ((usum[OWN] + west_block(usum)) * (east_block(v) - west_block(v))) - 0.5 * (
            v[OWN] * (get(V, k, OWN, 1) - vs[OWN]))
        gu = jnp.where(nuv[0, :, rs, :] > level, gu, 0.0)
        gv = jnp.where(nuv[1, :, rs, :] > level, gv, 0.0)
        inverse = table[0, k]
        eu = (u[OWN] + gu + VISC_NUMBER * eu) * inverse
        ev = (v[OWN] + gv + VISC_NUMBER * ev) * inverse
        sol[U][k, m, :, rs, :] = eu
        sol[V][k, m, :, rs, :] = ev
        return cx, cy, eu, ev, gu_sum + gu, gv_sum + gv

    for_strips(momentum, momentum_init, strips=(1, 1, 1))

    @pl.when(has_n)
    def _():
        to_s.wait_recv()
        to_se.wait_recv()

    @pl.when(has_s)
    def _():
        to_n.wait_recv()
        to_nw.wait_recv()

    sent = exchange(stage_block, stage_w, stage_e, ETA, 4, 8, row_sem, e_sem, w_sem, pk_e, pk_w)

    def unpack_rows(g, carry):
        rows = aligned(SUB * g)
        below, above = rcv_s[:T, :, rows, :], rcv_n[:S, :, rows, :]
        for j in OCTET:
            k, m = 4 * g + j // 2, j % 2
            cube[:T, k, m, OWN, pl.ds(PAD - 1, 1), :] = below[:, :, j:j + 1, :]
            cube[:S, k, m, OWN, pl.ds(PAD + ROWS, 1), :] = above[:, :, j:j + 1, :]
            cube[S, k, m, OWN, pl.ds(PAD + ROWS, 1), :] = jnp.zeros((M, 1, LANES), F32)
            if m:
                cube[V, k, :, 2, pl.ds(0, PAD), :] = turn(rcv_se[...], 127 - 2 * L - k)
                cube[U, k, :, 2, pl.ds(PAD + ROWS, PAD), :] = turn(rcv_nw[...], lax.rem(128 - k, 128))
        return carry

    def unpack_rows_later(g, carry):
        rows = aligned(SUB * g)
        below, above = rcv_s[T:, :, rows, :], rcv_n[S:, :, rows, :]
        for j in OCTET:
            k, m = 4 * g + j // 2, j % 2
            cube[T:, k, m, OWN, pl.ds(PAD - 1, 1), :] = below[:, :, j:j + 1, :]
            cube[T:, k, m, OWN, pl.ds(PAD + ROWS, 1), :] = above[:, :, j:j + 1, :]
        return carry

    lax.fori_loop(0, L // 4, unpack_rows, 0)
    kmt[:, pl.ds(ROWS, 8), :] = rcv_n[U, :, pl.ds(M * L, SUB), :]
    masks(2)
    for_strips(momentum, momentum_init, strips=(0, 2, 2))

    collect(stage_block, stage_w, ETA, 4, row_sem, e_sem, w_sem, pk_e, pk_w)

    def coefficients(i, carry):
        rs = aligned(PAD + 8 * i)
        depth = frame[DEPTH, :, rs, :]
        depth_e = east(depth)
        depth_n = frame[DEPTH, :, pl.ds(PAD + 8 * i + 1, 8), :]
        wet = depth > 0.0
        coef[0, :, rs, :] = jnp.where(wet, WAVE_COURANT, 0.0)
        coef[1, :, rs, :] = jnp.where(wet & (depth_e > 0.0), 0.5 * (depth + depth_e), 0.0)
        coef[2, :, rs, :] = jnp.where(wet & (depth_n > 0.0), 0.5 * (depth + depth_n), 0.0)
        return carry

    lax.fori_loop(0, 12, coefficients, 0)

    for d in PAIR:
        scale = coef[1 + d, OWN, own_rows, :] / (jnp.maximum(nuv[d], 1.0) * float(sub_count))
        for m in PAIR:
            fstage[m, d] = scale * sums[d, m]

    def put(m, rs, pack_w, pack_e):
        fstage_w[m, rs, :] = pack_w
        fstage_e[m, rs, :] = pack_e

    pack_2d(fstage, 2, put)
    sent += exchange(lambda m: fstage.at[m], lambda m: fstage_w.at[m], lambda m: fstage_e.at[m], FX, 2, 19, frow_sem, fe_sem, fw_sem, fpk_e, fpk_w)

    def back_init(m, rs):
        return (pair,) * 4, back_finish

    def back_finish(m, rs, state):
        for d in PAIR:
            sums[d, m, :, rs, :] = state[2 + d] / jnp.maximum(nuv[d, :, rs, :], 1.0)

    def back(k, m, rs, get, state):
        x, total = list(state[:2]), list(state[2:])
        level = k.astype(F32)
        for d in PAIR:
            e, n = sol[d][k, m, :, rs, :], nuv[d, :, rs, :]
            x[d] = e + table[1, k] * jnp.where(n > level + 1.0, x[d], e * table[2, k])
            sol[d][k, m, :, rs, :] = x[d]
            total[d] = total[d] + jnp.where(n > level, x[d], 0.0)
        return (*x, *total)

    for_strips(back, back_init, reverse=True)

    def tracer_init(m, rs):
        return (pair,) * 2, lambda *a: None

    def tracers(k, m, rs, get, state):
        level = k.astype(F32)
        u, v, vs = 0.5 * get(U, k, slice(0, 3)), 0.5 * get(V, k, OWN), 0.5 * get(V, k, OWN, -1)
        out = []
        for f, e in zip((T, S), state):
            t = get(f, k, slice(0, 3))
            fx = u * (t + jnp.concatenate([east_block(t), t[:1]], axis=0))
            t = t[OWN]
            b = t - fx[OWN] + west_block(fx) - v * (t + get(f, k, OWN, 1)) + vs * (t + get(f, k, OWN, -1))
            b = jnp.where(kmt[:, rs, :] > level, b, 0.0)
            out.append((b + DIFF_NUMBER * e) * table[3, k])
            sol[f][k, m, :, rs, :] = out[-1]
        return tuple(out)

    @pl.when(has_n)
    def _():
        to_s_later.wait_recv()

    @pl.when(has_s)
    def _():
        to_n_later.wait_recv()

    lax.fori_loop(0, L // 4, unpack_rows_later, 0)
    for_strips(tracers, tracer_init)
    acc[...] = jnp.zeros(acc.shape, F32)

    collect(lambda m: fstage.at[m], lambda m: fstage_w.at[m], FX, 2, frow_sem, fe_sem, fw_sem, fpk_e, fpk_w)

    def subcycles(first, last, tiles):
        base = PAD + chip * (8 * (12 - tiles))

        def body(n, carry):
            def rows_of(t):
                return aligned(base + 8 * t)

            def eta_tile(t):
                rs = rows_of(t)
                u, v = frame[TX, :, rs, :], frame[TY, :, rs, :]
                div = (u - west(u)) + (v - frame[TY, :, pl.ds(base + 8 * t - 1, 8), :])
                eta = frame[ETA, :, rs, :] - coef[0, :, rs, :] * div
                frame[ETA, :, rs, :] = eta
                return u, v, WAVE_COURANT * eta

            last_row = iota((3, 8, 128), 1) == 7
            following = eta_tile(0)
            for t in range(tiles):
                u, v, e = following
                if t + 1 < tiles:
                    following = eta_tile(t + 1)
                else:
                    following = (None, None, WAVE_COURANT * frame[ETA, :, rows_of(tiles), :])
                e_n = jnp.where(last_row, pltpu.roll(following[2], 7, 1), pltpu.roll(e, 7, 1))
                rs = rows_of(t)
                frame[TX, :, rs, :] = u + frame[FX, :, rs, :] - coef[1, :, rs, :] * (east(e) - e)
                frame[TY, :, rs, :] = v + frame[FY, :, rs, :] - coef[2, :, rs, :] * (e_n - e)
            chip_rows = aligned(PAD + 2 * ROWS * chip, 2 * ROWS)
            acc[...] += stage[1, KMT, n // ROWS, pl.ds(lax.rem(n, ROWS), 1), :] * frame[pl.ds(0, 3), OWN, chip_rows, :]
            return carry

        lax.fori_loop(first, last, body, 0)

    def tiles_at(n):
        return min(-(-(2 * ROWS + sub_count - n) // 16) * 2, 12)

    n = 0
    while n < sub_count:
        last = n
        while last < sub_count and tiles_at(last) == tiles_at(n):
            last += 1
        subcycles(n, last, tiles_at(n))
        n = last

    mine = aligned(ROWS * core, ROWS)
    theirs = aligned(ROWS * (1 - core), ROWS)
    result[...] = acc[:, :, theirs, :]
    swap = send(result, result_in, 30, swap_sem, row + 1 - 2 * core, col)
    swap.start()
    swap.wait_recv()
    for m in PAIR:
        whole = jnp.where(core == m, acc[:, :, mine, :], result_in[...])
        for lt in PAIR:
            ls = pl.ds(LANES * lt, LANES)
            eta_out[m, :, ls] = whole[ETA, lt]
            tx_out[m, :, ls] = whole[TX, lt]
            ty_out[m, :, ls] = whole[TY, lt]
            for d, out in enumerate((qu_out, qv_out)):
                depth = coef[1 + d, lt, own_rows, :]
                out[m, :, ls] = whole[TX + d, lt] / jnp.where(depth > 0.0, depth, 1.0) - sums[d, m, lt]
                nuv_out[d, :, ls] = nuv[d, lt]

    to_w.wait_send()
    to_e.wait_send()

    @pl.when(has_s)
    def _():
        to_s.wait_send()
        to_se.wait_send()
        to_s_later.wait_send()

    @pl.when(has_n)
    def _():
        to_n.wait_send()
        to_nw.wait_send()
        to_n_later.wait_send()

    for copy in sent:
        copy.wait_send()
    swap.wait_send()


def final_kernel(level_count, sol_u, sol_v, sol_t, sol_s, qu, qv, nuv, wet, eta_in, tx_in, ty_in, eta_out, tx_out, ty_out, u_out, v_out, t_out, s_out):
    ratio = sweep_constants(level_count, DIFF_NUMBER)[1]
    m = pl.program_id(0)
    rs = pl.ds(pl.multiple_of(pl.program_id(1) * 8, 8), 8)
    eta_out[...] = eta_in[...]
    tx_out[...] = tx_in[...]
    ty_out[...] = ty_in[...]
    for lt in PAIR:
        ls = pl.ds(LANES * lt, LANES)
        n_wet = wet[:, ls]
        for src, out in ((sol_t, t_out), (sol_s, s_out)):
            x = jnp.zeros(TILE, F32)
            for k in reversed(range(level_count)):
                e = src[k, m, lt, rs, :]
                x = e + ratio[k] * jnp.where(n_wet > k + 1, x, e * (1.0 / (1.0 - ratio[k])))
                out[k, 0, :, ls] = jnp.where(n_wet > k, x, 0.0)
        for d, (src, q, out) in enumerate(((sol_u, qu, u_out), (sol_v, qv, v_out))):
            n, mean = nuv[d, :, ls], q[0, :, ls]
            for k in range(level_count):
                out[k, 0, :, ls] = jnp.where(n > float(k), src[k, m, lt, rs, :] + mean, 0.0)


def solution(mesh):
    col_count = mesh.shape["col"]

    def local_step(vel_x, vel_y, pot_temp, salinity, surf_eta, trans_x, trans_y, col_depth, wet_levels, avg_weights):
        L = vel_x.shape[0]
        N = avg_weights.shape[0]
        hbm_spec = pl.BlockSpec(memory_space=pltpu.HBM)
        vmem_spec = pl.BlockSpec(memory_space=pltpu.VMEM)
        cube = jax.ShapeDtypeStruct(vel_x.shape, F32)
        flat = jax.ShapeDtypeStruct(surf_eta.shape, F32)
        vm = lambda *shape: pltpu.VMEM(shape, F32)
        dma = lambda n: pltpu.SemaphoreType.DMA((n,))
        stage = pl.pallas_call(
            functools.partial(stage_kernel, N),
            out_shape=jax.ShapeDtypeStruct((M, 6, M, ROWS, LANES), F32),
            in_specs=[vmem_spec] * 5 + [pl.BlockSpec(memory_space=pltpu.SMEM)],
            out_specs=vmem_spec,
            name="ocean_stage",
        )(surf_eta, trans_x, trans_y, col_depth, wet_levels, avg_weights)
        *sol, qu, qv, nuv, eta_o, tx_o, ty_o = pl.pallas_call(
            functools.partial(step_kernel, col_count, L, N),
            out_shape=[jax.ShapeDtypeStruct((L, M, M, ROWS, LANES), F32)] * 4 + [flat] * 6,
            in_specs=[hbm_spec] * 4 + [vmem_spec],
            out_specs=[vmem_spec] * 10,
            scratch_shapes=[
                vm(4, L, M, RING, XR, LANES), *[vm(4, M, 8, LANES)] * 4, vm(5, M, M * L + 8, LANES), vm(4, M, M * L, LANES), vm(5, M, M * L + 8, LANES), vm(4, M, M * L, LANES),
                *[vm(M, 8, LANES)] * 2, vm(M, ROWS + 8, LANES), vm(M, M, ROWS, LANES), vm(M, M, M, ROWS, LANES),
                *[vm(4, ROWS, LANES)] * M,
                vm(M, M, M, ROWS, LANES), *[vm(M, ROWS, LANES)] * M, *[vm(4, ROWS, LANES)] * M,
                vm(6, RING, FRAME, LANES), vm(RING, RING, FRAME, LANES), vm(RING, M, M * ROWS, LANES), *[vm(RING, M, ROWS, LANES)] * M,
                pltpu.SMEM((4, L), F32), dma(8), dma(31), dma(8), *[dma(4)] * 6, pltpu.SemaphoreType.DMA],
            compiler_params=pltpu.CompilerParams(collective_id=0, has_side_effects=True, vmem_limit_bytes=STEP_VMEM),
            name="ocean_step",
        )(vel_x, vel_y, pot_temp, salinity, stage)
        cube_spec = pl.BlockSpec((L, 1, 8, 256), lambda m, i: (0, m, i, 0))
        flat_spec = pl.BlockSpec((1, 8, 256), lambda m, i: (m, i, 0))
        outs = pl.pallas_call(
            functools.partial(final_kernel, L),
            grid=(2, 3),
            out_shape=[flat] * 3 + [cube] * 4,
            in_specs=[vmem_spec] * 4 + [flat_spec] * 2
            + [pl.BlockSpec((2, 8, 256), lambda m, i: (0, i, 0)), pl.BlockSpec((8, 256), lambda m, i: (i, 0))] + [flat_spec] * 3,
            out_specs=[flat_spec] * 3 + [cube_spec] * 4,
            name="ocean_final",
            compiler_params=pltpu.CompilerParams(vmem_limit_bytes=FINAL_VMEM),
        )(*sol, qu, qv, nuv, wet_levels, eta_o, tx_o, ty_o)
        return tuple(outs)

    spec_3d = P(None, None, "row", "col")
    spec_2d = P(None, "row", "col")
    spec_map = P("row", "col")
    return jax.shard_map(local_step, mesh=mesh, in_specs=(spec_3d,) * 4 + (spec_2d,) * 3 + (spec_map,) * 2 + (P(),),
                         out_specs=(spec_2d,) * 3 + (spec_3d,) * 4, check_vma=False)
```

```python
import functools

import jax
import jax.numpy as jnp
from jax import lax
from jax.experimental import pallas as pl
from jax.experimental.pallas import tpu as pltpu
from jax.sharding import PartitionSpec as P

WAVE_COURANT = 0.4
THERM_EXP = 0.2
HALINE_CON = 0.15
PRESS_SCALE = 0.5
VISC_NUMBER = 1.0
DIFF_NUMBER = 0.5

MESH = pl.DeviceIdType.MESH
F32 = jnp.float32
ROWS = 24
PAD = 8
XR = ROWS + 2 * PAD
EDGE_BLOCK = 12
TRACER_BLOCK = 12
SUB_BLOCK = 3
LEVEL_BLOCK = 12
LANES = 128
SUB = 8
TILE = (SUB, LANES)
PAIR, STRIPS, QUAD, OCTET = range(2), range(3), range(4), range(SUB)
RING = 3
M = 2
STEP_VMEM, FINAL_VMEM = 46 << 20, 8 << 20
TILES = 10
SHIFT = 16
FPAD = SHIFT + PAD
FRAME = 4 * ROWS + 2 * FPAD
HALO = 32


def sweep_constants(level_count, strength):
    inverse, ratio = [], []
    for k in range(level_count):
        pivot = 1.0 + strength if k == 0 else 1.0 + 2.0 * strength - strength * ratio[-1]
        inverse.append(1.0 / pivot)
        ratio.append(strength / pivot)
    return inverse, ratio


def iota(shape, axis):
    return lax.broadcasted_iota(jnp.int32, shape, axis)


def lanes(*lead):
    return iota((*lead, 8, 128), len(lead) + 1)


def turn(x, shift):
    return pltpu.roll(x, shift, x.ndim - 1)


def east(x):
    rolled = turn(x, 127)
    return jnp.where(lanes(3) == 127, jnp.concatenate([rolled[1:], rolled[:1]], axis=0), rolled)


def west(x):
    rolled = turn(x, 1)
    return jnp.where(lanes(3) == 0, jnp.concatenate([rolled[2:], rolled[:2]], axis=0), rolled)


def east_block(x):
    rolled = turn(x[:2], 127)
    return jnp.where(lanes(2) == 127, jnp.concatenate([rolled[1:], x[2:]], axis=0), rolled)


def west_block(x):
    rolled = turn(x[:2], 1)
    return jnp.where(lanes(2) == 0, jnp.concatenate([x[2:], rolled[:1]], axis=0), rolled)


ETA, TX, TY, DEPTH, PACK, KMT = range(6)


def pack_2d(stage, count, put):
    lane = lanes()
    for i in STRIPS:
        rs = pl.ds(SUB * i, SUB)
        for m in PAIR:
            pack_w = pack_e = jnp.zeros(TILE, F32)
            for j in range(count):
                here = lane // HALO == j
                pack_w = jnp.where(here, turn(stage[m, j, 0, rs, :], HALO * j), pack_w)
                pack_e = jnp.where(here, turn(stage[m, j, 1, rs, :], (HALO * j + HALO) % LANES), pack_e)
            put(m, rs, pack_w, pack_e)


def stage_kernel(sub_count, eta, tx, ty, depth, wet_in, weights, stage):
    for lt in PAIR:
        ls = pl.ds(LANES * lt, LANES)
        wet = wet_in[:, ls].astype(F32)
        masked = jnp.where(wet > 0.0, depth[:, ls], 0.0)
        stage[0, KMT, lt] = wet
        for m in PAIR:
            for j, field in ((ETA, eta), (TX, tx), (TY, ty)):
                stage[m, j, lt] = field[m, :, ls]
            stage[m, DEPTH, lt] = masked
    for n in range(sub_count):
        stage[1, KMT, n // ROWS, pl.ds(n % ROWS, 1), :] = jnp.full((1, LANES), weights[n], F32)

    def put(m, rs, pack_w, pack_e):
        stage[m, PACK, 0, rs, :] = pack_w
        stage[m, PACK, 1, rs, :] = pack_e

    pack_2d(stage, 4, put)


def step_kernel(
    col_count, level_count, sub_count,
    u_hbm, v_hbm, t_hbm, s_hbm, stage,
    sol_u, sol_v, sol_t, sol_s, qu_out, qv_out, nuv_out, eta_out, tx_out, ty_out,
    cube,
    col_w, col_e, rcv_e, rcv_w, row_s, row_n, rcv_n, rcv_s, rcv_se, rcv_nw,
    kmt, nuv, sums, pk_e, pk_w, fstage, fstage_w, fstage_e, fpk_e, fpk_w,
    frame, coef, acc, result, result_in,
    table, load_sem, send_sem, edge_sem, row_sem, e_sem, w_sem, frow_sem, fe_sem, fw_sem, swap_sem,
):
    L = level_count
    U, V, T, S = range(4)
    sol = (sol_u, sol_v, sol_t, sol_s)
    FX, FY = 4, 5
    OWN = slice(0, 2)
    col = lax.axis_index("col")
    row = lax.axis_index("row")
    chip = row // 2
    core = row % 2
    east_col = lax.rem(col + 1, col_count)
    west_col = lax.rem(col + col_count - 1, col_count)
    peers = [lax.rem(row + d, 4) for d in (1, 2, 3)]
    lane = lanes()
    zero = jnp.zeros(TILE, F32)

    def aligned(start, size=8):
        return pl.ds(pl.multiple_of(start, 8), size)

    barrier = pltpu.get_barrier_semaphore()
    for r in peers:
        pl.semaphore_signal(barrier, inc=1, device_id={"row": r, "col": col}, device_id_type=MESH)
    for other in (east_col, west_col):
        for r in QUAD:
            pl.semaphore_signal(barrier, inc=1, device_id={"row": r, "col": other}, device_id_type=MESH)

    loads = []
    for f, src in enumerate((u_hbm, v_hbm, t_hbm, s_hbm)):
        for lt in PAIR:
            loads.append(pltpu.make_async_copy(
                src.at[:, :, :, pl.ds(LANES * lt, LANES)], cube.at[f, :, :, lt, pl.ds(PAD, ROWS), :], load_sem.at[2 * f + lt]))
            loads[-1].start()

    inv_v, ratio_v = sweep_constants(L, VISC_NUMBER)
    for n, line in enumerate((inv_v, ratio_v, [1.0 / (1.0 - r) for r in ratio_v], sweep_constants(L, DIFF_NUMBER)[0])):
        for k in range(L):
            table[n, k] = line[k]

    kmt[:, pl.ds(0, ROWS), :] = stage[0, KMT]

    has_s, has_n = row > 0, row < 3

    @pl.when(row == 0)
    def _():
        rcv_s[...] = jnp.zeros(rcv_s.shape, F32)
        rcv_se[...] = jnp.zeros(rcv_se.shape, F32)

    @pl.when(row == 3)
    def _():
        rcv_n[...] = jnp.zeros(rcv_n.shape, F32)
        rcv_nw[...] = jnp.zeros(rcv_nw.shape, F32)

    outside = jnp.zeros((6, RING, PAD, LANES), F32)

    @pl.when(chip == 0)
    def _():
        frame[:, :, pl.ds(FPAD - PAD, PAD), :] = outside

    @pl.when(chip == 1)
    def _():
        frame[:, :, pl.ds(FPAD + SUB * TILES, PAD), :] = outside


    lane42 = lanes(4, 2)
    lane2 = lanes(M)
    empty = jnp.zeros((M, SUB, LANES), F32)
    for f in QUAD:
        for copy in loads[2 * f:2 * f + 2]:
            copy.wait()

        def pack(g, carry):
            west_pack, east_pack = carry
            for k, i in [(EDGE_BLOCK * g + j, i) for j in range(EDGE_BLOCK) for i in STRIPS]:
                slot = L * i + k
                rs = pl.ds(PAD + SUB * i, SUB)
                west_pack = jnp.where(lane2 == slot, turn(cube[f, k, :, 0, rs, :], slot), west_pack)
                east_pack = jnp.where(lane2 == slot, turn(cube[f, k, :, 1, rs, :], slot + 1), east_pack)
            for q in range(M * EDGE_BLOCK // SUB):
                rows = aligned(M * EDGE_BLOCK * g + SUB * q)
                low = high = empty
                for j in OCTET:
                    k, m = EDGE_BLOCK * g + (SUB * q + j) // M, j % M
                    low = jnp.where(sub2 == j, cube[f, k, m, OWN, pl.ds(PAD - j, SUB), :], low)
                    high = jnp.where(sub2 == j, cube[f, k, m, OWN, pl.ds(PAD + ROWS - 1 - j, SUB), :], high)
                row_n[f, :, rows, :] = high
                row_s[f if f < T else f + 1, :, rows, :] = low
                if f == S:
                    row_s[T, :, rows, :] = row_s[T + 1, :, rows, :] - (HALINE_CON / THERM_EXP) * low
            return west_pack, east_pack

        sub2 = iota((M, SUB, LANES), 1)
        col_w[f], col_e[f] = lax.fori_loop(0, L // EDGE_BLOCK, pack, (empty, empty))
    for i in STRIPS:
        slot = 3 * L + i
        col_w[0, 0] = jnp.where(lane == slot, turn(kmt[0, pl.ds(SUB * i, SUB), :], slot), col_w[0, 0])
    row_s[U, :, pl.ds(M * L, SUB), :] = kmt[:, pl.ds(0, SUB), :]

    pl.semaphore_wait(barrier, 11)

    def send(src, dst, ssem, rsem, r, c):
        return pltpu.make_async_remote_copy(
            src_ref=src, dst_ref=dst, send_sem=send_sem.at[ssem], recv_sem=rsem, device_id={"row": r, "col": c}, device_id_type=MESH)

    def frame_rows(r, at_chip):
        return aligned(FPAD + ROWS * r - SHIFT * at_chip, ROWS)

    own_rows = frame_rows(row, chip)
    south, north = jnp.maximum(row - 1, 0), jnp.minimum(row + 1, 3)
    to_w = send(col_w, rcv_e, 0, edge_sem.at[0], row, west_col)
    to_e = send(col_e, rcv_w, 1, edge_sem.at[1], row, east_col)
    first_s, first_n = pl.ds(0, 3), pl.ds(0, 2)
    later_s, later_n = pl.ds(3, 2), pl.ds(2, 2)
    to_s = send(row_s.at[first_s], rcv_n.at[first_s], 2, edge_sem.at[2], south, col)
    to_n = send(row_n.at[first_n], rcv_s.at[first_n], 3, edge_sem.at[3], north, col)
    to_s_later = send(row_s.at[later_s], rcv_n.at[later_s], 6, edge_sem.at[6], south, col)
    to_n_later = send(row_n.at[later_n], rcv_s.at[later_n], 7, edge_sem.at[7], north, col)
    to_nw = send(col_w.at[V], rcv_se, 4, edge_sem.at[4], north, west_col)
    to_se = send(col_e.at[U], rcv_nw, 5, edge_sem.at[5], south, east_col)
    to_w.start()
    to_e.start()

    @pl.when(has_s)
    def _():
        to_s.start()
        to_se.start()
        to_s_later.start()

    @pl.when(has_n)
    def _():
        to_n.start()
        to_nw.start()
        to_n_later.start()

    def exchange(block, pack_w, pack_e, first, count, base, rsem, esem, wsem, pe, pw):
        out = []
        for d, r in enumerate(peers):
            out.append(send(block(r % 2), frame.at[pl.ds(first, count), OWN, frame_rows(row, r // 2), :], base + d, rsem.at[row], r, col))
        for r in QUAD:
            out.append(send(pack_w(r % 2), pe.at[row], base + 3 + 2 * r, esem.at[row], r, west_col))
            out.append(send(pack_e(r % 2), pw.at[row], base + 4 + 2 * r, wsem.at[row], r, east_col))
        for copy in out:
            copy.start()
        frame[pl.ds(first, count), OWN, own_rows, :] = block(core)[...]
        return out

    def collect(block, pack_w, first, count, rsem, esem, wsem, pe, pw):
        for r in peers:
            rows = frame_rows(r, chip)
            send(block(0), frame.at[pl.ds(first, count), OWN, rows, :], 0, rsem.at[r], r, col).wait_recv()
        for r in QUAD:
            send(pack_w(0), pe.at[r], 0, esem.at[r], r, east_col).wait_recv()
            send(pack_w(0), pw.at[r], 0, wsem.at[r], r, west_col).wait_recv()
        side = lax.broadcasted_iota(jnp.int32, (ROWS, 128), 1) // HALO
        for r in QUAD:
            for j in range(count):
                frame[first + j, 2, frame_rows(r, chip), :] = jnp.where(
                    side == 0, turn(pe[r], (128 - HALO * j) % 128), jnp.where(side == 3, turn(pw[r], (128 - HALO * j - HALO) % 128), 0.0))

    def stage_block(m):
        return stage.at[m, pl.ds(0, PACK)]

    def stage_w(m):
        return stage.at[m, PACK, 0]

    def stage_e(m):
        return stage.at[m, PACK, 1]

    to_w.wait_recv()
    to_e.wait_recv()

    def unpack(g, carry):
        from_e, from_w = rcv_e[...], rcv_w[...]
        for k in [EDGE_BLOCK * g + j for j in range(EDGE_BLOCK)]:
            for i in STRIPS:
                slot = L * i + k
                cube[:, k, :, 2, pl.ds(PAD + SUB * i, SUB), :] = jnp.where(
                    lane42 < 64, turn(from_w, lax.rem(128 - slot, 128)), turn(from_e, 127 - slot))
        return carry

    lax.fori_loop(0, L // EDGE_BLOCK, unpack, 0)

    def masks(i):
        rs = pl.ds(SUB * i, SUB)
        wet = kmt[:, rs, :]
        halo = turn(rcv_e[0, 0], 127 - (3 * L + i))
        nuv[0, :, rs, :] = jnp.minimum(wet, east_block(jnp.concatenate([wet, halo[None]], axis=0)))
        nuv[1, :, rs, :] = jnp.minimum(wet, kmt[:, pl.ds(8 * i + 1, 8), :])

    masks(0)
    masks(1)

    press = PRESS_SCALE / L
    pair = jnp.zeros((M, SUB, LANES), F32)

    def for_strips(body, init, reverse=False, strips=(0, 1, 3), levels=LEVEL_BLOCK):
        start, step, count = strips

        def strip(s, carry):
            m = s // count
            i = start + step * (s - count * m)
            rs = aligned(SUB * i)

            def get(f, k, part, d=0):
                start = PAD + 8 * i + d
                return cube[f, k, m, part, pl.ds(start if d else pl.multiple_of(start, 8), 8), :]

            state, finish = init(m, rs)

            def block(b, state):
                for j in range(levels):
                    k = b * levels + j
                    state = body(L - 1 - k if reverse else k, m, rs, get, state)
                return state

            finish(m, rs, lax.fori_loop(0, L // levels, block, state))
            return carry

        lax.fori_loop(0, M * count, strip, 0)

    def momentum_init(m, rs):
        return (pair,) * 6, momentum_finish

    def momentum_finish(m, rs, state):
        sums[0, m, :, rs, :] = state[4]
        sums[1, m, :, rs, :] = state[5]

    def momentum(k, m, rs, get, state):
        cx, cy, eu, ev, gu_sum, gv_sum = state
        level = k.astype(F32)
        both = slice(0, 3)
        u, v, un, vs = get(U, k, both), get(V, k, both), get(U, k, both, 1), get(V, k, both, -1)
        rho = HALINE_CON * get(S, k, both) - THERM_EXP * get(T, k, both)
        dx = rho[OWN] - east_block(rho)
        dy = rho[OWN] - (HALINE_CON * get(S, k, OWN, 1) - THERM_EXP * get(T, k, OWN, 1))
        vsum, usum = v + vs, u + un
        cx, cy = cx + dx, cy + dy
        gu = press * (cx - 0.5 * dx) - 0.5 * (u[OWN] * (east_block(u) - west_block(u))) - 0.125 * (
            (vsum[OWN] + east_block(vsum)) * (un[OWN] - get(U, k, OWN, -1)))
        gv = press * (cy - 0.5 * dy) - 0.125 * ((usum[OWN] + west_block(usum)) * (east_block(v) - west_block(v))) - 0.5 * (
            v[OWN] * (get(V, k, OWN, 1) - vs[OWN]))
        gu = jnp.where(nuv[0, :, rs, :] > level, gu, 0.0)
        gv = jnp.where(nuv[1, :, rs, :] > level, gv, 0.0)
        inverse = table[0, k]
        eu = (u[OWN] + gu + VISC_NUMBER * eu) * inverse
        ev = (v[OWN] + gv + VISC_NUMBER * ev) * inverse
        sol[U][k, m, :, rs, :] = eu
        sol[V][k, m, :, rs, :] = ev
        return cx, cy, eu, ev, gu_sum + gu, gv_sum + gv

    for_strips(momentum, momentum_init, strips=(1, 1, 1))

    @pl.when(has_n)
    def _():
        to_s.wait_recv()
        to_se.wait_recv()

    @pl.when(has_s)
    def _():
        to_n.wait_recv()
        to_nw.wait_recv()

    sent = exchange(stage_block, stage_w, stage_e, ETA, 4, 8, row_sem, e_sem, w_sem, pk_e, pk_w)

    def unpack_rows(g, carry):
        rows = aligned(SUB * g)
        below, above = rcv_s[:T, :, rows, :], rcv_n[:S, :, rows, :]
        for j in OCTET:
            k, m = 4 * g + j // 2, j % 2
            cube[:T, k, m, OWN, pl.ds(PAD - 1, 1), :] = below[:, :, j:j + 1, :]
            cube[:S, k, m, OWN, pl.ds(PAD + ROWS, 1), :] = above[:, :, j:j + 1, :]
            cube[S, k, m, OWN, pl.ds(PAD + ROWS, 1), :] = jnp.zeros((M, 1, LANES), F32)
            if m:
                cube[V, k, :, 2, pl.ds(0, PAD), :] = turn(rcv_se[...], 127 - 2 * L - k)
                cube[U, k, :, 2, pl.ds(PAD + ROWS, PAD), :] = turn(rcv_nw[...], lax.rem(128 - k, 128))
        return carry

    def unpack_rows_later(g, carry):
        rows = aligned(SUB * g)
        below, above = rcv_s[T:, :, rows, :], rcv_n[S:, :, rows, :]
        for j in OCTET:
            k, m = 4 * g + j // 2, j % 2
            cube[T:, k, m, OWN, pl.ds(PAD - 1, 1), :] = below[:, :, j:j + 1, :]
            cube[T:, k, m, OWN, pl.ds(PAD + ROWS, 1), :] = above[:, :, j:j + 1, :]
        return carry

    lax.fori_loop(0, L // 4, unpack_rows, 0)
    kmt[:, pl.ds(ROWS, 8), :] = rcv_n[U, :, pl.ds(M * L, SUB), :]
    masks(2)
    for_strips(momentum, momentum_init, strips=(0, 2, 2))

    collect(stage_block, stage_w, ETA, 4, row_sem, e_sem, w_sem, pk_e, pk_w)

    def coefficients(i, carry):
        rs = aligned(FPAD + SUB * i)
        depth = frame[DEPTH, :, rs, :]
        depth_e = east(depth)
        depth_n = frame[DEPTH, :, pl.ds(FPAD + SUB * i + 1, SUB), :]
        wet = depth > 0.0
        coef[0, :, rs, :] = jnp.where(wet, WAVE_COURANT, 0.0)
        coef[1, :, rs, :] = jnp.where(wet & (depth_e > 0.0), 0.5 * (depth + depth_e), 0.0)
        coef[2, :, rs, :] = jnp.where(wet & (depth_n > 0.0), 0.5 * (depth + depth_n), 0.0)
        return carry

    lax.fori_loop(0, TILES, coefficients, 0)

    for d in PAIR:
        scale = coef[1 + d, OWN, own_rows, :] / (jnp.maximum(nuv[d], 1.0) * float(sub_count))
        for m in PAIR:
            fstage[m, d] = scale * sums[d, m]

    def put(m, rs, pack_w, pack_e):
        fstage_w[m, rs, :] = pack_w
        fstage_e[m, rs, :] = pack_e

    pack_2d(fstage, 2, put)
    sent += exchange(lambda m: fstage.at[m], lambda m: fstage_w.at[m], lambda m: fstage_e.at[m], FX, 2, 19, frow_sem, fe_sem, fw_sem, fpk_e, fpk_w)

    def back_init(m, rs):
        return (pair,) * 4, back_finish

    def back_finish(m, rs, state):
        for d in PAIR:
            sums[d, m, :, rs, :] = state[2 + d] / jnp.maximum(nuv[d, :, rs, :], 1.0)

    def back(k, m, rs, get, state):
        x, total = list(state[:2]), list(state[2:])
        level = k.astype(F32)
        for d in PAIR:
            e, n = sol[d][k, m, :, rs, :], nuv[d, :, rs, :]
            x[d] = e + table[1, k] * jnp.where(n > level + 1.0, x[d], e * table[2, k])
            sol[d][k, m, :, rs, :] = x[d]
            total[d] = total[d] + jnp.where(n > level, x[d], 0.0)
        return (*x, *total)

    for_strips(back, back_init, reverse=True)

    def tracer_init(m, rs):
        return (pair,) * 2, lambda *a: None

    def tracers(k, m, rs, get, state):
        level = k.astype(F32)
        u, v, vs = 0.5 * get(U, k, slice(0, 3)), 0.5 * get(V, k, OWN), 0.5 * get(V, k, OWN, -1)
        out = []
        for f, e in zip((T, S), state):
            t = get(f, k, slice(0, 3))
            fx = u * (t + jnp.concatenate([east_block(t), t[:1]], axis=0))
            t = t[OWN]
            b = t - fx[OWN] + west_block(fx) - v * (t + get(f, k, OWN, 1)) + vs * (t + get(f, k, OWN, -1))
            b = jnp.where(kmt[:, rs, :] > level, b, 0.0)
            out.append((b + DIFF_NUMBER * e) * table[3, k])
            sol[f][k, m, :, rs, :] = out[-1]
        return tuple(out)

    @pl.when(has_n)
    def _():
        to_s_later.wait_recv()

    @pl.when(has_s)
    def _():
        to_n_later.wait_recv()

    lax.fori_loop(0, L // 4, unpack_rows_later, 0)
    for_strips(tracers, tracer_init, levels=TRACER_BLOCK)
    acc[...] = jnp.zeros(acc.shape, F32)

    collect(lambda m: fstage.at[m], lambda m: fstage_w.at[m], FX, 2, frow_sem, fe_sem, fw_sem, fpk_e, fpk_w)

    def subcycle(n, tiles, base):
        def tile_rows(t):
            return aligned(base + SUB * t)

        def eta_tile(t):
            rs = tile_rows(t)
            u, v = frame[TX, :, rs, :], frame[TY, :, rs, :]
            div = (u - west(u)) + (v - frame[TY, :, pl.ds(base + SUB * t - 1, SUB), :])
            eta = frame[ETA, :, rs, :] - coef[0, :, rs, :] * div
            frame[ETA, :, rs, :] = eta
            return u, v, WAVE_COURANT * eta

        last_row = iota((RING, SUB, LANES), 1) == SUB - 1
        following = eta_tile(0)
        for t in range(tiles):
            u, v, e = following
            if t + 1 < tiles:
                following = eta_tile(t + 1)
            e_n = jnp.where(last_row, pltpu.roll(following[2], SUB - 1, 1), pltpu.roll(e, SUB - 1, 1))
            rs = tile_rows(t)
            frame[TX, :, rs, :] = u + frame[FX, :, rs, :] - coef[1, :, rs, :] * (east(e) - e)
            frame[TY, :, rs, :] = v + frame[FY, :, rs, :] - coef[2, :, rs, :] * (e_n - e)
        chip_rows = aligned(FPAD + (M * ROWS - SHIFT) * chip, M * ROWS)
        acc[...] += stage[1, KMT, n // ROWS, pl.ds(lax.rem(n, ROWS), 1), :] * frame[pl.ds(0, RING), OWN, chip_rows, :]

    def subcycles(first, last, tiles, base):
        def block(b, carry):
            for j in range(SUB_BLOCK):
                subcycle(SUB_BLOCK * b + j, tiles, base)
            return carry

        lax.fori_loop(first // SUB_BLOCK, last // SUB_BLOCK, block, 0)

    turning = -(-max(sub_count - SHIFT, 0) // SUB_BLOCK) * SUB_BLOCK
    subcycles(0, turning, TILES, FPAD)
    subcycles(turning, sub_count, TILES - SHIFT // SUB, FPAD + SHIFT * chip)

    mine = aligned(ROWS * core, ROWS)
    theirs = aligned(ROWS * (1 - core), ROWS)
    result[...] = acc[:, :, theirs, :]
    swap = send(result, result_in, 30, swap_sem, row + 1 - 2 * core, col)
    swap.start()
    swap.wait_recv()
    for m in PAIR:
        whole = jnp.where(core == m, acc[:, :, mine, :], result_in[...])
        for lt in PAIR:
            ls = pl.ds(LANES * lt, LANES)
            eta_out[m, :, ls] = whole[ETA, lt]
            tx_out[m, :, ls] = whole[TX, lt]
            ty_out[m, :, ls] = whole[TY, lt]
            for d, out in enumerate((qu_out, qv_out)):
                depth = coef[1 + d, lt, own_rows, :]
                out[m, :, ls] = whole[TX + d, lt] / jnp.where(depth > 0.0, depth, 1.0) - sums[d, m, lt]
                nuv_out[d, :, ls] = nuv[d, lt]

    to_w.wait_send()
    to_e.wait_send()

    @pl.when(has_s)
    def _():
        to_s.wait_send()
        to_se.wait_send()
        to_s_later.wait_send()

    @pl.when(has_n)
    def _():
        to_n.wait_send()
        to_nw.wait_send()
        to_n_later.wait_send()

    for copy in sent:
        copy.wait_send()
    swap.wait_send()


def final_kernel(level_count, sol_u, sol_v, sol_t, sol_s, qu, qv, nuv, wet, eta_in, tx_in, ty_in, eta_out, tx_out, ty_out, u_out, v_out, t_out, s_out):
    ratio = sweep_constants(level_count, DIFF_NUMBER)[1]
    m = pl.program_id(0)
    rs = pl.ds(pl.multiple_of(pl.program_id(1) * 8, 8), 8)
    eta_out[...] = eta_in[...]
    tx_out[...] = tx_in[...]
    ty_out[...] = ty_in[...]
    for lt in PAIR:
        ls = pl.ds(LANES * lt, LANES)
        n_wet = wet[:, ls]
        for src, out in ((sol_t, t_out), (sol_s, s_out)):
            x = jnp.zeros(TILE, F32)
            for k in reversed(range(level_count)):
                e = src[k, m, lt, rs, :]
                x = e + ratio[k] * jnp.where(n_wet > k + 1, x, e * (1.0 / (1.0 - ratio[k])))
                out[k, 0, :, ls] = jnp.where(n_wet > k, x, 0.0)
        for d, (src, q, out) in enumerate(((sol_u, qu, u_out), (sol_v, qv, v_out))):
            n, mean = nuv[d, :, ls], q[0, :, ls]
            for k in range(level_count):
                out[k, 0, :, ls] = jnp.where(n > float(k), src[k, m, lt, rs, :] + mean, 0.0)


def solution(mesh):
    col_count = mesh.shape["col"]

    def local_step(vel_x, vel_y, pot_temp, salinity, surf_eta, trans_x, trans_y, col_depth, wet_levels, avg_weights):
        L = vel_x.shape[0]
        N = avg_weights.shape[0]
        hbm_spec = pl.BlockSpec(memory_space=pltpu.HBM)
        vmem_spec = pl.BlockSpec(memory_space=pltpu.VMEM)
        cube = jax.ShapeDtypeStruct(vel_x.shape, F32)
        flat = jax.ShapeDtypeStruct(surf_eta.shape, F32)
        vm = lambda *shape: pltpu.VMEM(shape, F32)
        dma = lambda n: pltpu.SemaphoreType.DMA((n,))
        stage = pl.pallas_call(
            functools.partial(stage_kernel, N),
            out_shape=jax.ShapeDtypeStruct((M, 6, M, ROWS, LANES), F32),
            in_specs=[vmem_spec] * 5 + [pl.BlockSpec(memory_space=pltpu.SMEM)],
            out_specs=vmem_spec,
            name="ocean_stage",
        )(surf_eta, trans_x, trans_y, col_depth, wet_levels, avg_weights)
        *sol, qu, qv, nuv, eta_o, tx_o, ty_o = pl.pallas_call(
            functools.partial(step_kernel, col_count, L, N),
            out_shape=[jax.ShapeDtypeStruct((L, M, M, ROWS, LANES), F32)] * 4 + [flat] * 6,
            in_specs=[hbm_spec] * 4 + [vmem_spec],
            out_specs=[vmem_spec] * 10,
            scratch_shapes=[
                vm(4, L, M, RING, XR, LANES), *[vm(4, M, 8, LANES)] * 4, vm(5, M, M * L + 8, LANES), vm(4, M, M * L, LANES), vm(5, M, M * L + 8, LANES), vm(4, M, M * L, LANES),
                *[vm(M, 8, LANES)] * 2, vm(M, ROWS + 8, LANES), vm(M, M, ROWS, LANES), vm(M, M, M, ROWS, LANES),
                *[vm(4, ROWS, LANES)] * M,
                vm(M, M, M, ROWS, LANES), *[vm(M, ROWS, LANES)] * M, *[vm(4, ROWS, LANES)] * M,
                vm(6, RING, FRAME, LANES), vm(RING, RING, FRAME, LANES), vm(RING, M, M * ROWS, LANES), *[vm(RING, M, ROWS, LANES)] * M,
                pltpu.SMEM((4, L), F32), dma(8), dma(31), dma(8), *[dma(4)] * 6, pltpu.SemaphoreType.DMA],
            compiler_params=pltpu.CompilerParams(collective_id=0, has_side_effects=True, vmem_limit_bytes=STEP_VMEM),
            name="ocean_step",
        )(vel_x, vel_y, pot_temp, salinity, stage)
        cube_spec = pl.BlockSpec((L, 1, 8, 256), lambda m, i: (0, m, i, 0))
        flat_spec = pl.BlockSpec((1, 8, 256), lambda m, i: (m, i, 0))
        outs = pl.pallas_call(
            functools.partial(final_kernel, L),
            grid=(2, 3),
            out_shape=[flat] * 3 + [cube] * 4,
            in_specs=[vmem_spec] * 4 + [flat_spec] * 2
            + [pl.BlockSpec((2, 8, 256), lambda m, i: (0, i, 0)), pl.BlockSpec((8, 256), lambda m, i: (i, 0))] + [flat_spec] * 3,
            out_specs=[flat_spec] * 3 + [cube_spec] * 4,
            name="ocean_final",
            compiler_params=pltpu.CompilerParams(vmem_limit_bytes=FINAL_VMEM),
        )(*sol, qu, qv, nuv, wet_levels, eta_o, tx_o, ty_o)
        return tuple(outs)

    spec_3d = P(None, None, "row", "col")
    spec_2d = P(None, "row", "col")
    spec_map = P("row", "col")
    return jax.shard_map(local_step, mesh=mesh, in_specs=(spec_3d,) * 4 + (spec_2d,) * 3 + (spec_map,) * 2 + (P(),),
                         out_specs=(spec_2d,) * 3 + (spec_3d,) * 4, check_vma=False)
```

```python
import functools

import jax
import jax.numpy as jnp
from jax import lax
from jax.experimental import pallas as pl
from jax.experimental.pallas import tpu as pltpu
from jax.sharding import PartitionSpec as P

WAVE_COURANT = 0.4
THERM_EXP = 0.2
HALINE_CON = 0.15
PRESS_SCALE = 0.5
VISC_NUMBER = 1.0
DIFF_NUMBER = 0.5

MESH = pl.DeviceIdType.MESH
F32 = jnp.float32
ROWS = 24
PAD = 8
XR = ROWS + 2 * PAD
EDGE_BLOCK = 12
TRACER_BLOCK = 12
SUB_BLOCK = 3
LEVEL_BLOCK = 12
LANES = 128
SUB = 8
TILE = (SUB, LANES)
PAIR, STRIPS, QUAD, OCTET = range(2), range(3), range(4), range(SUB)
RING = 3
M = 2
TILES = 10
SHIFT = 16
FPAD = SHIFT + PAD
FRAME = 4 * ROWS + 2 * FPAD
HALO = 32


def sweep_constants(level_count, strength):
    inverse, ratio = [], []
    for k in range(level_count):
        pivot = 1.0 + strength if k == 0 else 1.0 + 2.0 * strength - strength * ratio[-1]
        inverse.append(1.0 / pivot)
        ratio.append(strength / pivot)
    return inverse, ratio


def iota(shape, axis):
    return lax.broadcasted_iota(jnp.int32, shape, axis)


def lanes(*lead):
    return iota((*lead, 8, 128), len(lead) + 1)


def turn(x, shift):
    return pltpu.roll(x, shift, x.ndim - 1)


def east(x):
    rolled = turn(x, 127)
    return jnp.where(lanes(3) == 127, jnp.concatenate([rolled[1:], rolled[:1]], axis=0), rolled)


def west(x):
    rolled = turn(x, 1)
    return jnp.where(lanes(3) == 0, jnp.concatenate([rolled[2:], rolled[:2]], axis=0), rolled)


def east_block(x):
    rolled = turn(x[:2], 127)
    return jnp.where(lanes(2) == 127, jnp.concatenate([rolled[1:], x[2:]], axis=0), rolled)


def west_block(x):
    rolled = turn(x[:2], 1)
    return jnp.where(lanes(2) == 0, jnp.concatenate([x[2:], rolled[:1]], axis=0), rolled)


ETA, TX, TY, DEPTH, PACK, KMT = range(6)


def pack_2d(stage, count, put):
    lane = lanes()
    for i in STRIPS:
        rs = pl.ds(SUB * i, SUB)
        for m in PAIR:
            pack_w = pack_e = jnp.zeros(TILE, F32)
            for j in range(count):
                here = lane // HALO == j
                pack_w = jnp.where(here, turn(stage[m, j, 0, rs, :], HALO * j), pack_w)
                pack_e = jnp.where(here, turn(stage[m, j, 1, rs, :], (HALO * j + HALO) % LANES), pack_e)
            put(m, rs, pack_w, pack_e)


def stage_planes(sub_count, eta, tx, ty, depth, wet_in, weights, stage):
    for lt in PAIR:
        ls = pl.ds(LANES * lt, LANES)
        wet = wet_in[:, ls].astype(F32)
        masked = jnp.where(wet > 0.0, depth[:, ls], 0.0)
        stage[0, KMT, lt] = wet
        for m in PAIR:
            for j, field in ((ETA, eta), (TX, tx), (TY, ty)):
                stage[m, j, lt] = field[m, :, ls]
            stage[m, DEPTH, lt] = masked
    for n in range(sub_count):
        stage[1, KMT, n // ROWS, pl.ds(n % ROWS, 1), :] = jnp.full((1, LANES), weights[n], F32)

    def put(m, rs, pack_w, pack_e):
        stage[m, PACK, 0, rs, :] = pack_w
        stage[m, PACK, 1, rs, :] = pack_e

    pack_2d(stage, 4, put)


def step_kernel(
    col_count, level_count, sub_count,
    u_hbm, v_hbm, t_hbm, s_hbm, eta_hbm, tx_hbm, ty_hbm, depth_hbm, wet_hbm, weights,
    xu_hbm, xv_hbm, ct_hbm, cs_hbm, qu_out, qv_out, nuv_out, eta_out, tx_out, ty_out,
    cube, sol_u, sol_v, sol_t, sol_s, eta_in, tx_in, ty_in, depth_in, wet_in, stage,
    col_w, col_e, rcv_e, rcv_w, row_s, row_n, rcv_n, rcv_s, rcv_se, rcv_nw,
    kmt, nuv, sums, pk_e, pk_w, fstage, fstage_w, fstage_e, fpk_e, fpk_w,
    frame, coef, acc, result, result_in,
    table, load_sem, small_sem, store_sem, send_sem, edge_sem, row_sem, e_sem, w_sem, frow_sem, fe_sem, fw_sem, swap_sem,
):
    L = level_count
    U, V, T, S = range(4)
    sol = (sol_u, sol_v, sol_t, sol_s)
    FX, FY = 4, 5
    OWN = slice(0, 2)
    col = lax.axis_index("col")
    row = lax.axis_index("row")
    chip = row // 2
    core = row % 2
    east_col = lax.rem(col + 1, col_count)
    west_col = lax.rem(col + col_count - 1, col_count)
    peers = [lax.rem(row + d, 4) for d in (1, 2, 3)]
    lane = lanes()
    zero = jnp.zeros(TILE, F32)

    def aligned(start, size=8):
        return pl.ds(pl.multiple_of(start, 8), size)

    barrier = pltpu.get_barrier_semaphore()
    for r in peers:
        pl.semaphore_signal(barrier, inc=1, device_id={"row": r, "col": col}, device_id_type=MESH)
    for other in (east_col, west_col):
        for r in QUAD:
            pl.semaphore_signal(barrier, inc=1, device_id={"row": r, "col": other}, device_id_type=MESH)

    loads = []
    for f, src in enumerate((u_hbm, v_hbm, t_hbm, s_hbm)):
        for lt in PAIR:
            loads.append(pltpu.make_async_copy(
                src.at[:, :, :, pl.ds(LANES * lt, LANES)], cube.at[f, :, :, lt, pl.ds(PAD, ROWS), :], load_sem.at[2 * f + lt]))
            loads[-1].start()

    inv_v, ratio_v = sweep_constants(L, VISC_NUMBER)
    for n, line in enumerate((inv_v, ratio_v, [1.0 / (1.0 - r) for r in ratio_v], sweep_constants(L, DIFF_NUMBER)[0])):
        for k in range(L):
            table[n, k] = line[k]

    smalls = []
    for n, (src, dst) in enumerate(((wet_hbm, wet_in), (eta_hbm, eta_in), (tx_hbm, tx_in), (ty_hbm, ty_in), (depth_hbm, depth_in))):
        smalls.append(pltpu.make_async_copy(src, dst, small_sem.at[n]))
        smalls[-1].start()

    has_s, has_n = row > 0, row < 3

    @pl.when(row == 0)
    def _():
        rcv_s[...] = jnp.zeros(rcv_s.shape, F32)
        rcv_se[...] = jnp.zeros(rcv_se.shape, F32)

    @pl.when(row == 3)
    def _():
        rcv_n[...] = jnp.zeros(rcv_n.shape, F32)
        rcv_nw[...] = jnp.zeros(rcv_nw.shape, F32)

    outside = jnp.zeros((6, RING, PAD, LANES), F32)

    @pl.when(chip == 0)
    def _():
        frame[:, :, pl.ds(FPAD - PAD, PAD), :] = outside

    @pl.when(chip == 1)
    def _():
        frame[:, :, pl.ds(FPAD + SUB * TILES, PAD), :] = outside


    lane42 = lanes(4, 2)
    lane2 = lanes(M)
    empty = jnp.zeros((M, SUB, LANES), F32)
    for f in QUAD:
        for copy in loads[2 * f:2 * f + 2]:
            copy.wait()

        def pack(g, carry):
            west_pack, east_pack = carry
            for k, i in [(EDGE_BLOCK * g + j, i) for j in range(EDGE_BLOCK) for i in STRIPS]:
                slot = L * i + k
                rs = pl.ds(PAD + SUB * i, SUB)
                west_pack = jnp.where(lane2 == slot, turn(cube[f, k, :, 0, rs, :], slot), west_pack)
                east_pack = jnp.where(lane2 == slot, turn(cube[f, k, :, 1, rs, :], slot + 1), east_pack)
            for q in range(M * EDGE_BLOCK // SUB):
                rows = aligned(M * EDGE_BLOCK * g + SUB * q)
                low = high = empty
                for j in OCTET:
                    k, m = EDGE_BLOCK * g + (SUB * q + j) // M, j % M
                    low = jnp.where(sub2 == j, cube[f, k, m, OWN, pl.ds(PAD - j, SUB), :], low)
                    high = jnp.where(sub2 == j, cube[f, k, m, OWN, pl.ds(PAD + ROWS - 1 - j, SUB), :], high)
                row_n[f, :, rows, :] = high
                row_s[f if f < T else f + 1, :, rows, :] = low
                if f == S:
                    row_s[T, :, rows, :] = row_s[T + 1, :, rows, :] - (HALINE_CON / THERM_EXP) * low
            return west_pack, east_pack

        sub2 = iota((M, SUB, LANES), 1)
        col_w[f], col_e[f] = lax.fori_loop(0, L // EDGE_BLOCK, pack, (empty, empty))
    smalls[0].wait()
    for lt in PAIR:
        kmt[lt, pl.ds(0, ROWS), :] = wet_in[:, pl.ds(LANES * lt, LANES)].astype(F32)
    for i in STRIPS:
        slot = 3 * L + i
        col_w[0, 0] = jnp.where(lane == slot, turn(kmt[0, pl.ds(SUB * i, SUB), :], slot), col_w[0, 0])
    row_s[U, :, pl.ds(M * L, SUB), :] = kmt[:, pl.ds(0, SUB), :]

    pl.semaphore_wait(barrier, 11)

    def send(src, dst, ssem, rsem, r, c):
        return pltpu.make_async_remote_copy(
            src_ref=src, dst_ref=dst, send_sem=send_sem.at[ssem], recv_sem=rsem, device_id={"row": r, "col": c}, device_id_type=MESH)

    def frame_rows(r, at_chip):
        return aligned(FPAD + ROWS * r - SHIFT * at_chip, ROWS)

    own_rows = frame_rows(row, chip)
    south, north = jnp.maximum(row - 1, 0), jnp.minimum(row + 1, 3)
    to_w = send(col_w, rcv_e, 0, edge_sem.at[0], row, west_col)
    to_e = send(col_e, rcv_w, 1, edge_sem.at[1], row, east_col)
    first_s, first_n = pl.ds(0, 3), pl.ds(0, 2)
    later_s, later_n = pl.ds(3, 2), pl.ds(2, 2)
    to_s = send(row_s.at[first_s], rcv_n.at[first_s], 2, edge_sem.at[2], south, col)
    to_n = send(row_n.at[first_n], rcv_s.at[first_n], 3, edge_sem.at[3], north, col)
    to_s_later = send(row_s.at[later_s], rcv_n.at[later_s], 6, edge_sem.at[6], south, col)
    to_n_later = send(row_n.at[later_n], rcv_s.at[later_n], 7, edge_sem.at[7], north, col)
    to_nw = send(col_w.at[V], rcv_se, 4, edge_sem.at[4], north, west_col)
    to_se = send(col_e.at[U], rcv_nw, 5, edge_sem.at[5], south, east_col)
    to_w.start()
    to_e.start()

    @pl.when(has_s)
    def _():
        to_s.start()
        to_se.start()
        to_s_later.start()

    @pl.when(has_n)
    def _():
        to_n.start()
        to_nw.start()
        to_n_later.start()

    def exchange(block, pack_w, pack_e, first, count, base, rsem, esem, wsem, pe, pw):
        out = []
        for d, r in enumerate(peers):
            out.append(send(block(r % 2), frame.at[pl.ds(first, count), OWN, frame_rows(row, r // 2), :], base + d, rsem.at[row], r, col))
        for r in QUAD:
            out.append(send(pack_w(r % 2), pe.at[row], base + 3 + 2 * r, esem.at[row], r, west_col))
            out.append(send(pack_e(r % 2), pw.at[row], base + 4 + 2 * r, wsem.at[row], r, east_col))
        for copy in out:
            copy.start()
        frame[pl.ds(first, count), OWN, own_rows, :] = block(core)[...]
        return out

    def collect(block, pack_w, first, count, rsem, esem, wsem, pe, pw):
        for r in peers:
            rows = frame_rows(r, chip)
            send(block(0), frame.at[pl.ds(first, count), OWN, rows, :], 0, rsem.at[r], r, col).wait_recv()
        for r in QUAD:
            send(pack_w(0), pe.at[r], 0, esem.at[r], r, east_col).wait_recv()
            send(pack_w(0), pw.at[r], 0, wsem.at[r], r, west_col).wait_recv()
        side = lax.broadcasted_iota(jnp.int32, (ROWS, 128), 1) // HALO
        for r in QUAD:
            for j in range(count):
                frame[first + j, 2, frame_rows(r, chip), :] = jnp.where(
                    side == 0, turn(pe[r], (128 - HALO * j) % 128), jnp.where(side == 3, turn(pw[r], (128 - HALO * j - HALO) % 128), 0.0))

    def stage_block(m):
        return stage.at[m, pl.ds(0, PACK)]

    def stage_w(m):
        return stage.at[m, PACK, 0]

    def stage_e(m):
        return stage.at[m, PACK, 1]

    for copy in smalls[1:]:
        copy.wait()
    stage_planes(sub_count, eta_in, tx_in, ty_in, depth_in, wet_in, weights, stage)

    to_w.wait_recv()
    to_e.wait_recv()

    def unpack(g, carry):
        from_e, from_w = rcv_e[...], rcv_w[...]
        for k in [EDGE_BLOCK * g + j for j in range(EDGE_BLOCK)]:
            for i in STRIPS:
                slot = L * i + k
                cube[:, k, :, 2, pl.ds(PAD + SUB * i, SUB), :] = jnp.where(
                    lane42 < 64, turn(from_w, lax.rem(128 - slot, 128)), turn(from_e, 127 - slot))
        return carry

    lax.fori_loop(0, L // EDGE_BLOCK, unpack, 0)

    def masks(i):
        rs = pl.ds(SUB * i, SUB)
        wet = kmt[:, rs, :]
        halo = turn(rcv_e[0, 0], 127 - (3 * L + i))
        nuv[0, :, rs, :] = jnp.minimum(wet, east_block(jnp.concatenate([wet, halo[None]], axis=0)))
        nuv[1, :, rs, :] = jnp.minimum(wet, kmt[:, pl.ds(8 * i + 1, 8), :])

    masks(0)
    masks(1)

    press = PRESS_SCALE / L
    pair = jnp.zeros((M, SUB, LANES), F32)

    def for_strips(body, init, reverse=False, strips=(0, 1, 3), levels=LEVEL_BLOCK):
        start, step, count = strips

        def strip(s, carry):
            m = s // count
            i = start + step * (s - count * m)
            rs = aligned(SUB * i)

            def get(f, k, part, d=0):
                start = PAD + 8 * i + d
                return cube[f, k, m, part, pl.ds(start if d else pl.multiple_of(start, 8), 8), :]

            state, finish = init(m, rs)

            def block(b, state):
                for j in range(levels):
                    k = b * levels + j
                    state = body(L - 1 - k if reverse else k, m, rs, get, state)
                return state

            finish(m, rs, lax.fori_loop(0, L // levels, block, state))
            return carry

        lax.fori_loop(0, M * count, strip, 0)

    def momentum_init(m, rs):
        return (pair,) * 6, momentum_finish

    def momentum_finish(m, rs, state):
        sums[0, m, :, rs, :] = state[4]
        sums[1, m, :, rs, :] = state[5]

    def momentum(k, m, rs, get, state):
        cx, cy, eu, ev, gu_sum, gv_sum = state
        level = k.astype(F32)
        both = slice(0, 3)
        u, v, un, vs = get(U, k, both), get(V, k, both), get(U, k, both, 1), get(V, k, both, -1)
        rho = HALINE_CON * get(S, k, both) - THERM_EXP * get(T, k, both)
        dx = rho[OWN] - east_block(rho)
        dy = rho[OWN] - (HALINE_CON * get(S, k, OWN, 1) - THERM_EXP * get(T, k, OWN, 1))
        vsum, usum = v + vs, u + un
        cx, cy = cx + dx, cy + dy
        gu = press * (cx - 0.5 * dx) - 0.5 * (u[OWN] * (east_block(u) - west_block(u))) - 0.125 * (
            (vsum[OWN] + east_block(vsum)) * (un[OWN] - get(U, k, OWN, -1)))
        gv = press * (cy - 0.5 * dy) - 0.125 * ((usum[OWN] + west_block(usum)) * (east_block(v) - west_block(v))) - 0.5 * (
            v[OWN] * (get(V, k, OWN, 1) - vs[OWN]))
        gu = jnp.where(nuv[0, :, rs, :] > level, gu, 0.0)
        gv = jnp.where(nuv[1, :, rs, :] > level, gv, 0.0)
        inverse = table[0, k]
        eu = (u[OWN] + gu + VISC_NUMBER * eu) * inverse
        ev = (v[OWN] + gv + VISC_NUMBER * ev) * inverse
        sol[U][k, m, :, rs, :] = eu
        sol[V][k, m, :, rs, :] = ev
        return cx, cy, eu, ev, gu_sum + gu, gv_sum + gv

    for_strips(momentum, momentum_init, strips=(1, 1, 1))

    @pl.when(has_n)
    def _():
        to_s.wait_recv()
        to_se.wait_recv()

    @pl.when(has_s)
    def _():
        to_n.wait_recv()
        to_nw.wait_recv()

    sent = exchange(stage_block, stage_w, stage_e, ETA, 4, 8, row_sem, e_sem, w_sem, pk_e, pk_w)

    def unpack_rows(g, carry):
        rows = aligned(SUB * g)
        below, above = rcv_s[:T, :, rows, :], rcv_n[:S, :, rows, :]
        for j in OCTET:
            k, m = 4 * g + j // 2, j % 2
            cube[:T, k, m, OWN, pl.ds(PAD - 1, 1), :] = below[:, :, j:j + 1, :]
            cube[:S, k, m, OWN, pl.ds(PAD + ROWS, 1), :] = above[:, :, j:j + 1, :]
            cube[S, k, m, OWN, pl.ds(PAD + ROWS, 1), :] = jnp.zeros((M, 1, LANES), F32)
            if m:
                cube[V, k, :, 2, pl.ds(0, PAD), :] = turn(rcv_se[...], 127 - 2 * L - k)
                cube[U, k, :, 2, pl.ds(PAD + ROWS, PAD), :] = turn(rcv_nw[...], lax.rem(128 - k, 128))
        return carry

    def unpack_rows_later(g, carry):
        rows = aligned(SUB * g)
        below, above = rcv_s[T:, :, rows, :], rcv_n[S:, :, rows, :]
        for j in OCTET:
            k, m = 4 * g + j // 2, j % 2
            cube[T:, k, m, OWN, pl.ds(PAD - 1, 1), :] = below[:, :, j:j + 1, :]
            cube[T:, k, m, OWN, pl.ds(PAD + ROWS, 1), :] = above[:, :, j:j + 1, :]
        return carry

    lax.fori_loop(0, L // 4, unpack_rows, 0)
    kmt[:, pl.ds(ROWS, 8), :] = rcv_n[U, :, pl.ds(M * L, SUB), :]
    masks(2)
    for_strips(momentum, momentum_init, strips=(0, 2, 2))

    collect(stage_block, stage_w, ETA, 4, row_sem, e_sem, w_sem, pk_e, pk_w)

    def coefficients(i, carry):
        rs = aligned(FPAD + SUB * i)
        depth = frame[DEPTH, :, rs, :]
        depth_e = east(depth)
        depth_n = frame[DEPTH, :, pl.ds(FPAD + SUB * i + 1, SUB), :]
        wet = depth > 0.0
        coef[0, :, rs, :] = jnp.where(wet, WAVE_COURANT, 0.0)
        coef[1, :, rs, :] = jnp.where(wet & (depth_e > 0.0), 0.5 * (depth + depth_e), 0.0)
        coef[2, :, rs, :] = jnp.where(wet & (depth_n > 0.0), 0.5 * (depth + depth_n), 0.0)
        return carry

    lax.fori_loop(0, TILES, coefficients, 0)

    for d in PAIR:
        scale = coef[1 + d, OWN, own_rows, :] / (jnp.maximum(nuv[d], 1.0) * float(sub_count))
        for m in PAIR:
            fstage[m, d] = scale * sums[d, m]

    def put(m, rs, pack_w, pack_e):
        fstage_w[m, rs, :] = pack_w
        fstage_e[m, rs, :] = pack_e

    pack_2d(fstage, 2, put)
    sent += exchange(lambda m: fstage.at[m], lambda m: fstage_w.at[m], lambda m: fstage_e.at[m], FX, 2, 19, frow_sem, fe_sem, fw_sem, fpk_e, fpk_w)

    def back_init(m, rs):
        return (pair,) * 4, back_finish

    def back_finish(m, rs, state):
        for d in PAIR:
            sums[d, m, :, rs, :] = state[2 + d] / jnp.maximum(nuv[d, :, rs, :], 1.0)

    def back(k, m, rs, get, state):
        x, total = list(state[:2]), list(state[2:])
        level = k.astype(F32)
        for d in PAIR:
            e, n = sol[d][k, m, :, rs, :], nuv[d, :, rs, :]
            x[d] = e + table[1, k] * jnp.where(n > level + 1.0, x[d], e * table[2, k])
            sol[d][k, m, :, rs, :] = x[d]
            total[d] = total[d] + jnp.where(n > level, x[d], 0.0)
        return (*x, *total)

    for_strips(back, back_init, reverse=True)
    stores = []

    def store(f, dst):
        for lt in PAIR:
            stores.append(pltpu.make_async_copy(
                sol[f].at[:, :, lt], dst.at[:, :, :, pl.ds(LANES * lt, LANES)], store_sem.at[2 * f + lt]))
            stores[-1].start()

    store(U, xu_hbm)
    store(V, xv_hbm)

    def tracer_init(m, rs):
        return (pair,) * 2, lambda *a: None

    def tracers(k, m, rs, get, state):
        level = k.astype(F32)
        u, v, vs = 0.5 * get(U, k, slice(0, 3)), 0.5 * get(V, k, OWN), 0.5 * get(V, k, OWN, -1)
        out = []
        for f, e in zip((T, S), state):
            t = get(f, k, slice(0, 3))
            fx = u * (t + jnp.concatenate([east_block(t), t[:1]], axis=0))
            t = t[OWN]
            b = t - fx[OWN] + west_block(fx) - v * (t + get(f, k, OWN, 1)) + vs * (t + get(f, k, OWN, -1))
            b = jnp.where(kmt[:, rs, :] > level, b, 0.0)
            out.append((b + DIFF_NUMBER * e) * table[3, k])
            sol[f][k, m, :, rs, :] = out[-1]
        return tuple(out)

    @pl.when(has_n)
    def _():
        to_s_later.wait_recv()

    @pl.when(has_s)
    def _():
        to_n_later.wait_recv()

    lax.fori_loop(0, L // 4, unpack_rows_later, 0)
    for_strips(tracers, tracer_init, levels=TRACER_BLOCK)
    store(T, ct_hbm)
    store(S, cs_hbm)
    acc[...] = jnp.zeros(acc.shape, F32)

    collect(lambda m: fstage.at[m], lambda m: fstage_w.at[m], FX, 2, frow_sem, fe_sem, fw_sem, fpk_e, fpk_w)

    def subcycle(n, tiles, base):
        def tile_rows(t):
            return aligned(base + SUB * t)

        def eta_tile(t):
            rs = tile_rows(t)
            u, v = frame[TX, :, rs, :], frame[TY, :, rs, :]
            div = (u - west(u)) + (v - frame[TY, :, pl.ds(base + SUB * t - 1, SUB), :])
            eta = frame[ETA, :, rs, :] - coef[0, :, rs, :] * div
            frame[ETA, :, rs, :] = eta
            return u, v, WAVE_COURANT * eta

        last_row = iota((RING, SUB, LANES), 1) == SUB - 1
        following = eta_tile(0)
        for t in range(tiles):
            u, v, e = following
            if t + 1 < tiles:
                following = eta_tile(t + 1)
            e_n = jnp.where(last_row, pltpu.roll(following[2], SUB - 1, 1), pltpu.roll(e, SUB - 1, 1))
            rs = tile_rows(t)
            frame[TX, :, rs, :] = u + frame[FX, :, rs, :] - coef[1, :, rs, :] * (east(e) - e)
            frame[TY, :, rs, :] = v + frame[FY, :, rs, :] - coef[2, :, rs, :] * (e_n - e)
        chip_rows = aligned(FPAD + (M * ROWS - SHIFT) * chip, M * ROWS)
        acc[...] += stage[1, KMT, n // ROWS, pl.ds(lax.rem(n, ROWS), 1), :] * frame[pl.ds(0, RING), OWN, chip_rows, :]

    def subcycles(first, last, tiles, base):
        def block(b, carry):
            for j in range(SUB_BLOCK):
                subcycle(SUB_BLOCK * b + j, tiles, base)
            return carry

        lax.fori_loop(first // SUB_BLOCK, last // SUB_BLOCK, block, 0)

    turning = -(-max(sub_count - SHIFT, 0) // SUB_BLOCK) * SUB_BLOCK
    subcycles(0, turning, TILES, FPAD)
    subcycles(turning, sub_count, TILES - SHIFT // SUB, FPAD + SHIFT * chip)

    mine = aligned(ROWS * core, ROWS)
    theirs = aligned(ROWS * (1 - core), ROWS)
    result[...] = acc[:, :, theirs, :]
    swap = send(result, result_in, 30, swap_sem, row + 1 - 2 * core, col)
    swap.start()
    swap.wait_recv()
    for m in PAIR:
        whole = jnp.where(core == m, acc[:, :, mine, :], result_in[...])
        for lt in PAIR:
            ls = pl.ds(LANES * lt, LANES)
            eta_out[m, :, ls] = whole[ETA, lt]
            tx_out[m, :, ls] = whole[TX, lt]
            ty_out[m, :, ls] = whole[TY, lt]
            for d, out in enumerate((qu_out, qv_out)):
                depth = coef[1 + d, lt, own_rows, :]
                out[m, :, ls] = whole[TX + d, lt] / jnp.where(depth > 0.0, depth, 1.0) - sums[d, m, lt]
                nuv_out[d, :, ls] = nuv[d, lt]

    for copy in stores:
        copy.wait()
    to_w.wait_send()
    to_e.wait_send()

    @pl.when(has_s)
    def _():
        to_s.wait_send()
        to_se.wait_send()
        to_s_later.wait_send()

    @pl.when(has_n)
    def _():
        to_n.wait_send()
        to_nw.wait_send()
        to_n_later.wait_send()

    for copy in sent:
        copy.wait_send()
    swap.wait_send()


def final_kernel(level_count, xu, xv, ct, cs, qu, qv, nuv, wet, eta_in, tx_in, ty_in,
                 eta_out, tx_out, ty_out, u_out, v_out, t_out, s_out,
                 cubes, planes, wet_v, cube_in, cube_out, plane_in, plane_out):
    ratio = sweep_constants(level_count, DIFF_NUMBER)[1]
    strips = M * len(STRIPS)

    def block(array, s):
        m = s // 3
        return array.at[:, m, pl.ds(pl.multiple_of(SUB * (s - 3 * m), SUB), SUB), :]

    def reads(s):
        return [pltpu.make_async_copy(block(src, s), cubes.at[f, s], cube_in.at[f, s]) for f, src in enumerate((ct, cs, xu, xv))]

    def writes(s):
        return [pltpu.make_async_copy(cubes.at[f, s], block(dst, s), cube_out.at[f, s]) for f, dst in enumerate((t_out, s_out, u_out, v_out))]

    small = [pltpu.make_async_copy(src, planes.at[n], plane_in.at[n]) for n, src in enumerate((qu, qv, nuv, eta_in, tx_in, ty_in))]
    small.append(pltpu.make_async_copy(wet, wet_v, plane_in.at[6]))
    passed = [pltpu.make_async_copy(planes.at[3 + n], dst, plane_out.at[n]) for n, dst in enumerate((eta_out, tx_out, ty_out))]

    def start(s, carry):
        for copy in reads(s):
            copy.start()
        return carry

    for copy in reads(0) + small:
        copy.start()
    lax.fori_loop(1, strips, start, 0)
    for copy in small:
        copy.wait()
    for copy in passed:
        copy.start()

    def strip(s, carry):
        m = s // 3
        rs = pl.ds(pl.multiple_of(SUB * (s - 3 * m), SUB), SUB)
        done = writes(s)
        for f, copy in enumerate(reads(s)):
            copy.wait()
            for lt in PAIR:
                ls = pl.ds(LANES * lt, LANES)
                if f < M:
                    n_wet = wet_v[rs, ls]
                    x = jnp.zeros(TILE, F32)
                    for k in reversed(range(level_count)):
                        e = cubes[f, s, k, :, ls]
                        x = e + ratio[k] * jnp.where(n_wet > k + 1, x, e * (1.0 / (1.0 - ratio[k])))
                        cubes[f, s, k, :, ls] = jnp.where(n_wet > k, x, 0.0)
                else:
                    n, mean = planes[2, f - M, rs, ls], planes[f - M, m, rs, ls]
                    for k in range(level_count):
                        cubes[f, s, k, :, ls] = jnp.where(n > float(k), cubes[f, s, k, :, ls] + mean, 0.0)
            done[f].start()
        return carry

    def finish(s, carry):
        for copy in writes(s):
            copy.wait()
        return carry

    lax.fori_loop(0, strips, strip, 0)
    lax.fori_loop(0, strips, finish, 0)
    for copy in passed:
        copy.wait()


def solution(mesh):
    col_count = mesh.shape["col"]

    def local_step(vel_x, vel_y, pot_temp, salinity, surf_eta, trans_x, trans_y, col_depth, wet_levels, avg_weights):
        L = vel_x.shape[0]
        N = avg_weights.shape[0]
        hbm_spec = pl.BlockSpec(memory_space=pltpu.HBM)
        vmem_spec = pl.BlockSpec(memory_space=pltpu.VMEM)
        cube = jax.ShapeDtypeStruct(vel_x.shape, F32)
        flat = jax.ShapeDtypeStruct(surf_eta.shape, F32)
        vm = lambda *shape: pltpu.VMEM(shape, F32)
        dma = lambda n: pltpu.SemaphoreType.DMA((n,))
        outs = pl.pallas_call(
            functools.partial(step_kernel, col_count, L, N),
            out_shape=[cube] * 4 + [flat] * 6,
            in_specs=[hbm_spec] * 9 + [pl.BlockSpec(memory_space=pltpu.SMEM)],
            out_specs=[hbm_spec] * 4 + [vmem_spec] * 6,
            scratch_shapes=[
                vm(4, L, M, RING, XR, LANES), *[vm(L, M, M, ROWS, LANES)] * 4, *[vm(M, ROWS, 256)] * 3, vm(ROWS, 256),
                pltpu.VMEM((ROWS, 256), jnp.int32), vm(M, 6, M, ROWS, LANES),
*[vm(4, M, 8, LANES)] * 4, vm(5, M, M * L + 8, LANES), vm(4, M, M * L, LANES), vm(5, M, M * L + 8, LANES), vm(4, M, M * L, LANES),
                *[vm(M, 8, LANES)] * 2, vm(M, ROWS + 8, LANES), vm(M, M, ROWS, LANES), vm(M, M, M, ROWS, LANES),
                *[vm(4, ROWS, LANES)] * M,
                vm(M, M, M, ROWS, LANES), *[vm(M, ROWS, LANES)] * M, *[vm(4, ROWS, LANES)] * M,
                vm(6, RING, FRAME, LANES), vm(RING, RING, FRAME, LANES), vm(RING, M, M * ROWS, LANES), *[vm(RING, M, ROWS, LANES)] * M,
                pltpu.SMEM((4, L), F32), dma(8), dma(5), dma(8), dma(31), dma(8), *[dma(4)] * 6, pltpu.SemaphoreType.DMA],
            compiler_params=pltpu.CompilerParams(collective_id=0, has_side_effects=True),
            name="ocean_step",
        )(vel_x, vel_y, pot_temp, salinity, surf_eta, trans_x, trans_y, col_depth, wet_levels, avg_weights)
        strips = M * len(STRIPS)
        outs = pl.pallas_call(
            functools.partial(final_kernel, L),
            out_shape=[flat] * 3 + [cube] * 4,
            in_specs=[hbm_spec] * 11,
            out_specs=[hbm_spec] * 7,
            scratch_shapes=[vm(4, strips, L, SUB, 256), vm(6, M, ROWS, 256), pltpu.VMEM((ROWS, 256), jnp.int32),
                            pltpu.SemaphoreType.DMA((4, strips)), pltpu.SemaphoreType.DMA((4, strips)), dma(7), dma(3)],
            name="ocean_final",
        )(*outs[:7], wet_levels, *outs[7:])
        return tuple(outs)

    spec_3d = P(None, None, "row", "col")
    spec_2d = P(None, "row", "col")
    spec_map = P("row", "col")
    return jax.shard_map(local_step, mesh=mesh, in_specs=(spec_3d,) * 4 + (spec_2d,) * 3 + (spec_map,) * 2 + (P(),),
                         out_specs=(spec_2d,) * 3 + (spec_3d,) * 4, check_vma=False)
```

```python
import functools

import jax
import jax.numpy as jnp
from jax import lax
from jax.experimental import pallas as pl
from jax.experimental.pallas import tpu as pltpu
from jax.sharding import PartitionSpec as P

WAVE_COURANT = 0.4
THERM_EXP = 0.2
HALINE_CON = 0.15
PRESS_SCALE = 0.5
VISC_NUMBER = 1.0
DIFF_NUMBER = 0.5

MESH = pl.DeviceIdType.MESH
F32 = jnp.float32
ROWS = 24
PAD = 8
XR = ROWS + 2 * PAD
EDGE_BLOCK = 12
TRACER_BLOCK = 12
BACK_BLOCK = 6
SUB_BLOCK = 3
LEVEL_BLOCK = 12
LANES = 128
SUB = 8
TILE = (SUB, LANES)
PAIR, STRIPS, QUAD, OCTET = range(2), range(3), range(4), range(SUB)
RING = 3
M = 2
STEP_VMEM, FINAL_VMEM = 46 << 20, 9 << 20
TILES = 10
SHIFT = 16
FPAD = SHIFT + PAD
FRAME = 4 * ROWS + 2 * FPAD
HALO = 32


def sweep_constants(level_count, strength):
    inverse, ratio = [], []
    for k in range(level_count):
        pivot = 1.0 + strength if k == 0 else 1.0 + 2.0 * strength - strength * ratio[-1]
        inverse.append(1.0 / pivot)
        ratio.append(strength / pivot)
    return inverse, ratio


def iota(shape, axis):
    return lax.broadcasted_iota(jnp.int32, shape, axis)


def lanes(*lead):
    return iota((*lead, 8, 128), len(lead) + 1)


def turn(x, shift):
    return pltpu.roll(x, shift, x.ndim - 1)


def east(x):
    rolled = turn(x, 127)
    return jnp.where(lanes(3) == 127, jnp.concatenate([rolled[1:], rolled[:1]], axis=0), rolled)


def west(x):
    rolled = turn(x, 1)
    return jnp.where(lanes(3) == 0, jnp.concatenate([rolled[2:], rolled[:2]], axis=0), rolled)


def east_block(x):
    rolled = turn(x[:2], 127)
    return jnp.where(lanes(2) == 127, jnp.concatenate([rolled[1:], x[2:]], axis=0), rolled)


def west_block(x):
    rolled = turn(x[:2], 1)
    return jnp.where(lanes(2) == 0, jnp.concatenate([x[2:], rolled[:1]], axis=0), rolled)


ETA, TX, TY, DEPTH, PACK, KMT = range(6)


def pack_2d(stage, count, put):
    lane = lanes()
    for i in STRIPS:
        rs = pl.ds(SUB * i, SUB)
        for m in PAIR:
            pack_w = pack_e = jnp.zeros(TILE, F32)
            for j in range(count):
                here = lane // HALO == j
                pack_w = jnp.where(here, turn(stage[m, j, 0, rs, :], HALO * j), pack_w)
                pack_e = jnp.where(here, turn(stage[m, j, 1, rs, :], (HALO * j + HALO) % LANES), pack_e)
            put(m, rs, pack_w, pack_e)


def stage_kernel(sub_count, eta, tx, ty, depth, wet_in, weights, stage):
    for lt in PAIR:
        ls = pl.ds(LANES * lt, LANES)
        wet = wet_in[:, ls].astype(F32)
        masked = jnp.where(wet > 0.0, depth[:, ls], 0.0)
        stage[0, KMT, lt] = wet
        for m in PAIR:
            for j, field in ((ETA, eta), (TX, tx), (TY, ty)):
                stage[m, j, lt] = field[m, :, ls]
            stage[m, DEPTH, lt] = masked
    for n in range(sub_count):
        stage[1, KMT, n // ROWS, pl.ds(n % ROWS, 1), :] = jnp.full((1, LANES), weights[n], F32)

    def put(m, rs, pack_w, pack_e):
        stage[m, PACK, 0, rs, :] = pack_w
        stage[m, PACK, 1, rs, :] = pack_e

    pack_2d(stage, 4, put)


def step_kernel(
    col_count, level_count, sub_count,
    u_hbm, v_hbm, t_hbm, s_hbm, stage,
    sol_u, sol_v, sol_t, sol_s, qu_out, qv_out, nuv_out, eta_out, tx_out, ty_out,
    cube,
    col_w, col_e, rcv_e, rcv_w, row_s, row_n, rcv_n, rcv_s, rcv_se, rcv_nw,
    kmt, nuv, sums, pk_e, pk_w, fstage, fstage_w, fstage_e, fpk_e, fpk_w,
    frame, coef, acc, result, result_in,
    table, load_sem, send_sem, edge_sem, row_sem, e_sem, w_sem, frow_sem, fe_sem, fw_sem, swap_sem,
):
    L = level_count
    U, V, T, S = range(4)
    sol = (sol_u, sol_v, sol_t, sol_s)
    FX, FY = 4, 5
    OWN = slice(0, 2)
    col = lax.axis_index("col")
    row = lax.axis_index("row")
    chip = row // 2
    core = row % 2
    east_col = lax.rem(col + 1, col_count)
    west_col = lax.rem(col + col_count - 1, col_count)
    peers = [lax.rem(row + d, 4) for d in (1, 2, 3)]
    lane = lanes()
    zero = jnp.zeros(TILE, F32)

    def aligned(start, size=8):
        return pl.ds(pl.multiple_of(start, 8), size)

    barrier = pltpu.get_barrier_semaphore()
    for r in peers:
        pl.semaphore_signal(barrier, inc=1, device_id={"row": r, "col": col}, device_id_type=MESH)
    for other in (east_col, west_col):
        for r in QUAD:
            pl.semaphore_signal(barrier, inc=1, device_id={"row": r, "col": other}, device_id_type=MESH)

    loads = []
    for f, src in enumerate((u_hbm, v_hbm, t_hbm, s_hbm)):
        for lt in PAIR:
            loads.append(pltpu.make_async_copy(
                src.at[:, :, :, pl.ds(LANES * lt, LANES)], cube.at[f, :, :, lt, pl.ds(PAD, ROWS), :], load_sem.at[2 * f + lt]))
            loads[-1].start()

    inv_v, ratio_v = sweep_constants(L, VISC_NUMBER)
    for n, line in enumerate((inv_v, ratio_v, [1.0 / (1.0 - r) for r in ratio_v], sweep_constants(L, DIFF_NUMBER)[0])):
        for k in range(L):
            table[n, k] = line[k]

    kmt[:, pl.ds(0, ROWS), :] = stage[0, KMT]

    has_s, has_n = row > 0, row < 3

    @pl.when(row == 0)
    def _():
        rcv_s[...] = jnp.zeros(rcv_s.shape, F32)
        rcv_se[...] = jnp.zeros(rcv_se.shape, F32)

    @pl.when(row == 3)
    def _():
        rcv_n[...] = jnp.zeros(rcv_n.shape, F32)
        rcv_nw[...] = jnp.zeros(rcv_nw.shape, F32)

    outside = jnp.zeros((6, RING, PAD, LANES), F32)

    @pl.when(chip == 0)
    def _():
        frame[:, :, pl.ds(FPAD - PAD, PAD), :] = outside

    @pl.when(chip == 1)
    def _():
        frame[:, :, pl.ds(FPAD + SUB * TILES, PAD), :] = outside


    lane42 = lanes(4, 2)
    lane2 = lanes(M)
    empty = jnp.zeros((M, SUB, LANES), F32)
    for f in QUAD:
        for copy in loads[2 * f:2 * f + 2]:
            copy.wait()

        def pack(g, carry):
            west_pack, east_pack = carry
            for k, i in [(EDGE_BLOCK * g + j, i) for j in range(EDGE_BLOCK) for i in STRIPS]:
                slot = L * i + k
                rs = pl.ds(PAD + SUB * i, SUB)
                west_pack = jnp.where(lane2 == slot, turn(cube[f, k, :, 0, rs, :], slot), west_pack)
                east_pack = jnp.where(lane2 == slot, turn(cube[f, k, :, 1, rs, :], slot + 1), east_pack)
            for q in range(M * EDGE_BLOCK // SUB):
                rows = aligned(M * EDGE_BLOCK * g + SUB * q)
                low = high = empty
                for j in OCTET:
                    k, m = EDGE_BLOCK * g + (SUB * q + j) // M, j % M
                    low = jnp.where(sub2 == j, cube[f, k, m, OWN, pl.ds(PAD - j, SUB), :], low)
                    high = jnp.where(sub2 == j, cube[f, k, m, OWN, pl.ds(PAD + ROWS - 1 - j, SUB), :], high)
                row_n[f, :, rows, :] = high
                row_s[f if f < T else f + 1, :, rows, :] = low
                if f == S:
                    row_s[T, :, rows, :] = row_s[T + 1, :, rows, :] - (HALINE_CON / THERM_EXP) * low
            return west_pack, east_pack

        sub2 = iota((M, SUB, LANES), 1)
        col_w[f], col_e[f] = lax.fori_loop(0, L // EDGE_BLOCK, pack, (empty, empty))
    for i in STRIPS:
        slot = 3 * L + i
        col_w[0, 0] = jnp.where(lane == slot, turn(kmt[0, pl.ds(SUB * i, SUB), :], slot), col_w[0, 0])
    row_s[U, :, pl.ds(M * L, SUB), :] = kmt[:, pl.ds(0, SUB), :]

    pl.semaphore_wait(barrier, 11)

    def send(src, dst, ssem, rsem, r, c):
        return pltpu.make_async_remote_copy(
            src_ref=src, dst_ref=dst, send_sem=send_sem.at[ssem], recv_sem=rsem, device_id={"row": r, "col": c}, device_id_type=MESH)

    def frame_rows(r, at_chip):
        return aligned(FPAD + ROWS * r - SHIFT * at_chip, ROWS)

    own_rows = frame_rows(row, chip)
    south, north = jnp.maximum(row - 1, 0), jnp.minimum(row + 1, 3)
    to_w = send(col_w, rcv_e, 0, edge_sem.at[0], row, west_col)
    to_e = send(col_e, rcv_w, 1, edge_sem.at[1], row, east_col)
    first_s, first_n = pl.ds(0, 3), pl.ds(0, 2)
    later_s, later_n = pl.ds(3, 2), pl.ds(2, 2)
    to_s = send(row_s.at[first_s], rcv_n.at[first_s], 2, edge_sem.at[2], south, col)
    to_n = send(row_n.at[first_n], rcv_s.at[first_n], 3, edge_sem.at[3], north, col)
    to_s_later = send(row_s.at[later_s], rcv_n.at[later_s], 6, edge_sem.at[6], south, col)
    to_n_later = send(row_n.at[later_n], rcv_s.at[later_n], 7, edge_sem.at[7], north, col)
    to_nw = send(col_w.at[V], rcv_se, 4, edge_sem.at[4], north, west_col)
    to_se = send(col_e.at[U], rcv_nw, 5, edge_sem.at[5], south, east_col)
    to_w.start()
    to_e.start()

    @pl.when(has_s)
    def _():
        to_s.start()
        to_se.start()
        to_s_later.start()

    @pl.when(has_n)
    def _():
        to_n.start()
        to_nw.start()
        to_n_later.start()

    def exchange(block, pack_w, pack_e, first, count, base, rsem, esem, wsem, pe, pw):
        out = []
        for d, r in enumerate(peers):
            out.append(send(block(r % 2), frame.at[pl.ds(first, count), OWN, frame_rows(row, r // 2), :], base + d, rsem.at[row], r, col))
        for r in QUAD:
            out.append(send(pack_w(r % 2), pe.at[row], base + 3 + 2 * r, esem.at[row], r, west_col))
            out.append(send(pack_e(r % 2), pw.at[row], base + 4 + 2 * r, wsem.at[row], r, east_col))
        for copy in out:
            copy.start()
        frame[pl.ds(first, count), OWN, own_rows, :] = block(core)[...]
        return out

    def collect(block, pack_w, first, count, rsem, esem, wsem, pe, pw):
        for r in peers:
            rows = frame_rows(r, chip)
            send(block(0), frame.at[pl.ds(first, count), OWN, rows, :], 0, rsem.at[r], r, col).wait_recv()
        for r in QUAD:
            send(pack_w(0), pe.at[r], 0, esem.at[r], r, east_col).wait_recv()
            send(pack_w(0), pw.at[r], 0, wsem.at[r], r, west_col).wait_recv()
        side = lax.broadcasted_iota(jnp.int32, (ROWS, 128), 1) // HALO
        for r in QUAD:
            for j in range(count):
                frame[first + j, 2, frame_rows(r, chip), :] = jnp.where(
                    side == 0, turn(pe[r], (128 - HALO * j) % 128), jnp.where(side == 3, turn(pw[r], (128 - HALO * j - HALO) % 128), 0.0))

    def stage_block(m):
        return stage.at[m, pl.ds(0, PACK)]

    def stage_w(m):
        return stage.at[m, PACK, 0]

    def stage_e(m):
        return stage.at[m, PACK, 1]

    to_w.wait_recv()
    to_e.wait_recv()

    def unpack(g, carry):
        from_e, from_w = rcv_e[...], rcv_w[...]
        for k in [EDGE_BLOCK * g + j for j in range(EDGE_BLOCK)]:
            for i in STRIPS:
                slot = L * i + k
                cube[:, k, :, 2, pl.ds(PAD + SUB * i, SUB), :] = jnp.where(
                    lane42 < 64, turn(from_w, lax.rem(128 - slot, 128)), turn(from_e, 127 - slot))
        return carry

    lax.fori_loop(0, L // EDGE_BLOCK, unpack, 0)

    def masks(i):
        rs = pl.ds(SUB * i, SUB)
        wet = kmt[:, rs, :]
        halo = turn(rcv_e[0, 0], 127 - (3 * L + i))
        nuv[0, :, rs, :] = jnp.minimum(wet, east_block(jnp.concatenate([wet, halo[None]], axis=0)))
        nuv[1, :, rs, :] = jnp.minimum(wet, kmt[:, pl.ds(8 * i + 1, 8), :])

    masks(0)
    masks(1)

    press = PRESS_SCALE / L
    pair = jnp.zeros((M, SUB, LANES), F32)

    def for_strips(body, init, strips=(0, 1, 3), levels=LEVEL_BLOCK):
        start, step, count = strips

        def strip(s, carry):
            m = s // count
            i = start + step * (s - count * m)
            rs = aligned(SUB * i)

            def get(f, k, part, d=0):
                start = PAD + 8 * i + d
                return cube[f, k, m, part, pl.ds(start if d else pl.multiple_of(start, 8), 8), :]

            state, finish = init(m, rs)

            def block(b, state):
                for j in range(levels):
                    k = b * levels + j
                    state = body(k, m, rs, get, state)
                return state

            finish(m, rs, lax.fori_loop(0, L // levels, block, state))
            return carry

        lax.fori_loop(0, M * count, strip, 0)

    def momentum_init(m, rs):
        return (pair,) * 6, momentum_finish

    def momentum_finish(m, rs, state):
        sums[0, m, :, rs, :] = state[4]
        sums[1, m, :, rs, :] = state[5]

    def momentum(k, m, rs, get, state):
        cx, cy, eu, ev, gu_sum, gv_sum = state
        level = k.astype(F32)
        both = slice(0, 3)
        u, v, un, vs = get(U, k, both), get(V, k, both), get(U, k, both, 1), get(V, k, both, -1)
        rho = (press * HALINE_CON) * get(S, k, both) - (press * THERM_EXP) * get(T, k, both)
        dx = rho[OWN] - east_block(rho)
        dy = rho[OWN] - ((press * HALINE_CON) * get(S, k, OWN, 1) - (press * THERM_EXP) * get(T, k, OWN, 1))
        vsum, usum = v + vs, u + un
        cx, cy = cx + dx, cy + dy
        gu = cx - 0.5 * (dx + u[OWN] * (east_block(u) - west_block(u))) - 0.125 * (
            (vsum[OWN] + east_block(vsum)) * (un[OWN] - get(U, k, OWN, -1)))
        gv = cy - 0.5 * (dy + v[OWN] * (get(V, k, OWN, 1) - vs[OWN])) - 0.125 * (
            (usum[OWN] + west_block(usum)) * (east_block(v) - west_block(v)))
        gu = jnp.where(nuv[0, :, rs, :] > level, gu, 0.0)
        gv = jnp.where(nuv[1, :, rs, :] > level, gv, 0.0)
        inverse = table[0, k]
        eu = (u[OWN] + gu + VISC_NUMBER * eu) * inverse
        ev = (v[OWN] + gv + VISC_NUMBER * ev) * inverse
        sol[U][k, m, :, rs, :] = eu
        sol[V][k, m, :, rs, :] = ev
        return cx, cy, eu, ev, gu_sum + gu, gv_sum + gv

    for_strips(momentum, momentum_init, strips=(1, 1, 1))

    @pl.when(has_n)
    def _():
        to_s.wait_recv()
        to_se.wait_recv()

    @pl.when(has_s)
    def _():
        to_n.wait_recv()
        to_nw.wait_recv()

    sent = exchange(stage_block, stage_w, stage_e, ETA, 4, 8, row_sem, e_sem, w_sem, pk_e, pk_w)

    def unpack_rows(g, carry):
        rows = aligned(SUB * g)
        below, above = rcv_s[:T, :, rows, :], rcv_n[:S, :, rows, :]
        for j in OCTET:
            k, m = 4 * g + j // 2, j % 2
            cube[:T, k, m, OWN, pl.ds(PAD - 1, 1), :] = below[:, :, j:j + 1, :]
            cube[:S, k, m, OWN, pl.ds(PAD + ROWS, 1), :] = above[:, :, j:j + 1, :]
            cube[S, k, m, OWN, pl.ds(PAD + ROWS, 1), :] = jnp.zeros((M, 1, LANES), F32)
            if m:
                cube[V, k, :, 2, pl.ds(0, PAD), :] = turn(rcv_se[...], 127 - 2 * L - k)
                cube[U, k, :, 2, pl.ds(PAD + ROWS, PAD), :] = turn(rcv_nw[...], lax.rem(128 - k, 128))
        return carry

    def unpack_rows_later(g, carry):
        rows = aligned(SUB * g)
        below, above = rcv_s[T:, :, rows, :], rcv_n[S:, :, rows, :]
        for j in OCTET:
            k, m = 4 * g + j // 2, j % 2
            cube[T:, k, m, OWN, pl.ds(PAD - 1, 1), :] = below[:, :, j:j + 1, :]
            cube[T:, k, m, OWN, pl.ds(PAD + ROWS, 1), :] = above[:, :, j:j + 1, :]
        return carry

    lax.fori_loop(0, L // 4, unpack_rows, 0)
    kmt[:, pl.ds(ROWS, 8), :] = rcv_n[U, :, pl.ds(M * L, SUB), :]
    masks(2)
    for_strips(momentum, momentum_init, strips=(0, 2, 2))

    collect(stage_block, stage_w, ETA, 4, row_sem, e_sem, w_sem, pk_e, pk_w)

    def coefficients(i, carry):
        rs = aligned(FPAD + SUB * i)
        depth = frame[DEPTH, :, rs, :]
        depth_e = east(depth)
        depth_n = frame[DEPTH, :, pl.ds(FPAD + SUB * i + 1, SUB), :]
        wet = depth > 0.0
        coef[0, :, rs, :] = jnp.where(wet, WAVE_COURANT, 0.0)
        coef[1, :, rs, :] = jnp.where(wet & (depth_e > 0.0), (0.5 * WAVE_COURANT) * (depth + depth_e), 0.0)
        coef[2, :, rs, :] = jnp.where(wet & (depth_n > 0.0), (0.5 * WAVE_COURANT) * (depth + depth_n), 0.0)
        return carry

    lax.fori_loop(0, TILES, coefficients, 0)

    for d in PAIR:
        scale = coef[1 + d, OWN, own_rows, :] / (jnp.maximum(nuv[d], 1.0) * (WAVE_COURANT * sub_count))
        for m in PAIR:
            fstage[m, d] = scale * sums[d, m]

    def put(m, rs, pack_w, pack_e):
        fstage_w[m, rs, :] = pack_w
        fstage_e[m, rs, :] = pack_e

    pack_2d(fstage, 2, put)
    sent += exchange(lambda m: fstage.at[m], lambda m: fstage_w.at[m], lambda m: fstage_e.at[m], FX, 2, 19, frow_sem, fe_sem, fw_sem, fpk_e, fpk_w)

    block_zero = jnp.zeros((M, ROWS, LANES), F32)

    def back(m, carry):
        def levels_back(b, state):
            x, total = list(state[:2]), list(state[2:])
            for j in range(BACK_BLOCK):
                k = L - 1 - (b * BACK_BLOCK + j)
                level = k.astype(F32)
                for d in PAIR:
                    e, n = sol[d][k, m], nuv[d]
                    x[d] = e + table[1, k] * jnp.where(n > level + 1.0, x[d], e * table[2, k])
                    sol[d][k, m] = x[d]
                    total[d] = total[d] + jnp.where(n > level, x[d], 0.0)
            return (*x, *total)

        state = lax.fori_loop(0, L // BACK_BLOCK, levels_back, (block_zero,) * 4)
        for d in PAIR:
            sums[d, m] = state[2 + d] / jnp.maximum(nuv[d], 1.0)
        return carry

    lax.fori_loop(0, M, back, 0)

    def tracer_init(m, rs):
        return pair, lambda *a: None

    def tracer(f):
        def body(k, m, rs, get, e):
            t, u = get(f, k, slice(0, 3)), get(U, k, slice(0, 3))
            fx = u * (t + jnp.concatenate([east_block(t), t[:1]], axis=0))
            t = t[OWN]
            gain = fx[OWN] - west_block(fx) + (get(V, k, OWN) * (t + get(f, k, OWN, 1)) - get(V, k, OWN, -1) * (t + get(f, k, OWN, -1)))
            e = (jnp.where(kmt[:, rs, :] > k.astype(F32), t - 0.5 * gain, 0.0) + DIFF_NUMBER * e) * table[3, k]
            sol[f][k, m, :, rs, :] = e
            return e

        return body

    @pl.when(has_n)
    def _():
        to_s_later.wait_recv()

    @pl.when(has_s)
    def _():
        to_n_later.wait_recv()

    lax.fori_loop(0, L // 4, unpack_rows_later, 0)
    for f in (T, S):
        for_strips(tracer(f), tracer_init, levels=TRACER_BLOCK)
    acc[...] = jnp.zeros(acc.shape, F32)

    collect(lambda m: fstage.at[m], lambda m: fstage_w.at[m], FX, 2, frow_sem, fe_sem, fw_sem, fpk_e, fpk_w)

    def subcycle(n, tiles, base):
        def tile_rows(t):
            return aligned(base + SUB * t)

        def eta_tile(t):
            rs = tile_rows(t)
            u, v = frame[TX, :, rs, :], frame[TY, :, rs, :]
            div = (u - west(u)) + (v - frame[TY, :, pl.ds(base + SUB * t - 1, SUB), :])
            eta = frame[ETA, :, rs, :] - coef[0, :, rs, :] * div
            frame[ETA, :, rs, :] = eta
            return u, v, eta

        last_row = iota((RING, SUB, LANES), 1) == SUB - 1
        following = eta_tile(0)
        for t in range(tiles):
            u, v, e = following
            if t + 1 < tiles:
                following = eta_tile(t + 1)
            e_n = jnp.where(last_row, pltpu.roll(following[2], SUB - 1, 1), pltpu.roll(e, SUB - 1, 1))
            rs = tile_rows(t)
            frame[TX, :, rs, :] = u + frame[FX, :, rs, :] - coef[1, :, rs, :] * (east(e) - e)
            frame[TY, :, rs, :] = v + frame[FY, :, rs, :] - coef[2, :, rs, :] * (e_n - e)
        chip_rows = aligned(FPAD + (M * ROWS - SHIFT) * chip, M * ROWS)
        acc[...] += stage[1, KMT, n // ROWS, pl.ds(lax.rem(n, ROWS), 1), :] * frame[pl.ds(0, RING), OWN, chip_rows, :]

    def subcycles(first, last, tiles, base):
        def block(b, carry):
            for j in range(SUB_BLOCK):
                subcycle(SUB_BLOCK * b + j, tiles, base)
            return carry

        lax.fori_loop(first // SUB_BLOCK, last // SUB_BLOCK, block, 0)

    turning = -(-max(sub_count - SHIFT, 0) // SUB_BLOCK) * SUB_BLOCK
    subcycles(0, turning, TILES, FPAD)
    subcycles(turning, sub_count, TILES - SHIFT // SUB, FPAD + SHIFT * chip)

    mine = aligned(ROWS * core, ROWS)
    theirs = aligned(ROWS * (1 - core), ROWS)
    result[...] = acc[:, :, theirs, :]
    swap = send(result, result_in, 30, swap_sem, row + 1 - 2 * core, col)
    swap.start()
    swap.wait_recv()
    for m in PAIR:
        whole = jnp.where(core == m, acc[:, :, mine, :], result_in[...])
        for lt in PAIR:
            ls = pl.ds(LANES * lt, LANES)
            eta_out[m, :, ls] = whole[ETA, lt]
            tx_out[m, :, ls] = whole[TX, lt]
            ty_out[m, :, ls] = whole[TY, lt]
            for d, out in enumerate((qu_out, qv_out)):
                depth = coef[1 + d, lt, own_rows, :]
                out[m, :, ls] = whole[TX + d, lt] / jnp.where(depth > 0.0, depth / WAVE_COURANT, 1.0) - sums[d, m, lt]
                nuv_out[d, :, ls] = nuv[d, lt]

    to_w.wait_send()
    to_e.wait_send()

    @pl.when(has_s)
    def _():
        to_s.wait_send()
        to_se.wait_send()
        to_s_later.wait_send()

    @pl.when(has_n)
    def _():
        to_n.wait_send()
        to_nw.wait_send()
        to_n_later.wait_send()

    for copy in sent:
        copy.wait_send()
    swap.wait_send()


def final_kernel(level_count, sol_u, sol_v, sol_t, sol_s, qu, qv, nuv, wet, eta_in, tx_in, ty_in,
                 eta_out, tx_out, ty_out, u_out, v_out, t_out, s_out, cubes, cube_sem):
    ratio = sweep_constants(level_count, DIFF_NUMBER)[1]
    strips = M * len(STRIPS)
    eta_out[...] = eta_in[...]
    tx_out[...] = tx_in[...]
    ty_out[...] = ty_in[...]

    def writes(s):
        m = s // 3
        rs = pl.ds(pl.multiple_of(SUB * (s - 3 * m), SUB), SUB)
        return m, rs, [pltpu.make_async_copy(cubes.at[f, s], dst.at[:, m, rs, :], cube_sem.at[f, s])
                       for f, dst in enumerate((t_out, s_out, u_out, v_out))]

    def strip(s, carry):
        m, rs, done = writes(s)
        for f, src in enumerate((sol_t, sol_s, sol_u, sol_v)):
            for lt in PAIR:
                ls = pl.ds(LANES * lt, LANES)
                if f < M:
                    n_wet = wet[rs, ls]
                    x = jnp.zeros(TILE, F32)
                    for k in reversed(range(level_count)):
                        e = src[k, m, lt, rs, :]
                        x = e + ratio[k] * jnp.where(n_wet > k + 1, x, e * (1.0 / (1.0 - ratio[k])))
                        cubes[f, s, k, :, ls] = jnp.where(n_wet > k, x, 0.0)
                else:
                    n, mean = nuv[f - M, rs, ls], (qu, qv)[f - M][m, rs, ls]
                    for k in range(level_count):
                        cubes[f, s, k, :, ls] = jnp.where(n > float(k), src[k, m, lt, rs, :] + mean, 0.0)
            done[f].start()
        return carry

    def finish(s, carry):
        for copy in writes(s)[-1]:
            copy.wait()
        return carry

    lax.fori_loop(0, strips, strip, 0)
    lax.fori_loop(0, strips, finish, 0)


def solution(mesh):
    col_count = mesh.shape["col"]

    def local_step(vel_x, vel_y, pot_temp, salinity, surf_eta, trans_x, trans_y, col_depth, wet_levels, avg_weights):
        L = vel_x.shape[0]
        N = avg_weights.shape[0]
        hbm_spec = pl.BlockSpec(memory_space=pltpu.HBM)
        vmem_spec = pl.BlockSpec(memory_space=pltpu.VMEM)
        cube = jax.ShapeDtypeStruct(vel_x.shape, F32)
        flat = jax.ShapeDtypeStruct(surf_eta.shape, F32)
        vm = lambda *shape: pltpu.VMEM(shape, F32)
        dma = lambda n: pltpu.SemaphoreType.DMA((n,))
        stage = pl.pallas_call(
            functools.partial(stage_kernel, N),
            out_shape=jax.ShapeDtypeStruct((M, 6, M, ROWS, LANES), F32),
            in_specs=[vmem_spec] * 5 + [pl.BlockSpec(memory_space=pltpu.SMEM)],
            out_specs=vmem_spec,
            name="ocean_stage",
        )(surf_eta, trans_x, trans_y, col_depth, wet_levels, avg_weights)
        *sol, qu, qv, nuv, eta_o, tx_o, ty_o = pl.pallas_call(
            functools.partial(step_kernel, col_count, L, N),
            out_shape=[jax.ShapeDtypeStruct((L, M, M, ROWS, LANES), F32)] * 4 + [flat] * 6,
            in_specs=[hbm_spec] * 4 + [vmem_spec],
            out_specs=[vmem_spec] * 10,
            scratch_shapes=[
                vm(4, L, M, RING, XR, LANES), *[vm(4, M, 8, LANES)] * 4, vm(5, M, M * L + 8, LANES), vm(4, M, M * L, LANES), vm(5, M, M * L + 8, LANES), vm(4, M, M * L, LANES),
                *[vm(M, 8, LANES)] * 2, vm(M, ROWS + 8, LANES), vm(M, M, ROWS, LANES), vm(M, M, M, ROWS, LANES),
                *[vm(4, ROWS, LANES)] * M,
                vm(M, M, M, ROWS, LANES), *[vm(M, ROWS, LANES)] * M, *[vm(4, ROWS, LANES)] * M,
                vm(6, RING, FRAME, LANES), vm(RING, RING, FRAME, LANES), vm(RING, M, M * ROWS, LANES), *[vm(RING, M, ROWS, LANES)] * M,
                pltpu.SMEM((4, L), F32), dma(8), dma(31), dma(8), *[dma(4)] * 6, pltpu.SemaphoreType.DMA],
            compiler_params=pltpu.CompilerParams(collective_id=0, has_side_effects=True, vmem_limit_bytes=STEP_VMEM),
            name="ocean_step",
        )(vel_x, vel_y, pot_temp, salinity, stage)
        outs = pl.pallas_call(
            functools.partial(final_kernel, L),
            out_shape=[flat] * 3 + [cube] * 4,
            in_specs=[vmem_spec] * 11,
            out_specs=[vmem_spec] * 3 + [hbm_spec] * 4,
            scratch_shapes=[vm(4, M * len(STRIPS), L, SUB, 256), pltpu.SemaphoreType.DMA((4, M * len(STRIPS)))],
            name="ocean_final",
            compiler_params=pltpu.CompilerParams(vmem_limit_bytes=FINAL_VMEM),
        )(*sol, qu, qv, nuv, wet_levels, eta_o, tx_o, ty_o)
        return tuple(outs)

    spec_3d = P(None, None, "row", "col")
    spec_2d = P(None, "row", "col")
    spec_map = P("row", "col")
    return jax.shard_map(local_step, mesh=mesh, in_specs=(spec_3d,) * 4 + (spec_2d,) * 3 + (spec_map,) * 2 + (P(),),
                         out_specs=(spec_2d,) * 3 + (spec_3d,) * 4, check_vma=False)
```

```python
import functools

import jax
import jax.numpy as jnp
from jax import lax
from jax.experimental import pallas as pl
from jax.experimental.pallas import tpu as pltpu
from jax.sharding import PartitionSpec as P

WAVE_COURANT = 0.4
THERM_EXP = 0.2
HALINE_CON = 0.15
PRESS_SCALE = 0.5
VISC_NUMBER = 1.0
DIFF_NUMBER = 0.5

MESH = pl.DeviceIdType.MESH
F32 = jnp.float32
ROWS = 24
PAD = 8
XR = ROWS + 2 * PAD
EDGE_BLOCK = 12
TRACER_BLOCK = 36
BACK_BLOCK = 36
SUB_BLOCK = 3
LEVEL_BLOCK = 36
LANES = 128
SUB = 8
TILE = (SUB, LANES)
PAIR, STRIPS, QUAD, OCTET = range(2), range(3), range(4), range(SUB)
RING = 3
M = 2
STEP_VMEM, FINAL_VMEM = 46 << 20, 9 << 20
TILES = 10
SHIFT = 16
FPAD = SHIFT + PAD
FRAME = 4 * ROWS + 2 * FPAD
HALO = 32


def sweep_constants(level_count, strength):
    inverse, ratio = [], []
    for k in range(level_count):
        pivot = 1.0 + strength if k == 0 else 1.0 + 2.0 * strength - strength * ratio[-1]
        inverse.append(1.0 / pivot)
        ratio.append(strength / pivot)
    return inverse, ratio


def iota(shape, axis):
    return lax.broadcasted_iota(jnp.int32, shape, axis)


def lanes(*lead):
    return iota((*lead, 8, 128), len(lead) + 1)


def turn(x, shift):
    return pltpu.roll(x, shift, x.ndim - 1)


def east(x):
    rolled = turn(x, 127)
    return jnp.where(lanes(3) == 127, jnp.concatenate([rolled[1:], rolled[:1]], axis=0), rolled)


def west(x):
    rolled = turn(x, 1)
    return jnp.where(lanes(3) == 0, jnp.concatenate([rolled[2:], rolled[:2]], axis=0), rolled)


def east_block(x):
    rolled = turn(x[:2], 127)
    return jnp.where(lanes(2) == 127, jnp.concatenate([rolled[1:], x[2:]], axis=0), rolled)


def west_block(x):
    rolled = turn(x[:2], 1)
    return jnp.where(lanes(2) == 0, jnp.concatenate([x[2:], rolled[:1]], axis=0), rolled)


ETA, TX, TY, DEPTH, PACK, KMT = range(6)


def pack_2d(stage, count, put):
    lane = lanes()
    for i in STRIPS:
        rs = pl.ds(SUB * i, SUB)
        for m in PAIR:
            pack_w = pack_e = jnp.zeros(TILE, F32)
            for j in range(count):
                here = lane // HALO == j
                pack_w = jnp.where(here, turn(stage[m, j, 0, rs, :], HALO * j), pack_w)
                pack_e = jnp.where(here, turn(stage[m, j, 1, rs, :], (HALO * j + HALO) % LANES), pack_e)
            put(m, rs, pack_w, pack_e)


def stage_kernel(sub_count, eta, tx, ty, depth, wet_in, weights, stage):
    for lt in PAIR:
        ls = pl.ds(LANES * lt, LANES)
        wet = wet_in[:, ls].astype(F32)
        masked = jnp.where(wet > 0.0, depth[:, ls], 0.0)
        stage[0, KMT, lt] = wet
        for m in PAIR:
            for j, field in ((ETA, eta), (TX, tx), (TY, ty)):
                stage[m, j, lt] = field[m, :, ls]
            stage[m, DEPTH, lt] = masked
    for n in range(sub_count):
        stage[1, KMT, n // ROWS, pl.ds(n % ROWS, 1), :] = jnp.full((1, LANES), weights[n], F32)

    def put(m, rs, pack_w, pack_e):
        stage[m, PACK, 0, rs, :] = pack_w
        stage[m, PACK, 1, rs, :] = pack_e

    pack_2d(stage, 4, put)


def step_kernel(
    col_count, level_count, sub_count,
    u_hbm, v_hbm, t_hbm, s_hbm, stage,
    sol_u, sol_v, sol_t, sol_s, qu_out, qv_out, nuv_out, eta_out, tx_out, ty_out,
    cube,
    col_w, col_e, rcv_e, rcv_w, row_s, row_n, rcv_n, rcv_s, rcv_se, rcv_nw,
    kmt, nuv, sums, pk_e, pk_w, fstage, fstage_w, fstage_e, fpk_e, fpk_w,
    frame, coef, acc, result, result_in,
    table, load_sem, send_sem, edge_sem, row_sem, e_sem, w_sem, frow_sem, fe_sem, fw_sem, swap_sem,
):
    L = level_count
    U, V, T, S = range(4)
    sol = (sol_u, sol_v, sol_t, sol_s)
    FX, FY = 4, 5
    OWN = slice(0, 2)
    col = lax.axis_index("col")
    row = lax.axis_index("row")
    chip = row // 2
    core = row % 2
    east_col = lax.rem(col + 1, col_count)
    west_col = lax.rem(col + col_count - 1, col_count)
    peers = [lax.rem(row + d, 4) for d in (1, 2, 3)]
    lane = lanes()
    zero = jnp.zeros(TILE, F32)

    def aligned(start, size=8):
        return pl.ds(pl.multiple_of(start, 8), size)

    barrier = pltpu.get_barrier_semaphore()
    for r in peers:
        pl.semaphore_signal(barrier, inc=1, device_id={"row": r, "col": col}, device_id_type=MESH)
    for other in (east_col, west_col):
        for r in QUAD:
            pl.semaphore_signal(barrier, inc=1, device_id={"row": r, "col": other}, device_id_type=MESH)

    loads = []
    for f, src in enumerate((u_hbm, v_hbm, t_hbm, s_hbm)):
        for lt in PAIR:
            loads.append(pltpu.make_async_copy(
                src.at[:, :, :, pl.ds(LANES * lt, LANES)], cube.at[f, :, :, lt, pl.ds(PAD, ROWS), :], load_sem.at[2 * f + lt]))
            loads[-1].start()

    inv_v, ratio_v = sweep_constants(L, VISC_NUMBER)
    for n, line in enumerate((inv_v, ratio_v, [1.0 / (1.0 - r) for r in ratio_v], sweep_constants(L, DIFF_NUMBER)[0])):
        for k in range(L):
            table[n, k] = line[k]

    kmt[:, pl.ds(0, ROWS), :] = stage[0, KMT]

    has_s, has_n = row > 0, row < 3

    @pl.when(row == 0)
    def _():
        rcv_s[...] = jnp.zeros(rcv_s.shape, F32)
        rcv_se[...] = jnp.zeros(rcv_se.shape, F32)

    @pl.when(row == 3)
    def _():
        rcv_n[...] = jnp.zeros(rcv_n.shape, F32)
        rcv_nw[...] = jnp.zeros(rcv_nw.shape, F32)

    outside = jnp.zeros((6, RING, PAD, LANES), F32)

    @pl.when(chip == 0)
    def _():
        frame[:, :, pl.ds(FPAD - PAD, PAD), :] = outside

    @pl.when(chip == 1)
    def _():
        frame[:, :, pl.ds(FPAD + SUB * TILES, PAD), :] = outside


    lane42 = lanes(4, 2)
    lane2 = lanes(M)
    empty = jnp.zeros((M, SUB, LANES), F32)
    for f in QUAD:
        for copy in loads[2 * f:2 * f + 2]:
            copy.wait()

        def pack(g, carry):
            west_pack, east_pack = carry
            for k, i in [(EDGE_BLOCK * g + j, i) for j in range(EDGE_BLOCK) for i in STRIPS]:
                slot = L * i + k
                rs = pl.ds(PAD + SUB * i, SUB)
                west_pack = jnp.where(lane2 == slot, turn(cube[f, k, :, 0, rs, :], slot), west_pack)
                east_pack = jnp.where(lane2 == slot, turn(cube[f, k, :, 1, rs, :], slot + 1), east_pack)
            for q in range(M * EDGE_BLOCK // SUB):
                rows = aligned(M * EDGE_BLOCK * g + SUB * q)
                low = high = empty
                for j in OCTET:
                    k, m = EDGE_BLOCK * g + (SUB * q + j) // M, j % M
                    low = jnp.where(sub2 == j, cube[f, k, m, OWN, pl.ds(PAD - j, SUB), :], low)
                    high = jnp.where(sub2 == j, cube[f, k, m, OWN, pl.ds(PAD + ROWS - 1 - j, SUB), :], high)
                row_n[f, :, rows, :] = high
                row_s[f if f < T else f + 1, :, rows, :] = low
                if f == S:
                    row_s[T, :, rows, :] = row_s[T + 1, :, rows, :] - (HALINE_CON / THERM_EXP) * low
            return west_pack, east_pack

        sub2 = iota((M, SUB, LANES), 1)
        col_w[f], col_e[f] = lax.fori_loop(0, L // EDGE_BLOCK, pack, (empty, empty))
    for i in STRIPS:
        slot = 3 * L + i
        col_w[0, 0] = jnp.where(lane == slot, turn(kmt[0, pl.ds(SUB * i, SUB), :], slot), col_w[0, 0])
    row_s[U, :, pl.ds(M * L, SUB), :] = kmt[:, pl.ds(0, SUB), :]

    pl.semaphore_wait(barrier, 11)

    def send(src, dst, ssem, rsem, r, c):
        return pltpu.make_async_remote_copy(
            src_ref=src, dst_ref=dst, send_sem=send_sem.at[ssem], recv_sem=rsem, device_id={"row": r, "col": c}, device_id_type=MESH)

    def frame_rows(r, at_chip):
        return aligned(FPAD + ROWS * r - SHIFT * at_chip, ROWS)

    own_rows = frame_rows(row, chip)
    south, north = jnp.maximum(row - 1, 0), jnp.minimum(row + 1, 3)
    to_w = send(col_w, rcv_e, 0, edge_sem.at[0], row, west_col)
    to_e = send(col_e, rcv_w, 1, edge_sem.at[1], row, east_col)
    first_s, first_n = pl.ds(0, 3), pl.ds(0, 2)
    later_s, later_n = pl.ds(3, 2), pl.ds(2, 2)
    to_s = send(row_s.at[first_s], rcv_n.at[first_s], 2, edge_sem.at[2], south, col)
    to_n = send(row_n.at[first_n], rcv_s.at[first_n], 3, edge_sem.at[3], north, col)
    to_s_later = send(row_s.at[later_s], rcv_n.at[later_s], 6, edge_sem.at[6], south, col)
    to_n_later = send(row_n.at[later_n], rcv_s.at[later_n], 7, edge_sem.at[7], north, col)
    to_nw = send(col_w.at[V], rcv_se, 4, edge_sem.at[4], north, west_col)
    to_se = send(col_e.at[U], rcv_nw, 5, edge_sem.at[5], south, east_col)
    to_w.start()
    to_e.start()

    @pl.when(has_s)
    def _():
        to_s.start()
        to_se.start()
        to_s_later.start()

    @pl.when(has_n)
    def _():
        to_n.start()
        to_nw.start()
        to_n_later.start()

    def exchange(block, pack_w, pack_e, first, count, base, rsem, esem, wsem, pe, pw):
        out = []
        for d, r in enumerate(peers):
            out.append(send(block(r % 2), frame.at[pl.ds(first, count), OWN, frame_rows(row, r // 2), :], base + d, rsem.at[row], r, col))
        for r in QUAD:
            out.append(send(pack_w(r % 2), pe.at[row], base + 3 + 2 * r, esem.at[row], r, west_col))
            out.append(send(pack_e(r % 2), pw.at[row], base + 4 + 2 * r, wsem.at[row], r, east_col))
        for copy in out:
            copy.start()
        frame[pl.ds(first, count), OWN, own_rows, :] = block(core)[...]
        return out

    def collect(block, pack_w, first, count, rsem, esem, wsem, pe, pw):
        for r in peers:
            rows = frame_rows(r, chip)
            send(block(0), frame.at[pl.ds(first, count), OWN, rows, :], 0, rsem.at[r], r, col).wait_recv()
        for r in QUAD:
            send(pack_w(0), pe.at[r], 0, esem.at[r], r, east_col).wait_recv()
            send(pack_w(0), pw.at[r], 0, wsem.at[r], r, west_col).wait_recv()
        side = lax.broadcasted_iota(jnp.int32, (ROWS, 128), 1) // HALO
        for r in QUAD:
            for j in range(count):
                frame[first + j, 2, frame_rows(r, chip), :] = jnp.where(
                    side == 0, turn(pe[r], (128 - HALO * j) % 128), jnp.where(side == 3, turn(pw[r], (128 - HALO * j - HALO) % 128), 0.0))

    def stage_block(m):
        return stage.at[m, pl.ds(0, PACK)]

    def stage_w(m):
        return stage.at[m, PACK, 0]

    def stage_e(m):
        return stage.at[m, PACK, 1]

    to_w.wait_recv()
    to_e.wait_recv()

    def unpack(g, carry):
        from_e, from_w = rcv_e[...], rcv_w[...]
        for k in [EDGE_BLOCK * g + j for j in range(EDGE_BLOCK)]:
            for i in STRIPS:
                slot = L * i + k
                cube[:, k, :, 2, pl.ds(PAD + SUB * i, SUB), :] = jnp.where(
                    lane42 < 64, turn(from_w, lax.rem(128 - slot, 128)), turn(from_e, 127 - slot))
        return carry

    lax.fori_loop(0, L // EDGE_BLOCK, unpack, 0)

    def masks(i):
        rs = pl.ds(SUB * i, SUB)
        wet = kmt[:, rs, :]
        halo = turn(rcv_e[0, 0], 127 - (3 * L + i))
        nuv[0, :, rs, :] = jnp.minimum(wet, east_block(jnp.concatenate([wet, halo[None]], axis=0)))
        nuv[1, :, rs, :] = jnp.minimum(wet, kmt[:, pl.ds(8 * i + 1, 8), :])

    masks(0)
    masks(1)

    press = PRESS_SCALE / L
    pair = jnp.zeros((M, SUB, LANES), F32)

    def for_strips(body, init, strips=(0, 1, 3), levels=LEVEL_BLOCK):
        start, step, count = strips

        def strip(s, carry):
            m = s // count
            i = start + step * (s - count * m)
            rs = aligned(SUB * i)

            def get(f, k, part, d=0):
                start = PAD + 8 * i + d
                return cube[f, k, m, part, pl.ds(start if d else pl.multiple_of(start, 8), 8), :]

            state, finish = init(m, rs)

            def block(b, state):
                for j in range(levels):
                    k = b * levels + j
                    state = body(k, m, rs, get, state)
                return state

            finish(m, rs, lax.fori_loop(0, L // levels, block, state))
            return carry

        lax.fori_loop(0, M * count, strip, 0)

    def momentum_init(m, rs):
        return (pair,) * 6, momentum_finish

    def momentum_finish(m, rs, state):
        sums[0, m, :, rs, :] = state[4]
        sums[1, m, :, rs, :] = state[5]

    def momentum(k, m, rs, get, state):
        cx, cy, eu, ev, gu_sum, gv_sum = state
        level = k.astype(F32)
        both = slice(0, 3)
        u, v, un, vs = get(U, k, both), get(V, k, both), get(U, k, both, 1), get(V, k, both, -1)
        rho = (press * HALINE_CON) * get(S, k, both) - (press * THERM_EXP) * get(T, k, both)
        dx = rho[OWN] - east_block(rho)
        dy = rho[OWN] - ((press * HALINE_CON) * get(S, k, OWN, 1) - (press * THERM_EXP) * get(T, k, OWN, 1))
        vsum, usum = v + vs, u + un
        cx, cy = cx + dx, cy + dy
        gu = cx - 0.5 * (dx + u[OWN] * (east_block(u) - west_block(u))) - 0.125 * (
            (vsum[OWN] + east_block(vsum)) * (un[OWN] - get(U, k, OWN, -1)))
        gv = cy - 0.5 * (dy + v[OWN] * (get(V, k, OWN, 1) - vs[OWN])) - 0.125 * (
            (usum[OWN] + west_block(usum)) * (east_block(v) - west_block(v)))
        gu = jnp.where(nuv[0, :, rs, :] > level, gu, 0.0)
        gv = jnp.where(nuv[1, :, rs, :] > level, gv, 0.0)
        inverse = table[0, k]
        eu = (u[OWN] + gu + VISC_NUMBER * eu) * inverse
        ev = (v[OWN] + gv + VISC_NUMBER * ev) * inverse
        sol[U][k, m, :, rs, :] = eu
        sol[V][k, m, :, rs, :] = ev
        return cx, cy, eu, ev, gu_sum + gu, gv_sum + gv

    for_strips(momentum, momentum_init, strips=(1, 1, 1))

    @pl.when(has_n)
    def _():
        to_s.wait_recv()
        to_se.wait_recv()

    @pl.when(has_s)
    def _():
        to_n.wait_recv()
        to_nw.wait_recv()

    sent = exchange(stage_block, stage_w, stage_e, ETA, 4, 8, row_sem, e_sem, w_sem, pk_e, pk_w)

    def unpack_rows(g, carry):
        rows = aligned(SUB * g)
        below, above = rcv_s[:T, :, rows, :], rcv_n[:S, :, rows, :]
        for j in OCTET:
            k, m = 4 * g + j // 2, j % 2
            cube[:T, k, m, OWN, pl.ds(PAD - 1, 1), :] = below[:, :, j:j + 1, :]
            cube[:S, k, m, OWN, pl.ds(PAD + ROWS, 1), :] = above[:, :, j:j + 1, :]
            cube[S, k, m, OWN, pl.ds(PAD + ROWS, 1), :] = jnp.zeros((M, 1, LANES), F32)
            if m:
                cube[V, k, :, 2, pl.ds(0, PAD), :] = turn(rcv_se[...], 127 - 2 * L - k)
                cube[U, k, :, 2, pl.ds(PAD + ROWS, PAD), :] = turn(rcv_nw[...], lax.rem(128 - k, 128))
        return carry

    def unpack_rows_later(g, carry):
        rows = aligned(SUB * g)
        below, above = rcv_s[T:, :, rows, :], rcv_n[S:, :, rows, :]
        for j in OCTET:
            k, m = 4 * g + j // 2, j % 2
            cube[T:, k, m, OWN, pl.ds(PAD - 1, 1), :] = below[:, :, j:j + 1, :]
            cube[T:, k, m, OWN, pl.ds(PAD + ROWS, 1), :] = above[:, :, j:j + 1, :]
        return carry

    lax.fori_loop(0, L // 4, unpack_rows, 0)
    kmt[:, pl.ds(ROWS, 8), :] = rcv_n[U, :, pl.ds(M * L, SUB), :]
    masks(2)
    for_strips(momentum, momentum_init, strips=(0, 2, 2))

    collect(stage_block, stage_w, ETA, 4, row_sem, e_sem, w_sem, pk_e, pk_w)

    def coefficients(i, carry):
        rs = aligned(FPAD + SUB * i)
        depth = frame[DEPTH, :, rs, :]
        depth_e = east(depth)
        depth_n = frame[DEPTH, :, pl.ds(FPAD + SUB * i + 1, SUB), :]
        wet = depth > 0.0
        coef[0, :, rs, :] = jnp.where(wet, WAVE_COURANT, 0.0)
        coef[1, :, rs, :] = jnp.where(wet & (depth_e > 0.0), (0.5 * WAVE_COURANT) * (depth + depth_e), 0.0)
        coef[2, :, rs, :] = jnp.where(wet & (depth_n > 0.0), (0.5 * WAVE_COURANT) * (depth + depth_n), 0.0)
        return carry

    lax.fori_loop(0, TILES, coefficients, 0)

    for d in PAIR:
        scale = coef[1 + d, OWN, own_rows, :] / (jnp.maximum(nuv[d], 1.0) * (WAVE_COURANT * sub_count))
        for m in PAIR:
            fstage[m, d] = scale * sums[d, m]

    def put(m, rs, pack_w, pack_e):
        fstage_w[m, rs, :] = pack_w
        fstage_e[m, rs, :] = pack_e

    pack_2d(fstage, 2, put)
    sent += exchange(lambda m: fstage.at[m], lambda m: fstage_w.at[m], lambda m: fstage_e.at[m], FX, 2, 19, frow_sem, fe_sem, fw_sem, fpk_e, fpk_w)

    block_zero = jnp.zeros((M, ROWS, LANES), F32)

    def back(m, carry):
        def levels_back(b, state):
            x, total = list(state[:2]), list(state[2:])
            for j in range(BACK_BLOCK):
                k = L - 1 - (b * BACK_BLOCK + j)
                level = k.astype(F32)
                for d in PAIR:
                    e, n = sol[d][k, m], nuv[d]
                    x[d] = e + table[1, k] * jnp.where(n > level + 1.0, x[d], e * table[2, k])
                    sol[d][k, m] = x[d]
                    total[d] = total[d] + jnp.where(n > level, x[d], 0.0)
            return (*x, *total)

        state = lax.fori_loop(0, L // BACK_BLOCK, levels_back, (block_zero,) * 4)
        for d in PAIR:
            sums[d, m] = state[2 + d] / jnp.maximum(nuv[d], 1.0)
        return carry

    lax.fori_loop(0, M, back, 0)

    def tracer_init(m, rs):
        return pair, lambda *a: None

    def tracer(f):
        def body(k, m, rs, get, e):
            t, u = get(f, k, slice(0, 3)), get(U, k, slice(0, 3))
            fx = u * (t + jnp.concatenate([east_block(t), t[:1]], axis=0))
            t = t[OWN]
            gain = fx[OWN] - west_block(fx) + (get(V, k, OWN) * (t + get(f, k, OWN, 1)) - get(V, k, OWN, -1) * (t + get(f, k, OWN, -1)))
            e = (jnp.where(kmt[:, rs, :] > k.astype(F32), t - 0.5 * gain, 0.0) + DIFF_NUMBER * e) * table[3, k]
            sol[f][k, m, :, rs, :] = e
            return e

        return body

    @pl.when(has_n)
    def _():
        to_s_later.wait_recv()

    @pl.when(has_s)
    def _():
        to_n_later.wait_recv()

    lax.fori_loop(0, L // 4, unpack_rows_later, 0)
    for f in (T, S):
        for_strips(tracer(f), tracer_init, levels=TRACER_BLOCK)
    acc[...] = jnp.zeros(acc.shape, F32)

    collect(lambda m: fstage.at[m], lambda m: fstage_w.at[m], FX, 2, frow_sem, fe_sem, fw_sem, fpk_e, fpk_w)

    def subcycle(n, tiles, base):
        def tile_rows(t):
            return aligned(base + SUB * t)

        def eta_tile(t):
            rs = tile_rows(t)
            u, v = frame[TX, :, rs, :], frame[TY, :, rs, :]
            div = (u - west(u)) + (v - frame[TY, :, pl.ds(base + SUB * t - 1, SUB), :])
            eta = frame[ETA, :, rs, :] - coef[0, :, rs, :] * div
            frame[ETA, :, rs, :] = eta
            return u, v, eta

        last_row = iota((RING, SUB, LANES), 1) == SUB - 1
        following = eta_tile(0)
        for t in range(tiles):
            u, v, e = following
            if t + 1 < tiles:
                following = eta_tile(t + 1)
            e_n = jnp.where(last_row, pltpu.roll(following[2], SUB - 1, 1), pltpu.roll(e, SUB - 1, 1))
            rs = tile_rows(t)
            frame[TX, :, rs, :] = u + frame[FX, :, rs, :] - coef[1, :, rs, :] * (east(e) - e)
            frame[TY, :, rs, :] = v + frame[FY, :, rs, :] - coef[2, :, rs, :] * (e_n - e)
        chip_rows = aligned(FPAD + (M * ROWS - SHIFT) * chip, M * ROWS)
        acc[...] += stage[1, KMT, n // ROWS, pl.ds(lax.rem(n, ROWS), 1), :] * frame[pl.ds(0, RING), OWN, chip_rows, :]

    def subcycles(first, last, tiles, base):
        def block(b, carry):
            for j in range(SUB_BLOCK):
                subcycle(SUB_BLOCK * b + j, tiles, base)
            return carry

        lax.fori_loop(first // SUB_BLOCK, last // SUB_BLOCK, block, 0)

    turning = -(-max(sub_count - SHIFT, 0) // SUB_BLOCK) * SUB_BLOCK
    subcycles(0, turning, TILES, FPAD)
    subcycles(turning, sub_count, TILES - SHIFT // SUB, FPAD + SHIFT * chip)

    mine = aligned(ROWS * core, ROWS)
    theirs = aligned(ROWS * (1 - core), ROWS)
    result[...] = acc[:, :, theirs, :]
    swap = send(result, result_in, 30, swap_sem, row + 1 - 2 * core, col)
    swap.start()
    swap.wait_recv()
    for m in PAIR:
        whole = jnp.where(core == m, acc[:, :, mine, :], result_in[...])
        for lt in PAIR:
            ls = pl.ds(LANES * lt, LANES)
            eta_out[m, :, ls] = whole[ETA, lt]
            tx_out[m, :, ls] = whole[TX, lt]
            ty_out[m, :, ls] = whole[TY, lt]
            for d, out in enumerate((qu_out, qv_out)):
                depth = coef[1 + d, lt, own_rows, :]
                out[m, :, ls] = whole[TX + d, lt] / jnp.where(depth > 0.0, depth / WAVE_COURANT, 1.0) - sums[d, m, lt]
                nuv_out[d, :, ls] = nuv[d, lt]

    to_w.wait_send()
    to_e.wait_send()

    @pl.when(has_s)
    def _():
        to_s.wait_send()
        to_se.wait_send()
        to_s_later.wait_send()

    @pl.when(has_n)
    def _():
        to_n.wait_send()
        to_nw.wait_send()
        to_n_later.wait_send()

    for copy in sent:
        copy.wait_send()
    swap.wait_send()


def final_kernel(level_count, sol_u, sol_v, sol_t, sol_s, qu, qv, nuv, wet, eta_in, tx_in, ty_in,
                 eta_out, tx_out, ty_out, u_out, v_out, t_out, s_out, cubes, cube_sem):
    ratio = sweep_constants(level_count, DIFF_NUMBER)[1]
    strips = M * len(STRIPS)
    eta_out[...] = eta_in[...]
    tx_out[...] = tx_in[...]
    ty_out[...] = ty_in[...]

    def writes(s):
        m = s // 3
        rs = pl.ds(pl.multiple_of(SUB * (s - 3 * m), SUB), SUB)
        return m, rs, [pltpu.make_async_copy(cubes.at[f, s], dst.at[:, m, rs, :], cube_sem.at[f, s])
                       for f, dst in enumerate((t_out, s_out, u_out, v_out))]

    def strip(s, carry):
        m, rs, done = writes(s)
        for f, src in enumerate((sol_t, sol_s, sol_u, sol_v)):
            for lt in PAIR:
                ls = pl.ds(LANES * lt, LANES)
                if f < M:
                    n_wet = wet[rs, ls]
                    x = jnp.zeros(TILE, F32)
                    for k in reversed(range(level_count)):
                        e = src[k, m, lt, rs, :]
                        x = e + ratio[k] * jnp.where(n_wet > k + 1, x, e * (1.0 / (1.0 - ratio[k])))
                        cubes[f, s, k, :, ls] = jnp.where(n_wet > k, x, 0.0)
                else:
                    n, mean = nuv[f - M, rs, ls], (qu, qv)[f - M][m, rs, ls]
                    for k in range(level_count):
                        cubes[f, s, k, :, ls] = jnp.where(n > float(k), src[k, m, lt, rs, :] + mean, 0.0)
            done[f].start()
        return carry

    def finish(s, carry):
        for copy in writes(s)[-1]:
            copy.wait()
        return carry

    lax.fori_loop(0, strips, strip, 0)
    lax.fori_loop(0, strips, finish, 0)


def solution(mesh):
    col_count = mesh.shape["col"]

    def local_step(vel_x, vel_y, pot_temp, salinity, surf_eta, trans_x, trans_y, col_depth, wet_levels, avg_weights):
        L = vel_x.shape[0]
        N = avg_weights.shape[0]
        hbm_spec = pl.BlockSpec(memory_space=pltpu.HBM)
        vmem_spec = pl.BlockSpec(memory_space=pltpu.VMEM)
        cube = jax.ShapeDtypeStruct(vel_x.shape, F32)
        flat = jax.ShapeDtypeStruct(surf_eta.shape, F32)
        vm = lambda *shape: pltpu.VMEM(shape, F32)
        dma = lambda n: pltpu.SemaphoreType.DMA((n,))
        stage = pl.pallas_call(
            functools.partial(stage_kernel, N),
            out_shape=jax.ShapeDtypeStruct((M, 6, M, ROWS, LANES), F32),
            in_specs=[vmem_spec] * 5 + [pl.BlockSpec(memory_space=pltpu.SMEM)],
            out_specs=vmem_spec,
            name="ocean_stage",
        )(surf_eta, trans_x, trans_y, col_depth, wet_levels, avg_weights)
        *sol, qu, qv, nuv, eta_o, tx_o, ty_o = pl.pallas_call(
            functools.partial(step_kernel, col_count, L, N),
            out_shape=[jax.ShapeDtypeStruct((L, M, M, ROWS, LANES), F32)] * 4 + [flat] * 6,
            in_specs=[hbm_spec] * 4 + [vmem_spec],
            out_specs=[vmem_spec] * 10,
            scratch_shapes=[
                vm(4, L, M, RING, XR, LANES), *[vm(4, M, 8, LANES)] * 4, vm(5, M, M * L + 8, LANES), vm(4, M, M * L, LANES), vm(5, M, M * L + 8, LANES), vm(4, M, M * L, LANES),
                *[vm(M, 8, LANES)] * 2, vm(M, ROWS + 8, LANES), vm(M, M, ROWS, LANES), vm(M, M, M, ROWS, LANES),
                *[vm(4, ROWS, LANES)] * M,
                vm(M, M, M, ROWS, LANES), *[vm(M, ROWS, LANES)] * M, *[vm(4, ROWS, LANES)] * M,
                vm(6, RING, FRAME, LANES), vm(RING, RING, FRAME, LANES), vm(RING, M, M * ROWS, LANES), *[vm(RING, M, ROWS, LANES)] * M,
                pltpu.SMEM((4, L), F32), dma(8), dma(31), dma(8), *[dma(4)] * 6, pltpu.SemaphoreType.DMA],
            compiler_params=pltpu.CompilerParams(collective_id=0, has_side_effects=True, vmem_limit_bytes=STEP_VMEM),
            name="ocean_step",
        )(vel_x, vel_y, pot_temp, salinity, stage)
        outs = pl.pallas_call(
            functools.partial(final_kernel, L),
            out_shape=[flat] * 3 + [cube] * 4,
            in_specs=[vmem_spec] * 11,
            out_specs=[vmem_spec] * 3 + [hbm_spec] * 4,
            scratch_shapes=[vm(4, M * len(STRIPS), L, SUB, 256), pltpu.SemaphoreType.DMA((4, M * len(STRIPS)))],
            name="ocean_final",
            compiler_params=pltpu.CompilerParams(vmem_limit_bytes=FINAL_VMEM),
        )(*sol, qu, qv, nuv, wet_levels, eta_o, tx_o, ty_o)
        return tuple(outs)

    spec_3d = P(None, None, "row", "col")
    spec_2d = P(None, "row", "col")
    spec_map = P("row", "col")
    return jax.shard_map(local_step, mesh=mesh, in_specs=(spec_3d,) * 4 + (spec_2d,) * 3 + (spec_map,) * 2 + (P(),),
                         out_specs=(spec_2d,) * 3 + (spec_3d,) * 4, check_vma=False)
```

```python
import functools

import jax
import jax.numpy as jnp
from jax import lax
from jax.experimental import pallas as pl
from jax.experimental.pallas import tpu as pltpu
from jax.sharding import PartitionSpec as P

WAVE_COURANT = 0.4
THERM_EXP = 0.2
HALINE_CON = 0.15
PRESS_SCALE = 0.5
VISC_NUMBER = 1.0
DIFF_NUMBER = 0.5

MESH = pl.DeviceIdType.MESH
F32 = jnp.float32
ROWS = 24
PAD = 8
XR = ROWS + 2 * PAD
EDGE_BLOCK = 12
TRACER_BLOCK = 36
BACK_BLOCK = 36
SUB_BLOCK = 3
LEVEL_BLOCK = 36
LANES = 128
SUB = 8
TILE = (SUB, LANES)
PAIR, STRIPS, QUAD, OCTET = range(2), range(3), range(4), range(SUB)
RING = 3
M = 2
STEP_VMEM, FINAL_VMEM = 46 << 20, 9 << 20
TILES = 10
SHIFT = 16
FPAD = SHIFT + PAD
FRAME = 4 * ROWS + 2 * FPAD
HALO = 32


def sweep_constants(level_count, strength):
    inverse, ratio = [], []
    for k in range(level_count):
        pivot = 1.0 + strength if k == 0 else 1.0 + 2.0 * strength - strength * ratio[-1]
        inverse.append(1.0 / pivot)
        ratio.append(strength / pivot)
    return inverse, ratio


def iota(shape, axis):
    return lax.broadcasted_iota(jnp.int32, shape, axis)


def lanes(*lead):
    return iota((*lead, 8, 128), len(lead) + 1)


def turn(x, shift):
    return pltpu.roll(x, shift, x.ndim - 1)


def east(x):
    rolled = turn(x, 127)
    return jnp.where(lanes(3) == 127, jnp.concatenate([rolled[1:], rolled[:1]], axis=0), rolled)


def west(x):
    rolled = turn(x, 1)
    return jnp.where(lanes(3) == 0, jnp.concatenate([rolled[2:], rolled[:2]], axis=0), rolled)


def east_block(x):
    rolled = turn(x[:2], 127)
    return jnp.where(lanes(2) == 127, jnp.concatenate([rolled[1:], x[2:]], axis=0), rolled)


def west_block(x):
    rolled = turn(x[:2], 1)
    return jnp.where(lanes(2) == 0, jnp.concatenate([x[2:], rolled[:1]], axis=0), rolled)


STAGED = 6
ROOM = 240
ETA, TX, TY, DEPTH, PACK, KMT = range(STAGED)


def pack_2d(stage, count, put):
    lane = lanes()
    for i in STRIPS:
        rs = pl.ds(SUB * i, SUB)
        for m in PAIR:
            pack_w = pack_e = jnp.zeros(TILE, F32)
            for j in range(count):
                here = lane // HALO == j
                pack_w = jnp.where(here, turn(stage[m, j, 0, rs, :], HALO * j), pack_w)
                pack_e = jnp.where(here, turn(stage[m, j, 1, rs, :], (HALO * j + HALO) % LANES), pack_e)
            put(m, rs, pack_w, pack_e)


def stage_kernel(sub_count, eta, tx, ty, depth, wet_in, weights, out, stage, sem):
    for lt in PAIR:
        ls = pl.ds(LANES * lt, LANES)
        wet = wet_in[:, ls].astype(F32)
        masked = jnp.where(wet > 0.0, depth[:, ls], 0.0)
        stage[0, KMT, lt] = wet
        for m in PAIR:
            for j, field in ((ETA, eta), (TX, tx), (TY, ty)):
                stage[m, j, lt] = field[m, :, ls]
            stage[m, DEPTH, lt] = masked
    for n in range(sub_count):
        stage[1, KMT, n // ROWS, pl.ds(n % ROWS, 1), :] = jnp.full((1, LANES), weights[n], F32)

    def put(m, rs, pack_w, pack_e):
        stage[m, PACK, 0, rs, :] = pack_w
        stage[m, PACK, 1, rs, :] = pack_e

    pack_2d(stage, 4, put)
    copy = pltpu.make_async_copy(stage, out.at[:, pl.ds(0, STAGED)], sem)
    copy.start()
    copy.wait()


def step_kernel(
    col_count, level_count, sub_count,
    u_hbm, v_hbm, t_hbm, s_hbm, stage_hbm,
    sol_u, sol_v, sol_t, sol_s, qu_out, qv_out, nuv_out, eta_out, tx_out, ty_out,
    cube, stage,
    col_w, col_e, rcv_e, rcv_w, row_s, row_n, rcv_n, rcv_s, rcv_se, rcv_nw,
    kmt, nuv, sums, pk_e, pk_w, fstage, fstage_w, fstage_e, fpk_e, fpk_w,
    frame, coef, acc, result, result_in,
    table, load_sem, stage_sem, send_sem, edge_sem, row_sem, e_sem, w_sem, frow_sem, fe_sem, fw_sem, swap_sem,
):
    L = level_count
    U, V, T, S = range(4)
    sol = (sol_u, sol_v, sol_t, sol_s)
    FX, FY = 4, 5
    OWN = slice(0, 2)
    col = lax.axis_index("col")
    row = lax.axis_index("row")
    chip = row // 2
    core = row % 2
    east_col = lax.rem(col + 1, col_count)
    west_col = lax.rem(col + col_count - 1, col_count)
    peers = [lax.rem(row + d, 4) for d in (1, 2, 3)]
    lane = lanes()
    zero = jnp.zeros(TILE, F32)

    def aligned(start, size=8):
        return pl.ds(pl.multiple_of(start, 8), size)

    barrier = pltpu.get_barrier_semaphore()
    for r in peers:
        pl.semaphore_signal(barrier, inc=1, device_id={"row": r, "col": col}, device_id_type=MESH)
    for other in (east_col, west_col):
        for r in QUAD:
            pl.semaphore_signal(barrier, inc=1, device_id={"row": r, "col": other}, device_id_type=MESH)

    loads = []
    for f, src in enumerate((u_hbm, v_hbm, t_hbm, s_hbm)):
        for lt in PAIR:
            loads.append(pltpu.make_async_copy(
                src.at[:, :, :, pl.ds(LANES * lt, LANES)], cube.at[f, :, :, lt, pl.ds(PAD, ROWS), :], load_sem.at[2 * f + lt]))
            loads[-1].start()

    inv_v, ratio_v = sweep_constants(L, VISC_NUMBER)
    for n, line in enumerate((inv_v, ratio_v, [1.0 / (1.0 - r) for r in ratio_v], sweep_constants(L, DIFF_NUMBER)[0])):
        for k in range(L):
            table[n, k] = line[k]

    staged = pltpu.make_async_copy(stage_hbm.at[:, pl.ds(0, STAGED)], stage, stage_sem)
    staged.start()

    has_s, has_n = row > 0, row < 3

    @pl.when(row == 0)
    def _():
        rcv_s[...] = jnp.zeros(rcv_s.shape, F32)
        rcv_se[...] = jnp.zeros(rcv_se.shape, F32)

    @pl.when(row == 3)
    def _():
        rcv_n[...] = jnp.zeros(rcv_n.shape, F32)
        rcv_nw[...] = jnp.zeros(rcv_nw.shape, F32)

    outside = jnp.zeros((6, RING, PAD, LANES), F32)

    @pl.when(chip == 0)
    def _():
        frame[:, :, pl.ds(FPAD - PAD, PAD), :] = outside

    @pl.when(chip == 1)
    def _():
        frame[:, :, pl.ds(FPAD + SUB * TILES, PAD), :] = outside


    lane42 = lanes(4, 2)
    lane2 = lanes(M)
    empty = jnp.zeros((M, SUB, LANES), F32)
    for f in QUAD:
        for copy in loads[2 * f:2 * f + 2]:
            copy.wait()

        def pack(g, carry):
            west_pack, east_pack = carry
            for k, i in [(EDGE_BLOCK * g + j, i) for j in range(EDGE_BLOCK) for i in STRIPS]:
                slot = L * i + k
                rs = pl.ds(PAD + SUB * i, SUB)
                west_pack = jnp.where(lane2 == slot, turn(cube[f, k, :, 0, rs, :], slot), west_pack)
                east_pack = jnp.where(lane2 == slot, turn(cube[f, k, :, 1, rs, :], slot + 1), east_pack)
            for q in range(M * EDGE_BLOCK // SUB):
                rows = aligned(M * EDGE_BLOCK * g + SUB * q)
                low = high = empty
                for j in OCTET:
                    k, m = EDGE_BLOCK * g + (SUB * q + j) // M, j % M
                    low = jnp.where(sub2 == j, cube[f, k, m, OWN, pl.ds(PAD - j, SUB), :], low)
                    high = jnp.where(sub2 == j, cube[f, k, m, OWN, pl.ds(PAD + ROWS - 1 - j, SUB), :], high)
                row_n[f, :, rows, :] = high
                row_s[f if f < T else f + 1, :, rows, :] = low
                if f == S:
                    row_s[T, :, rows, :] = row_s[T + 1, :, rows, :] - (HALINE_CON / THERM_EXP) * low
            return west_pack, east_pack

        sub2 = iota((M, SUB, LANES), 1)
        col_w[f], col_e[f] = lax.fori_loop(0, L // EDGE_BLOCK, pack, (empty, empty))
    staged.wait()
    kmt[:, pl.ds(0, ROWS), :] = stage[0, KMT]
    for i in STRIPS:
        slot = 3 * L + i
        col_w[0, 0] = jnp.where(lane == slot, turn(kmt[0, pl.ds(SUB * i, SUB), :], slot), col_w[0, 0])
    row_s[U, :, pl.ds(M * L, SUB), :] = kmt[:, pl.ds(0, SUB), :]

    pl.semaphore_wait(barrier, 11)

    def send(src, dst, ssem, rsem, r, c):
        return pltpu.make_async_remote_copy(
            src_ref=src, dst_ref=dst, send_sem=send_sem.at[ssem], recv_sem=rsem, device_id={"row": r, "col": c}, device_id_type=MESH)

    def frame_rows(r, at_chip):
        return aligned(FPAD + ROWS * r - SHIFT * at_chip, ROWS)

    own_rows = frame_rows(row, chip)
    south, north = jnp.maximum(row - 1, 0), jnp.minimum(row + 1, 3)
    to_w = send(col_w, rcv_e, 0, edge_sem.at[0], row, west_col)
    to_e = send(col_e, rcv_w, 1, edge_sem.at[1], row, east_col)
    first_s, first_n = pl.ds(0, 3), pl.ds(0, 2)
    later_s, later_n = pl.ds(3, 2), pl.ds(2, 2)
    to_s = send(row_s.at[first_s], rcv_n.at[first_s], 2, edge_sem.at[2], south, col)
    to_n = send(row_n.at[first_n], rcv_s.at[first_n], 3, edge_sem.at[3], north, col)
    to_s_later = send(row_s.at[later_s], rcv_n.at[later_s], 6, edge_sem.at[6], south, col)
    to_n_later = send(row_n.at[later_n], rcv_s.at[later_n], 7, edge_sem.at[7], north, col)
    to_nw = send(col_w.at[V], rcv_se, 4, edge_sem.at[4], north, west_col)
    to_se = send(col_e.at[U], rcv_nw, 5, edge_sem.at[5], south, east_col)
    to_w.start()
    to_e.start()

    @pl.when(has_s)
    def _():
        to_s.start()
        to_se.start()
        to_s_later.start()

    @pl.when(has_n)
    def _():
        to_n.start()
        to_nw.start()
        to_n_later.start()

    def exchange(block, pack_w, pack_e, first, count, base, rsem, esem, wsem, pe, pw):
        out = []
        for d, r in enumerate(peers):
            out.append(send(block(r % 2), frame.at[pl.ds(first, count), OWN, frame_rows(row, r // 2), :], base + d, rsem.at[row], r, col))
        for r in QUAD:
            out.append(send(pack_w(r % 2), pe.at[row], base + 3 + 2 * r, esem.at[row], r, west_col))
            out.append(send(pack_e(r % 2), pw.at[row], base + 4 + 2 * r, wsem.at[row], r, east_col))
        for copy in out:
            copy.start()
        frame[pl.ds(first, count), OWN, own_rows, :] = block(core)[...]
        return out

    def collect(block, pack_w, first, count, rsem, esem, wsem, pe, pw):
        for r in peers:
            rows = frame_rows(r, chip)
            send(block(0), frame.at[pl.ds(first, count), OWN, rows, :], 0, rsem.at[r], r, col).wait_recv()
        for r in QUAD:
            send(pack_w(0), pe.at[r], 0, esem.at[r], r, east_col).wait_recv()
            send(pack_w(0), pw.at[r], 0, wsem.at[r], r, west_col).wait_recv()
        side = lax.broadcasted_iota(jnp.int32, (ROWS, 128), 1) // HALO
        for r in QUAD:
            for j in range(count):
                frame[first + j, 2, frame_rows(r, chip), :] = jnp.where(
                    side == 0, turn(pe[r], (128 - HALO * j) % 128), jnp.where(side == 3, turn(pw[r], (128 - HALO * j - HALO) % 128), 0.0))

    def stage_block(m):
        return stage.at[m, pl.ds(0, PACK)]

    def stage_w(m):
        return stage.at[m, PACK, 0]

    def stage_e(m):
        return stage.at[m, PACK, 1]

    to_w.wait_recv()
    to_e.wait_recv()

    def unpack(g, carry):
        from_e, from_w = rcv_e[...], rcv_w[...]
        for k in [EDGE_BLOCK * g + j for j in range(EDGE_BLOCK)]:
            for i in STRIPS:
                slot = L * i + k
                cube[:, k, :, 2, pl.ds(PAD + SUB * i, SUB), :] = jnp.where(
                    lane42 < 64, turn(from_w, lax.rem(128 - slot, 128)), turn(from_e, 127 - slot))
        return carry

    lax.fori_loop(0, L // EDGE_BLOCK, unpack, 0)

    def masks(i):
        rs = pl.ds(SUB * i, SUB)
        wet = kmt[:, rs, :]
        halo = turn(rcv_e[0, 0], 127 - (3 * L + i))
        nuv[0, :, rs, :] = jnp.minimum(wet, east_block(jnp.concatenate([wet, halo[None]], axis=0)))
        nuv[1, :, rs, :] = jnp.minimum(wet, kmt[:, pl.ds(8 * i + 1, 8), :])

    masks(0)
    masks(1)

    press = PRESS_SCALE / L
    pair = jnp.zeros((M, SUB, LANES), F32)

    def for_strips(body, init, strips=(0, 1, 3), levels=LEVEL_BLOCK):
        start, step, count = strips

        def strip(s, carry):
            m = s // count
            i = start + step * (s - count * m)
            rs = aligned(SUB * i)

            def get(f, k, part, d=0):
                start = PAD + 8 * i + d
                return cube[f, k, m, part, pl.ds(start if d else pl.multiple_of(start, 8), 8), :]

            state, finish = init(m, rs)

            def block(b, state):
                for j in range(levels):
                    k = b * levels + j
                    state = body(k, m, rs, get, state)
                return state

            finish(m, rs, lax.fori_loop(0, L // levels, block, state))
            return carry

        lax.fori_loop(0, M * count, strip, 0)

    def momentum_init(m, rs):
        return (pair,) * 6, momentum_finish

    def momentum_finish(m, rs, state):
        sums[0, m, :, rs, :] = state[4]
        sums[1, m, :, rs, :] = state[5]

    def momentum(k, m, rs, get, state):
        cx, cy, eu, ev, gu_sum, gv_sum = state
        level = k.astype(F32)
        both = slice(0, 3)
        u, v, un, vs = get(U, k, both), get(V, k, both), get(U, k, both, 1), get(V, k, both, -1)
        rho = (press * HALINE_CON) * get(S, k, both) - (press * THERM_EXP) * get(T, k, both)
        dx = rho[OWN] - east_block(rho)
        dy = rho[OWN] - ((press * HALINE_CON) * get(S, k, OWN, 1) - (press * THERM_EXP) * get(T, k, OWN, 1))
        vsum, usum = v + vs, u + un
        cx, cy = cx + dx, cy + dy
        gu = cx - 0.5 * (dx + u[OWN] * (east_block(u) - west_block(u))) - 0.125 * (
            (vsum[OWN] + east_block(vsum)) * (un[OWN] - get(U, k, OWN, -1)))
        gv = cy - 0.5 * (dy + v[OWN] * (get(V, k, OWN, 1) - vs[OWN])) - 0.125 * (
            (usum[OWN] + west_block(usum)) * (east_block(v) - west_block(v)))
        gu = jnp.where(nuv[0, :, rs, :] > level, gu, 0.0)
        gv = jnp.where(nuv[1, :, rs, :] > level, gv, 0.0)
        inverse = table[0, k]
        eu = (u[OWN] + gu + VISC_NUMBER * eu) * inverse
        ev = (v[OWN] + gv + VISC_NUMBER * ev) * inverse
        sol[U][k, m, :, rs, :] = eu
        sol[V][k, m, :, rs, :] = ev
        return cx, cy, eu, ev, gu_sum + gu, gv_sum + gv

    for_strips(momentum, momentum_init, strips=(1, 1, 1))

    @pl.when(has_n)
    def _():
        to_s.wait_recv()
        to_se.wait_recv()

    @pl.when(has_s)
    def _():
        to_n.wait_recv()
        to_nw.wait_recv()

    sent = exchange(stage_block, stage_w, stage_e, ETA, 4, 8, row_sem, e_sem, w_sem, pk_e, pk_w)

    def unpack_rows(g, carry):
        rows = aligned(SUB * g)
        below, above = rcv_s[:T, :, rows, :], rcv_n[:S, :, rows, :]
        for j in OCTET:
            k, m = 4 * g + j // 2, j % 2
            cube[:T, k, m, OWN, pl.ds(PAD - 1, 1), :] = below[:, :, j:j + 1, :]
            cube[:S, k, m, OWN, pl.ds(PAD + ROWS, 1), :] = above[:, :, j:j + 1, :]
            cube[S, k, m, OWN, pl.ds(PAD + ROWS, 1), :] = jnp.zeros((M, 1, LANES), F32)
            if m:
                cube[V, k, :, 2, pl.ds(0, PAD), :] = turn(rcv_se[...], 127 - 2 * L - k)
                cube[U, k, :, 2, pl.ds(PAD + ROWS, PAD), :] = turn(rcv_nw[...], lax.rem(128 - k, 128))
        return carry

    def unpack_rows_later(g, carry):
        rows = aligned(SUB * g)
        below, above = rcv_s[T:, :, rows, :], rcv_n[S:, :, rows, :]
        for j in OCTET:
            k, m = 4 * g + j // 2, j % 2
            cube[T:, k, m, OWN, pl.ds(PAD - 1, 1), :] = below[:, :, j:j + 1, :]
            cube[T:, k, m, OWN, pl.ds(PAD + ROWS, 1), :] = above[:, :, j:j + 1, :]
        return carry

    lax.fori_loop(0, L // 4, unpack_rows, 0)
    kmt[:, pl.ds(ROWS, 8), :] = rcv_n[U, :, pl.ds(M * L, SUB), :]
    masks(2)
    for_strips(momentum, momentum_init, strips=(0, 2, 2))

    collect(stage_block, stage_w, ETA, 4, row_sem, e_sem, w_sem, pk_e, pk_w)

    def coefficients(i, carry):
        rs = aligned(FPAD + SUB * i)
        depth = frame[DEPTH, :, rs, :]
        depth_e = east(depth)
        depth_n = frame[DEPTH, :, pl.ds(FPAD + SUB * i + 1, SUB), :]
        wet = depth > 0.0
        coef[0, :, rs, :] = jnp.where(wet, WAVE_COURANT, 0.0)
        coef[1, :, rs, :] = jnp.where(wet & (depth_e > 0.0), (0.5 * WAVE_COURANT) * (depth + depth_e), 0.0)
        coef[2, :, rs, :] = jnp.where(wet & (depth_n > 0.0), (0.5 * WAVE_COURANT) * (depth + depth_n), 0.0)
        return carry

    lax.fori_loop(0, TILES, coefficients, 0)

    for d in PAIR:
        scale = coef[1 + d, OWN, own_rows, :] / (jnp.maximum(nuv[d], 1.0) * (WAVE_COURANT * sub_count))
        for m in PAIR:
            fstage[m, d] = scale * sums[d, m]

    def put(m, rs, pack_w, pack_e):
        fstage_w[m, rs, :] = pack_w
        fstage_e[m, rs, :] = pack_e

    pack_2d(fstage, 2, put)
    sent += exchange(lambda m: fstage.at[m], lambda m: fstage_w.at[m], lambda m: fstage_e.at[m], FX, 2, 19, frow_sem, fe_sem, fw_sem, fpk_e, fpk_w)

    block_zero = jnp.zeros((M, ROWS, LANES), F32)

    def back(m, carry):
        def levels_back(b, state):
            x, total = list(state[:2]), list(state[2:])
            for j in range(BACK_BLOCK):
                k = L - 1 - (b * BACK_BLOCK + j)
                level = k.astype(F32)
                for d in PAIR:
                    e, n = sol[d][k, m], nuv[d]
                    x[d] = e + table[1, k] * jnp.where(n > level + 1.0, x[d], e * table[2, k])
                    sol[d][k, m] = x[d]
                    total[d] = total[d] + jnp.where(n > level, x[d], 0.0)
            return (*x, *total)

        state = lax.fori_loop(0, L // BACK_BLOCK, levels_back, (block_zero,) * 4)
        for d in PAIR:
            sums[d, m] = state[2 + d] / jnp.maximum(nuv[d], 1.0)
        return carry

    lax.fori_loop(0, M, back, 0)

    def tracer_init(m, rs):
        return pair, lambda *a: None

    def tracer(f):
        def body(k, m, rs, get, e):
            t, u = get(f, k, slice(0, 3)), get(U, k, slice(0, 3))
            fx = u * (t + jnp.concatenate([east_block(t), t[:1]], axis=0))
            t = t[OWN]
            gain = fx[OWN] - west_block(fx) + (get(V, k, OWN) * (t + get(f, k, OWN, 1)) - get(V, k, OWN, -1) * (t + get(f, k, OWN, -1)))
            e = (jnp.where(kmt[:, rs, :] > k.astype(F32), t - 0.5 * gain, 0.0) + DIFF_NUMBER * e) * table[3, k]
            sol[f][k, m, :, rs, :] = e
            return e

        return body

    @pl.when(has_n)
    def _():
        to_s_later.wait_recv()

    @pl.when(has_s)
    def _():
        to_n_later.wait_recv()

    lax.fori_loop(0, L // 4, unpack_rows_later, 0)
    for f in (T, S):
        for_strips(tracer(f), tracer_init, levels=TRACER_BLOCK)
    acc[...] = jnp.zeros(acc.shape, F32)

    collect(lambda m: fstage.at[m], lambda m: fstage_w.at[m], FX, 2, frow_sem, fe_sem, fw_sem, fpk_e, fpk_w)

    def subcycle(n, tiles, base):
        def tile_rows(t):
            return aligned(base + SUB * t)

        def eta_tile(t):
            rs = tile_rows(t)
            u, v = frame[TX, :, rs, :], frame[TY, :, rs, :]
            div = (u - west(u)) + (v - frame[TY, :, pl.ds(base + SUB * t - 1, SUB), :])
            eta = frame[ETA, :, rs, :] - coef[0, :, rs, :] * div
            frame[ETA, :, rs, :] = eta
            return u, v, eta

        last_row = iota((RING, SUB, LANES), 1) == SUB - 1
        following = eta_tile(0)
        for t in range(tiles):
            u, v, e = following
            if t + 1 < tiles:
                following = eta_tile(t + 1)
            e_n = jnp.where(last_row, pltpu.roll(following[2], SUB - 1, 1), pltpu.roll(e, SUB - 1, 1))
            rs = tile_rows(t)
            frame[TX, :, rs, :] = u + frame[FX, :, rs, :] - coef[1, :, rs, :] * (east(e) - e)
            frame[TY, :, rs, :] = v + frame[FY, :, rs, :] - coef[2, :, rs, :] * (e_n - e)
        chip_rows = aligned(FPAD + (M * ROWS - SHIFT) * chip, M * ROWS)
        acc[...] += stage[1, KMT, n // ROWS, pl.ds(lax.rem(n, ROWS), 1), :] * frame[pl.ds(0, RING), OWN, chip_rows, :]

    def subcycles(first, last, tiles, base):
        def block(b, carry):
            for j in range(SUB_BLOCK):
                subcycle(SUB_BLOCK * b + j, tiles, base)
            return carry

        lax.fori_loop(first // SUB_BLOCK, last // SUB_BLOCK, block, 0)

    turning = -(-max(sub_count - SHIFT, 0) // SUB_BLOCK) * SUB_BLOCK
    subcycles(0, turning, TILES, FPAD)
    subcycles(turning, sub_count, TILES - SHIFT // SUB, FPAD + SHIFT * chip)

    mine = aligned(ROWS * core, ROWS)
    theirs = aligned(ROWS * (1 - core), ROWS)
    result[...] = acc[:, :, theirs, :]
    swap = send(result, result_in, 30, swap_sem, row + 1 - 2 * core, col)
    swap.start()
    swap.wait_recv()
    for m in PAIR:
        whole = jnp.where(core == m, acc[:, :, mine, :], result_in[...])
        for lt in PAIR:
            ls = pl.ds(LANES * lt, LANES)
            eta_out[m, :, ls] = whole[ETA, lt]
            tx_out[m, :, ls] = whole[TX, lt]
            ty_out[m, :, ls] = whole[TY, lt]
            for d, out in enumerate((qu_out, qv_out)):
                depth = coef[1 + d, lt, own_rows, :]
                out[m, :, ls] = whole[TX + d, lt] / jnp.where(depth > 0.0, depth / WAVE_COURANT, 1.0) - sums[d, m, lt]
                nuv_out[d, :, ls] = nuv[d, lt]

    to_w.wait_send()
    to_e.wait_send()

    @pl.when(has_s)
    def _():
        to_s.wait_send()
        to_se.wait_send()
        to_s_later.wait_send()

    @pl.when(has_n)
    def _():
        to_n.wait_send()
        to_nw.wait_send()
        to_n_later.wait_send()

    for copy in sent:
        copy.wait_send()
    swap.wait_send()


def final_kernel(level_count, sol_u, sol_v, sol_t, sol_s, qu, qv, nuv, wet, eta_in, tx_in, ty_in,
                 eta_out, tx_out, ty_out, u_out, v_out, t_out, s_out, cubes, cube_sem, plane_sem):
    ratio = sweep_constants(level_count, DIFF_NUMBER)[1]
    strips = M * len(STRIPS)
    passed = [pltpu.make_async_copy(src, dst, plane_sem.at[n])
              for n, (src, dst) in enumerate(((eta_in, eta_out), (tx_in, tx_out), (ty_in, ty_out)))]
    for copy in passed:
        copy.start()

    def writes(s):
        m = s // 3
        rs = pl.ds(pl.multiple_of(SUB * (s - 3 * m), SUB), SUB)
        return m, rs, [pltpu.make_async_copy(cubes.at[f, s], dst.at[:, m, rs, :], cube_sem.at[f, s])
                       for f, dst in enumerate((t_out, s_out, u_out, v_out))]

    def strip(s, carry):
        m, rs, done = writes(s)
        for f, src in enumerate((sol_t, sol_s, sol_u, sol_v)):
            for lt in PAIR:
                ls = pl.ds(LANES * lt, LANES)
                if f < M:
                    n_wet = wet[rs, ls]
                    x = jnp.zeros(TILE, F32)
                    for k in reversed(range(level_count)):
                        e = src[k, m, lt, rs, :]
                        x = e + ratio[k] * jnp.where(n_wet > k + 1, x, e * (1.0 / (1.0 - ratio[k])))
                        cubes[f, s, k, :, ls] = jnp.where(n_wet > k, x, 0.0)
                else:
                    n, mean = nuv[f - M, rs, ls], (qu, qv)[f - M][m, rs, ls]
                    for k in range(level_count):
                        cubes[f, s, k, :, ls] = jnp.where(n > float(k), src[k, m, lt, rs, :] + mean, 0.0)
            done[f].start()
        return carry

    def finish(s, carry):
        for copy in writes(s)[-1]:
            copy.wait()
        return carry

    lax.fori_loop(0, strips, strip, 0)
    lax.fori_loop(0, strips, finish, 0)
    for copy in passed:
        copy.wait()


def solution(mesh):
    col_count = mesh.shape["col"]

    def local_step(vel_x, vel_y, pot_temp, salinity, surf_eta, trans_x, trans_y, col_depth, wet_levels, avg_weights):
        L = vel_x.shape[0]
        N = avg_weights.shape[0]
        hbm_spec = pl.BlockSpec(memory_space=pltpu.HBM)
        vmem_spec = pl.BlockSpec(memory_space=pltpu.VMEM)
        cube = jax.ShapeDtypeStruct(vel_x.shape, F32)
        flat = jax.ShapeDtypeStruct(surf_eta.shape, F32)
        vm = lambda *shape: pltpu.VMEM(shape, F32)
        dma = lambda n: pltpu.SemaphoreType.DMA((n,))
        stage = pl.pallas_call(
            functools.partial(stage_kernel, N),
            out_shape=jax.ShapeDtypeStruct((M, ROOM, M, ROWS, LANES), F32),
            in_specs=[vmem_spec] * 5 + [pl.BlockSpec(memory_space=pltpu.SMEM)],
            out_specs=hbm_spec,
            scratch_shapes=[vm(M, STAGED, M, ROWS, LANES), pltpu.SemaphoreType.DMA],
            name="ocean_stage",
        )(surf_eta, trans_x, trans_y, col_depth, wet_levels, avg_weights)
        *sol, qu, qv, nuv, eta_o, tx_o, ty_o = pl.pallas_call(
            functools.partial(step_kernel, col_count, L, N),
            out_shape=[jax.ShapeDtypeStruct((L, M, M, ROWS, LANES), F32)] * 4 + [flat] * 6,
            in_specs=[hbm_spec] * 5,
            out_specs=[vmem_spec] * 10,
            scratch_shapes=[
                vm(4, L, M, RING, XR, LANES), vm(M, STAGED, M, ROWS, LANES), *[vm(4, M, 8, LANES)] * 4, vm(5, M, M * L + 8, LANES), vm(4, M, M * L, LANES), vm(5, M, M * L + 8, LANES), vm(4, M, M * L, LANES),
                *[vm(M, 8, LANES)] * 2, vm(M, ROWS + 8, LANES), vm(M, M, ROWS, LANES), vm(M, M, M, ROWS, LANES),
                *[vm(4, ROWS, LANES)] * M,
                vm(M, M, M, ROWS, LANES), *[vm(M, ROWS, LANES)] * M, *[vm(4, ROWS, LANES)] * M,
                vm(6, RING, FRAME, LANES), vm(RING, RING, FRAME, LANES), vm(RING, M, M * ROWS, LANES), *[vm(RING, M, ROWS, LANES)] * M,
                pltpu.SMEM((4, L), F32), dma(8), pltpu.SemaphoreType.DMA, dma(31), dma(8), *[dma(4)] * 6, pltpu.SemaphoreType.DMA],
            compiler_params=pltpu.CompilerParams(collective_id=0, has_side_effects=True, vmem_limit_bytes=STEP_VMEM),
            name="ocean_step",
        )(vel_x, vel_y, pot_temp, salinity, stage)
        outs = pl.pallas_call(
            functools.partial(final_kernel, L),
            out_shape=[flat] * 3 + [cube] * 4,
            in_specs=[vmem_spec] * 11,
            out_specs=[hbm_spec] * 7,
            scratch_shapes=[vm(4, M * len(STRIPS), L, SUB, 256), pltpu.SemaphoreType.DMA((4, M * len(STRIPS))), dma(3)],
            name="ocean_final",
            compiler_params=pltpu.CompilerParams(vmem_limit_bytes=FINAL_VMEM),
        )(*sol, qu, qv, nuv, wet_levels, eta_o, tx_o, ty_o)
        return tuple(outs)

    spec_3d = P(None, None, "row", "col")
    spec_2d = P(None, "row", "col")
    spec_map = P("row", "col")
    return jax.shard_map(local_step, mesh=mesh, in_specs=(spec_3d,) * 4 + (spec_2d,) * 3 + (spec_map,) * 2 + (P(),),
                         out_specs=(spec_2d,) * 3 + (spec_3d,) * 4, check_vma=False)
```

```python
import functools

import jax
import jax.numpy as jnp
from jax import lax
from jax.experimental import pallas as pl
from jax.experimental.pallas import tpu as pltpu
from jax.sharding import PartitionSpec as P

WAVE_COURANT = 0.4
THERM_EXP = 0.2
HALINE_CON = 0.15
PRESS_SCALE = 0.5
VISC_NUMBER = 1.0
DIFF_NUMBER = 0.5

MESH = pl.DeviceIdType.MESH
F32 = jnp.float32
ROWS = 24
PAD = 8
XR = ROWS + 2 * PAD
EDGE_BLOCK = 12
TRACER_BLOCK = 36
BACK_BLOCK = 36
SUB_BLOCK = 5
LEVEL_BLOCK = 36
LANES = 128
SUB = 8
TILE = (SUB, LANES)
PAIR, STRIPS, QUAD, OCTET = range(2), range(3), range(4), range(SUB)
RING = 3
M = 2
STEP_VMEM, FINAL_VMEM = 46 << 20, 9 << 20
TILES = 10
SHIFT = 16
FPAD = SHIFT + PAD
FRAME = 4 * ROWS + 2 * FPAD
HALO = 32


def sweep_constants(level_count, strength):
    inverse, ratio = [], []
    for k in range(level_count):
        pivot = 1.0 + strength if k == 0 else 1.0 + 2.0 * strength - strength * ratio[-1]
        inverse.append(1.0 / pivot)
        ratio.append(strength / pivot)
    return inverse, ratio


def iota(shape, axis):
    return lax.broadcasted_iota(jnp.int32, shape, axis)


def lanes(*lead):
    return iota((*lead, 8, 128), len(lead) + 1)


def turn(x, shift):
    return pltpu.roll(x, shift, x.ndim - 1)


def east(x):
    rolled = turn(x, 127)
    return jnp.where(lanes(3) == 127, jnp.concatenate([rolled[1:], rolled[:1]], axis=0), rolled)


def west(x):
    rolled = turn(x, 1)
    return jnp.where(lanes(3) == 0, jnp.concatenate([rolled[2:], rolled[:2]], axis=0), rolled)


def east_block(x):
    rolled = turn(x[..., :2, :, :], 127)
    following = jnp.concatenate([rolled[..., 1:, :, :], x[..., 2:, :, :]], axis=-3)
    return jnp.where(iota(rolled.shape, x.ndim - 1) == 127, following, rolled)


def west_block(x):
    rolled = turn(x[..., :2, :, :], 1)
    before = jnp.concatenate([x[..., 2:, :, :], rolled[..., :1, :, :]], axis=-3)
    return jnp.where(iota(rolled.shape, x.ndim - 1) == 0, before, rolled)


STAGED = 6
ROOM = 240
ETA, TX, TY, DEPTH, PACK, KMT = range(STAGED)


def pack_2d(stage, count, put):
    lane = lanes()
    for i in STRIPS:
        rs = pl.ds(SUB * i, SUB)
        for m in PAIR:
            pack_w = pack_e = jnp.zeros(TILE, F32)
            for j in range(count):
                here = lane // HALO == j
                pack_w = jnp.where(here, turn(stage[m, j, 0, rs, :], HALO * j), pack_w)
                pack_e = jnp.where(here, turn(stage[m, j, 1, rs, :], (HALO * j + HALO) % LANES), pack_e)
            put(m, rs, pack_w, pack_e)


def stage_kernel(sub_count, eta, tx, ty, depth, wet_in, weights, out, stage, sem):
    for lt in PAIR:
        ls = pl.ds(LANES * lt, LANES)
        wet = wet_in[:, ls].astype(F32)
        masked = jnp.where(wet > 0.0, depth[:, ls], 0.0)
        stage[0, KMT, lt] = wet
        for m in PAIR:
            for j, field in ((ETA, eta), (TX, tx), (TY, ty)):
                stage[m, j, lt] = field[m, :, ls]
            stage[m, DEPTH, lt] = masked
    for n in range(sub_count):
        stage[1, KMT, n // ROWS, pl.ds(n % ROWS, 1), :] = jnp.full((1, LANES), weights[n], F32)

    def put(m, rs, pack_w, pack_e):
        stage[m, PACK, 0, rs, :] = pack_w
        stage[m, PACK, 1, rs, :] = pack_e

    pack_2d(stage, 4, put)
    copy = pltpu.make_async_copy(stage, out.at[:, pl.ds(0, STAGED)], sem)
    copy.start()
    copy.wait()


def step_kernel(
    col_count, level_count, sub_count,
    u_hbm, v_hbm, t_hbm, s_hbm, stage_hbm,
    sol_u, sol_v, sol_t, sol_s, qu_out, qv_out, nuv_out, eta_out, tx_out, ty_out,
    cube, stage,
    col_w, col_e, rcv_e, rcv_w, row_s, row_n, rcv_n, rcv_s, rcv_se, rcv_nw,
    kmt, nuv, sums, pk_e, pk_w, fstage, fstage_w, fstage_e, fpk_e, fpk_w,
    frame, coef, acc, result, result_in,
    table, load_sem, stage_sem, send_sem, edge_sem, row_sem, e_sem, w_sem, frow_sem, fe_sem, fw_sem, swap_sem,
):
    L = level_count
    U, V, T, S = range(4)
    sol = (sol_u, sol_v, sol_t, sol_s)
    FX, FY = 4, 5
    OWN = slice(0, 2)
    col = lax.axis_index("col")
    row = lax.axis_index("row")
    chip = row // 2
    core = row % 2
    east_col = lax.rem(col + 1, col_count)
    west_col = lax.rem(col + col_count - 1, col_count)
    peers = [lax.rem(row + d, 4) for d in (1, 2, 3)]
    lane = lanes()
    zero = jnp.zeros(TILE, F32)

    def aligned(start, size=8):
        return pl.ds(pl.multiple_of(start, 8), size)

    barrier = pltpu.get_barrier_semaphore()
    for r in peers:
        pl.semaphore_signal(barrier, inc=1, device_id={"row": r, "col": col}, device_id_type=MESH)
    for other in (east_col, west_col):
        for r in QUAD:
            pl.semaphore_signal(barrier, inc=1, device_id={"row": r, "col": other}, device_id_type=MESH)

    loads = []
    for f, src in enumerate((u_hbm, v_hbm, t_hbm, s_hbm)):
        for lt in PAIR:
            loads.append(pltpu.make_async_copy(
                src.at[:, :, :, pl.ds(LANES * lt, LANES)], cube.at[f, :, :, lt, pl.ds(PAD, ROWS), :], load_sem.at[2 * f + lt]))
            loads[-1].start()

    inv_v, ratio_v = sweep_constants(L, VISC_NUMBER)
    for n, line in enumerate((inv_v, ratio_v, [1.0 / (1.0 - r) for r in ratio_v], sweep_constants(L, DIFF_NUMBER)[0])):
        for k in range(L):
            table[n, k] = line[k]

    staged = pltpu.make_async_copy(stage_hbm.at[:, pl.ds(0, STAGED)], stage, stage_sem)
    staged.start()

    has_s, has_n = row > 0, row < 3

    @pl.when(row == 0)
    def _():
        rcv_s[...] = jnp.zeros(rcv_s.shape, F32)
        rcv_se[...] = jnp.zeros(rcv_se.shape, F32)

    @pl.when(row == 3)
    def _():
        rcv_n[...] = jnp.zeros(rcv_n.shape, F32)
        rcv_nw[...] = jnp.zeros(rcv_nw.shape, F32)

    outside = jnp.zeros((6, RING, PAD, LANES), F32)

    @pl.when(chip == 0)
    def _():
        frame[:, :, pl.ds(FPAD - PAD, PAD), :] = outside

    @pl.when(chip == 1)
    def _():
        frame[:, :, pl.ds(FPAD + SUB * TILES, PAD), :] = outside


    lane42 = lanes(4, 2)
    lane2 = lanes(M)
    empty = jnp.zeros((M, SUB, LANES), F32)
    for f in QUAD:
        for copy in loads[2 * f:2 * f + 2]:
            copy.wait()

        def pack(g, carry):
            west_pack, east_pack = carry
            for k, i in [(EDGE_BLOCK * g + j, i) for j in range(EDGE_BLOCK) for i in STRIPS]:
                slot = L * i + k
                rs = pl.ds(PAD + SUB * i, SUB)
                west_pack = jnp.where(lane2 == slot, turn(cube[f, k, :, 0, rs, :], slot), west_pack)
                east_pack = jnp.where(lane2 == slot, turn(cube[f, k, :, 1, rs, :], slot + 1), east_pack)
            for q in range(M * EDGE_BLOCK // SUB):
                rows = aligned(M * EDGE_BLOCK * g + SUB * q)
                low = high = empty
                for j in OCTET:
                    k, m = EDGE_BLOCK * g + (SUB * q + j) // M, j % M
                    low = jnp.where(sub2 == j, cube[f, k, m, OWN, pl.ds(PAD - j, SUB), :], low)
                    high = jnp.where(sub2 == j, cube[f, k, m, OWN, pl.ds(PAD + ROWS - 1 - j, SUB), :], high)
                row_n[f, :, rows, :] = high
                row_s[f if f < T else f + 1, :, rows, :] = low
                if f == S:
                    row_s[T, :, rows, :] = row_s[T + 1, :, rows, :] - (HALINE_CON / THERM_EXP) * low
            return west_pack, east_pack

        sub2 = iota((M, SUB, LANES), 1)
        col_w[f], col_e[f] = lax.fori_loop(0, L // EDGE_BLOCK, pack, (empty, empty))
    staged.wait()
    kmt[:, pl.ds(0, ROWS), :] = stage[0, KMT]
    for i in STRIPS:
        slot = 3 * L + i
        col_w[0, 0] = jnp.where(lane == slot, turn(kmt[0, pl.ds(SUB * i, SUB), :], slot), col_w[0, 0])
    row_s[U, :, pl.ds(M * L, SUB), :] = kmt[:, pl.ds(0, SUB), :]

    pl.semaphore_wait(barrier, 11)

    def send(src, dst, ssem, rsem, r, c):
        return pltpu.make_async_remote_copy(
            src_ref=src, dst_ref=dst, send_sem=send_sem.at[ssem], recv_sem=rsem, device_id={"row": r, "col": c}, device_id_type=MESH)

    def frame_rows(r, at_chip):
        return aligned(FPAD + ROWS * r - SHIFT * at_chip, ROWS)

    own_rows = frame_rows(row, chip)
    south, north = jnp.maximum(row - 1, 0), jnp.minimum(row + 1, 3)
    to_w = send(col_w, rcv_e, 0, edge_sem.at[0], row, west_col)
    to_e = send(col_e, rcv_w, 1, edge_sem.at[1], row, east_col)
    first_s, first_n = pl.ds(0, 3), pl.ds(0, 2)
    later_s, later_n = pl.ds(3, 2), pl.ds(2, 2)
    to_s = send(row_s.at[first_s], rcv_n.at[first_s], 2, edge_sem.at[2], south, col)
    to_n = send(row_n.at[first_n], rcv_s.at[first_n], 3, edge_sem.at[3], north, col)
    to_s_later = send(row_s.at[later_s], rcv_n.at[later_s], 6, edge_sem.at[6], south, col)
    to_n_later = send(row_n.at[later_n], rcv_s.at[later_n], 7, edge_sem.at[7], north, col)
    to_nw = send(col_w.at[V], rcv_se, 4, edge_sem.at[4], north, west_col)
    to_se = send(col_e.at[U], rcv_nw, 5, edge_sem.at[5], south, east_col)
    to_w.start()
    to_e.start()

    @pl.when(has_s)
    def _():
        to_s.start()
        to_se.start()
        to_s_later.start()

    @pl.when(has_n)
    def _():
        to_n.start()
        to_nw.start()
        to_n_later.start()

    def exchange(block, pack_w, pack_e, first, count, base, rsem, esem, wsem, pe, pw):
        out = []
        for d, r in enumerate(peers):
            out.append(send(block(r % 2), frame.at[pl.ds(first, count), OWN, frame_rows(row, r // 2), :], base + d, rsem.at[row], r, col))
        for r in QUAD:
            out.append(send(pack_w(r % 2), pe.at[row], base + 3 + 2 * r, esem.at[row], r, west_col))
            out.append(send(pack_e(r % 2), pw.at[row], base + 4 + 2 * r, wsem.at[row], r, east_col))
        for copy in out:
            copy.start()
        frame[pl.ds(first, count), OWN, own_rows, :] = block(core)[...]
        return out

    def collect(block, pack_w, first, count, rsem, esem, wsem, pe, pw):
        for r in peers:
            rows = frame_rows(r, chip)
            send(block(0), frame.at[pl.ds(first, count), OWN, rows, :], 0, rsem.at[r], r, col).wait_recv()
        for r in QUAD:
            send(pack_w(0), pe.at[r], 0, esem.at[r], r, east_col).wait_recv()
            send(pack_w(0), pw.at[r], 0, wsem.at[r], r, west_col).wait_recv()
        side = lax.broadcasted_iota(jnp.int32, (ROWS, 128), 1) // HALO
        for r in QUAD:
            for j in range(count):
                frame[first + j, 2, frame_rows(r, chip), :] = jnp.where(
                    side == 0, turn(pe[r], (128 - HALO * j) % 128), jnp.where(side == 3, turn(pw[r], (128 - HALO * j - HALO) % 128), 0.0))

    def stage_block(m):
        return stage.at[m, pl.ds(0, PACK)]

    def stage_w(m):
        return stage.at[m, PACK, 0]

    def stage_e(m):
        return stage.at[m, PACK, 1]

    to_w.wait_recv()
    to_e.wait_recv()

    def unpack(g, carry):
        from_e, from_w = rcv_e[...], rcv_w[...]
        for k in [EDGE_BLOCK * g + j for j in range(EDGE_BLOCK)]:
            for i in STRIPS:
                slot = L * i + k
                cube[:, k, :, 2, pl.ds(PAD + SUB * i, SUB), :] = jnp.where(
                    lane42 < 64, turn(from_w, lax.rem(128 - slot, 128)), turn(from_e, 127 - slot))
        return carry

    lax.fori_loop(0, L // EDGE_BLOCK, unpack, 0)

    def masks(i):
        rs = pl.ds(SUB * i, SUB)
        wet = kmt[:, rs, :]
        halo = turn(rcv_e[0, 0], 127 - (3 * L + i))
        nuv[0, :, rs, :] = jnp.minimum(wet, east_block(jnp.concatenate([wet, halo[None]], axis=0)))
        nuv[1, :, rs, :] = jnp.minimum(wet, kmt[:, pl.ds(8 * i + 1, 8), :])

    masks(0)
    masks(1)

    press = PRESS_SCALE / L
    pair = jnp.zeros((M, SUB, LANES), F32)

    def for_strips(body, init, strips=(0, 1, 3), levels=LEVEL_BLOCK):
        start, step, count = strips

        def strip(s, carry):
            m = s // count
            i = start + step * (s - count * m)
            rs = aligned(SUB * i)

            def get(f, k, part, d=0):
                start = PAD + 8 * i + d
                return cube[f, k, m, part, pl.ds(start if d else pl.multiple_of(start, 8), 8), :]

            state, finish = init(m, rs)

            def block(b, state):
                for j in range(levels):
                    k = b * levels + j
                    state = body(k, m, rs, get, state)
                return state

            finish(m, rs, lax.fori_loop(0, L // levels, block, state))
            return carry

        lax.fori_loop(0, M * count, strip, 0)

    def momentum_init(m, rs):
        return (pair,) * 6, momentum_finish

    def momentum_finish(m, rs, state):
        sums[0, m, :, rs, :] = state[4]
        sums[1, m, :, rs, :] = state[5]

    def momentum(k, m, rs, get, state):
        cx, cy, eu, ev, gu_sum, gv_sum = state
        level = k.astype(F32)
        both = slice(0, 3)
        u, v, un, vs = get(U, k, both), get(V, k, both), get(U, k, both, 1), get(V, k, both, -1)
        rho = (press * HALINE_CON) * get(S, k, both) - (press * THERM_EXP) * get(T, k, both)
        dx = rho[OWN] - east_block(rho)
        dy = rho[OWN] - ((press * HALINE_CON) * get(S, k, OWN, 1) - (press * THERM_EXP) * get(T, k, OWN, 1))
        vsum, usum = v + vs, u + un
        cx, cy = cx + dx, cy + dy
        gu = cx - 0.5 * (dx + u[OWN] * (east_block(u) - west_block(u))) - 0.125 * (
            (vsum[OWN] + east_block(vsum)) * (un[OWN] - get(U, k, OWN, -1)))
        gv = cy - 0.5 * (dy + v[OWN] * (get(V, k, OWN, 1) - vs[OWN])) - 0.125 * (
            (usum[OWN] + west_block(usum)) * (east_block(v) - west_block(v)))
        gu = jnp.where(nuv[0, :, rs, :] > level, gu, 0.0)
        gv = jnp.where(nuv[1, :, rs, :] > level, gv, 0.0)
        inverse = table[0, k]
        eu = (u[OWN] + gu + VISC_NUMBER * eu) * inverse
        ev = (v[OWN] + gv + VISC_NUMBER * ev) * inverse
        sol[U][k, m, :, rs, :] = eu
        sol[V][k, m, :, rs, :] = ev
        return cx, cy, eu, ev, gu_sum + gu, gv_sum + gv

    for_strips(momentum, momentum_init, strips=(1, 1, 1))

    @pl.when(has_n)
    def _():
        to_s.wait_recv()
        to_se.wait_recv()

    @pl.when(has_s)
    def _():
        to_n.wait_recv()
        to_nw.wait_recv()

    sent = exchange(stage_block, stage_w, stage_e, ETA, 4, 8, row_sem, e_sem, w_sem, pk_e, pk_w)

    def unpack_rows(g, carry):
        rows = aligned(SUB * g)
        below, above = rcv_s[:T, :, rows, :], rcv_n[:S, :, rows, :]
        for j in OCTET:
            k, m = 4 * g + j // 2, j % 2
            cube[:T, k, m, OWN, pl.ds(PAD - 1, 1), :] = below[:, :, j:j + 1, :]
            cube[:S, k, m, OWN, pl.ds(PAD + ROWS, 1), :] = above[:, :, j:j + 1, :]
            cube[S, k, m, OWN, pl.ds(PAD + ROWS, 1), :] = jnp.zeros((M, 1, LANES), F32)
            if m:
                cube[V, k, :, 2, pl.ds(0, PAD), :] = turn(rcv_se[...], 127 - 2 * L - k)
                cube[U, k, :, 2, pl.ds(PAD + ROWS, PAD), :] = turn(rcv_nw[...], lax.rem(128 - k, 128))
        return carry

    def unpack_rows_later(g, carry):
        rows = aligned(SUB * g)
        below, above = rcv_s[T:, :, rows, :], rcv_n[S:, :, rows, :]
        for j in OCTET:
            k, m = 4 * g + j // 2, j % 2
            cube[T:, k, m, OWN, pl.ds(PAD - 1, 1), :] = below[:, :, j:j + 1, :]
            cube[T:, k, m, OWN, pl.ds(PAD + ROWS, 1), :] = above[:, :, j:j + 1, :]
        return carry

    lax.fori_loop(0, L // 4, unpack_rows, 0)
    kmt[:, pl.ds(ROWS, 8), :] = rcv_n[U, :, pl.ds(M * L, SUB), :]
    masks(2)
    for_strips(momentum, momentum_init, strips=(0, 2, 2))

    collect(stage_block, stage_w, ETA, 4, row_sem, e_sem, w_sem, pk_e, pk_w)

    def coefficients(i, carry):
        rs = aligned(FPAD + SUB * i)
        depth = frame[DEPTH, :, rs, :]
        depth_e = east(depth)
        depth_n = frame[DEPTH, :, pl.ds(FPAD + SUB * i + 1, SUB), :]
        wet = depth > 0.0
        coef[0, :, rs, :] = jnp.where(wet, WAVE_COURANT, 0.0)
        coef[1, :, rs, :] = jnp.where(wet & (depth_e > 0.0), (0.5 * WAVE_COURANT) * (depth + depth_e), 0.0)
        coef[2, :, rs, :] = jnp.where(wet & (depth_n > 0.0), (0.5 * WAVE_COURANT) * (depth + depth_n), 0.0)
        return carry

    lax.fori_loop(0, TILES, coefficients, 0)

    for d in PAIR:
        scale = coef[1 + d, OWN, own_rows, :] / (jnp.maximum(nuv[d], 1.0) * (WAVE_COURANT * sub_count))
        for m in PAIR:
            fstage[m, d] = scale * sums[d, m]

    def put(m, rs, pack_w, pack_e):
        fstage_w[m, rs, :] = pack_w
        fstage_e[m, rs, :] = pack_e

    pack_2d(fstage, 2, put)
    sent += exchange(lambda m: fstage.at[m], lambda m: fstage_w.at[m], lambda m: fstage_e.at[m], FX, 2, 19, frow_sem, fe_sem, fw_sem, fpk_e, fpk_w)

    block_zero = jnp.zeros((M, ROWS, LANES), F32)

    def back(m, carry):
        def levels_back(b, state):
            x, total = list(state[:2]), list(state[2:])
            for j in range(BACK_BLOCK):
                k = L - 1 - (b * BACK_BLOCK + j)
                level = k.astype(F32)
                for d in PAIR:
                    e, n = sol[d][k, m], nuv[d]
                    x[d] = e + table[1, k] * jnp.where(n > level + 1.0, x[d], e * table[2, k])
                    sol[d][k, m] = x[d]
                    total[d] = total[d] + jnp.where(n > level, x[d], 0.0)
            return (*x, *total)

        state = lax.fori_loop(0, L // BACK_BLOCK, levels_back, (block_zero,) * 4)
        for d in PAIR:
            sums[d, m] = state[2 + d] / jnp.maximum(nuv[d], 1.0)
        return carry

    lax.fori_loop(0, M, back, 0)

    def tracer_init(m, rs):
        return jnp.zeros((M, M, SUB, LANES), F32), lambda *a: None

    def tracers(k, m, rs, get, e):
        both = pl.ds(T, M)
        t, u = get(both, k, slice(0, 3)), get(U, k, slice(0, 3))
        fx = u * (t + jnp.concatenate([east_block(t), t[:, :1]], axis=1))
        t = t[:, OWN]
        gain = fx[:, OWN] - west_block(fx) + (
            get(V, k, OWN) * (t + get(both, k, OWN, 1)) - get(V, k, OWN, -1) * (t + get(both, k, OWN, -1)))
        e = (jnp.where(kmt[:, rs, :] > k.astype(F32), t - 0.5 * gain, 0.0) + DIFF_NUMBER * e) * table[3, k]
        sol[T][k, m, :, rs, :] = e[0]
        sol[S][k, m, :, rs, :] = e[1]
        return e

    @pl.when(has_n)
    def _():
        to_s_later.wait_recv()

    @pl.when(has_s)
    def _():
        to_n_later.wait_recv()

    lax.fori_loop(0, L // 4, unpack_rows_later, 0)
    for_strips(tracers, tracer_init, levels=TRACER_BLOCK)
    acc[...] = jnp.zeros(acc.shape, F32)

    collect(lambda m: fstage.at[m], lambda m: fstage_w.at[m], FX, 2, frow_sem, fe_sem, fw_sem, fpk_e, fpk_w)

    def subcycle(n, tiles, base):
        def tile_rows(t):
            return aligned(base + SUB * t)

        def eta_tile(t):
            rs = tile_rows(t)
            u, v = frame[TX, :, rs, :], frame[TY, :, rs, :]
            div = (u - west(u)) + (v - frame[TY, :, pl.ds(base + SUB * t - 1, SUB), :])
            eta = frame[ETA, :, rs, :] - coef[0, :, rs, :] * div
            frame[ETA, :, rs, :] = eta
            return u, v, eta

        last_row = iota((RING, SUB, LANES), 1) == SUB - 1
        following = eta_tile(0)
        for t in range(tiles):
            u, v, e = following
            if t + 1 < tiles:
                following = eta_tile(t + 1)
            e_n = jnp.where(last_row, pltpu.roll(following[2], SUB - 1, 1), pltpu.roll(e, SUB - 1, 1))
            rs = tile_rows(t)
            frame[TX, :, rs, :] = u + frame[FX, :, rs, :] - coef[1, :, rs, :] * (east(e) - e)
            frame[TY, :, rs, :] = v + frame[FY, :, rs, :] - coef[2, :, rs, :] * (e_n - e)
        chip_rows = aligned(FPAD + (M * ROWS - SHIFT) * chip, M * ROWS)
        acc[...] += stage[1, KMT, n // ROWS, pl.ds(lax.rem(n, ROWS), 1), :] * frame[pl.ds(0, RING), OWN, chip_rows, :]

    def subcycles(first, last, tiles, base):
        def block(b, carry):
            for j in range(SUB_BLOCK):
                subcycle(SUB_BLOCK * b + j, tiles, base)
            return carry

        lax.fori_loop(first // SUB_BLOCK, last // SUB_BLOCK, block, 0)

    turning = -(-max(sub_count - SHIFT, 0) // SUB_BLOCK) * SUB_BLOCK
    subcycles(0, turning, TILES, FPAD)
    subcycles(turning, sub_count, TILES - SHIFT // SUB, FPAD + SHIFT * chip)

    mine = aligned(ROWS * core, ROWS)
    theirs = aligned(ROWS * (1 - core), ROWS)
    result[...] = acc[:, :, theirs, :]
    swap = send(result, result_in, 30, swap_sem, row + 1 - 2 * core, col)
    swap.start()
    swap.wait_recv()
    for m in PAIR:
        whole = jnp.where(core == m, acc[:, :, mine, :], result_in[...])
        for lt in PAIR:
            ls = pl.ds(LANES * lt, LANES)
            eta_out[m, :, ls] = whole[ETA, lt]
            tx_out[m, :, ls] = whole[TX, lt]
            ty_out[m, :, ls] = whole[TY, lt]
            for d, out in enumerate((qu_out, qv_out)):
                depth = coef[1 + d, lt, own_rows, :]
                out[m, :, ls] = whole[TX + d, lt] / jnp.where(depth > 0.0, depth / WAVE_COURANT, 1.0) - sums[d, m, lt]
                nuv_out[d, :, ls] = nuv[d, lt]

    to_w.wait_send()
    to_e.wait_send()

    @pl.when(has_s)
    def _():
        to_s.wait_send()
        to_se.wait_send()
        to_s_later.wait_send()

    @pl.when(has_n)
    def _():
        to_n.wait_send()
        to_nw.wait_send()
        to_n_later.wait_send()

    for copy in sent:
        copy.wait_send()
    swap.wait_send()


def final_kernel(level_count, sol_u, sol_v, sol_t, sol_s, qu, qv, nuv, wet, eta_in, tx_in, ty_in,
                 eta_out, tx_out, ty_out, u_out, v_out, t_out, s_out, cubes, cube_sem, plane_sem):
    ratio = sweep_constants(level_count, DIFF_NUMBER)[1]
    strips = M * len(STRIPS)
    passed = [pltpu.make_async_copy(src, dst, plane_sem.at[n])
              for n, (src, dst) in enumerate(((eta_in, eta_out), (tx_in, tx_out), (ty_in, ty_out)))]
    for copy in passed:
        copy.start()

    def writes(s):
        m = s // 3
        rs = pl.ds(pl.multiple_of(SUB * (s - 3 * m), SUB), SUB)
        return m, rs, [pltpu.make_async_copy(cubes.at[f, s], dst.at[:, m, rs, :], cube_sem.at[f, s])
                       for f, dst in enumerate((t_out, s_out, u_out, v_out))]

    def strip(s, carry):
        m, rs, done = writes(s)
        for f, src in enumerate((sol_t, sol_s, sol_u, sol_v)):
            for lt in PAIR:
                ls = pl.ds(LANES * lt, LANES)
                if f < M:
                    n_wet = wet[rs, ls]
                    x = jnp.zeros(TILE, F32)
                    for k in reversed(range(level_count)):
                        e = src[k, m, lt, rs, :]
                        x = e + ratio[k] * jnp.where(n_wet > k + 1, x, e * (1.0 / (1.0 - ratio[k])))
                        cubes[f, s, k, :, ls] = jnp.where(n_wet > k, x, 0.0)
                else:
                    n, mean = nuv[f - M, rs, ls], (qu, qv)[f - M][m, rs, ls]
                    for k in range(level_count):
                        cubes[f, s, k, :, ls] = jnp.where(n > float(k), src[k, m, lt, rs, :] + mean, 0.0)
            done[f].start()
        return carry

    def finish(s, carry):
        for copy in writes(s)[-1]:
            copy.wait()
        return carry

    lax.fori_loop(0, strips, strip, 0)
    lax.fori_loop(0, strips, finish, 0)
    for copy in passed:
        copy.wait()


def solution(mesh):
    col_count = mesh.shape["col"]

    def local_step(vel_x, vel_y, pot_temp, salinity, surf_eta, trans_x, trans_y, col_depth, wet_levels, avg_weights):
        L = vel_x.shape[0]
        N = avg_weights.shape[0]
        hbm_spec = pl.BlockSpec(memory_space=pltpu.HBM)
        vmem_spec = pl.BlockSpec(memory_space=pltpu.VMEM)
        cube = jax.ShapeDtypeStruct(vel_x.shape, F32)
        flat = jax.ShapeDtypeStruct(surf_eta.shape, F32)
        vm = lambda *shape: pltpu.VMEM(shape, F32)
        dma = lambda n: pltpu.SemaphoreType.DMA((n,))
        stage = pl.pallas_call(
            functools.partial(stage_kernel, N),
            out_shape=jax.ShapeDtypeStruct((M, ROOM, M, ROWS, LANES), F32),
            in_specs=[vmem_spec] * 5 + [pl.BlockSpec(memory_space=pltpu.SMEM)],
            out_specs=hbm_spec,
            scratch_shapes=[vm(M, STAGED, M, ROWS, LANES), pltpu.SemaphoreType.DMA],
            name="ocean_stage",
        )(surf_eta, trans_x, trans_y, col_depth, wet_levels, avg_weights)
        *sol, qu, qv, nuv, eta_o, tx_o, ty_o = pl.pallas_call(
            functools.partial(step_kernel, col_count, L, N),
            out_shape=[jax.ShapeDtypeStruct((L, M, M, ROWS, LANES), F32)] * 4 + [flat] * 6,
            in_specs=[hbm_spec] * 5,
            out_specs=[vmem_spec] * 10,
            scratch_shapes=[
                vm(4, L, M, RING, XR, LANES), vm(M, STAGED, M, ROWS, LANES), *[vm(4, M, 8, LANES)] * 4, vm(5, M, M * L + 8, LANES), vm(4, M, M * L, LANES), vm(5, M, M * L + 8, LANES), vm(4, M, M * L, LANES),
                *[vm(M, 8, LANES)] * 2, vm(M, ROWS + 8, LANES), vm(M, M, ROWS, LANES), vm(M, M, M, ROWS, LANES),
                *[vm(4, ROWS, LANES)] * M,
                vm(M, M, M, ROWS, LANES), *[vm(M, ROWS, LANES)] * M, *[vm(4, ROWS, LANES)] * M,
                vm(6, RING, FRAME, LANES), vm(RING, RING, FRAME, LANES), vm(RING, M, M * ROWS, LANES), *[vm(RING, M, ROWS, LANES)] * M,
                pltpu.SMEM((4, L), F32), dma(8), pltpu.SemaphoreType.DMA, dma(31), dma(8), *[dma(4)] * 6, pltpu.SemaphoreType.DMA],
            compiler_params=pltpu.CompilerParams(collective_id=0, has_side_effects=True, vmem_limit_bytes=STEP_VMEM),
            name="ocean_step",
        )(vel_x, vel_y, pot_temp, salinity, stage)
        outs = pl.pallas_call(
            functools.partial(final_kernel, L),
            out_shape=[flat] * 3 + [cube] * 4,
            in_specs=[vmem_spec] * 11,
            out_specs=[hbm_spec] * 7,
            scratch_shapes=[vm(4, M * len(STRIPS), L, SUB, 256), pltpu.SemaphoreType.DMA((4, M * len(STRIPS))), dma(3)],
            name="ocean_final",
            compiler_params=pltpu.CompilerParams(vmem_limit_bytes=FINAL_VMEM),
        )(*sol, qu, qv, nuv, wet_levels, eta_o, tx_o, ty_o)
        return tuple(outs)

    spec_3d = P(None, None, "row", "col")
    spec_2d = P(None, "row", "col")
    spec_map = P("row", "col")
    return jax.shard_map(local_step, mesh=mesh, in_specs=(spec_3d,) * 4 + (spec_2d,) * 3 + (spec_map,) * 2 + (P(),),
                         out_specs=(spec_2d,) * 3 + (spec_3d,) * 4, check_vma=False)
```

```python
import functools

import jax
import jax.numpy as jnp
from jax import lax
from jax.experimental import pallas as pl
from jax.experimental.pallas import tpu as pltpu
from jax.sharding import PartitionSpec as P

WAVE_COURANT = 0.4
THERM_EXP = 0.2
HALINE_CON = 0.15
PRESS_SCALE = 0.5
VISC_NUMBER = 1.0
DIFF_NUMBER = 0.5

MESH = pl.DeviceIdType.MESH
F32 = jnp.float32
ROWS = 24
PAD = 8
XR = ROWS + 2 * PAD
EDGE_BLOCK = 12
TRACER_BLOCK = 36
BACK_BLOCK = 36
SUB_BLOCK = 3
LEVEL_BLOCK = 36
LANES = 128
SUB = 8
TILE = (SUB, LANES)
PAIR, STRIPS, QUAD, OCTET = range(2), range(3), range(4), range(SUB)
RING = 3
M = 2
STEP_VMEM, FINAL_VMEM = 46 << 20, 9 << 20
TILES = 10
SHIFT = 16
FPAD = SHIFT + PAD
FRAME = 4 * ROWS + 2 * FPAD
HALO = 32


def sweep_constants(level_count, strength):
    inverse, ratio = [], []
    for k in range(level_count):
        pivot = 1.0 + strength if k == 0 else 1.0 + 2.0 * strength - strength * ratio[-1]
        inverse.append(1.0 / pivot)
        ratio.append(strength / pivot)
    return inverse, ratio


def iota(shape, axis):
    return lax.broadcasted_iota(jnp.int32, shape, axis)


def lanes(*lead):
    return iota((*lead, 8, 128), len(lead) + 1)


def turn(x, shift):
    return pltpu.roll(x, shift, x.ndim - 1)


def east(x):
    rolled = turn(x, 127)
    return jnp.where(lanes(3) == 127, jnp.concatenate([rolled[1:], rolled[:1]], axis=0), rolled)


def west(x):
    rolled = turn(x, 1)
    return jnp.where(lanes(3) == 0, jnp.concatenate([rolled[2:], rolled[:2]], axis=0), rolled)


def east_block(x):
    rolled = turn(x[:2], 127)
    return jnp.where(lanes(2) == 127, jnp.concatenate([rolled[1:], x[2:]], axis=0), rolled)


def west_block(x):
    rolled = turn(x[:2], 1)
    return jnp.where(lanes(2) == 0, jnp.concatenate([x[2:], rolled[:1]], axis=0), rolled)


STAGED = 6
ROOM = 240
ETA, TX, TY, DEPTH, PACK, KMT = range(STAGED)


def pack_2d(stage, count, put):
    lane = lanes()
    for i in STRIPS:
        rs = pl.ds(SUB * i, SUB)
        for m in PAIR:
            pack_w = pack_e = jnp.zeros(TILE, F32)
            for j in range(count):
                here = lane // HALO == j
                pack_w = jnp.where(here, turn(stage[m, j, 0, rs, :], HALO * j), pack_w)
                pack_e = jnp.where(here, turn(stage[m, j, 1, rs, :], (HALO * j + HALO) % LANES), pack_e)
            put(m, rs, pack_w, pack_e)


def stage_kernel(sub_count, eta, tx, ty, depth, wet_in, weights, out, stage, sem):
    for lt in PAIR:
        ls = pl.ds(LANES * lt, LANES)
        wet = wet_in[:, ls].astype(F32)
        masked = jnp.where(wet > 0.0, depth[:, ls], 0.0)
        stage[0, KMT, lt] = wet
        for m in PAIR:
            for j, field in ((ETA, eta), (TX, tx), (TY, ty)):
                stage[m, j, lt] = field[m, :, ls]
            stage[m, DEPTH, lt] = masked
    for n in range(sub_count):
        stage[1, KMT, n // ROWS, pl.ds(n % ROWS, 1), :] = jnp.full((1, LANES), weights[n], F32)

    def put(m, rs, pack_w, pack_e):
        stage[m, PACK, 0, rs, :] = pack_w
        stage[m, PACK, 1, rs, :] = pack_e

    pack_2d(stage, 4, put)
    copy = pltpu.make_async_copy(stage, out.at[:, pl.ds(0, STAGED)], sem)
    copy.start()
    copy.wait()


def step_kernel(
    col_count, level_count, sub_count,
    u_hbm, v_hbm, t_hbm, s_hbm, stage_hbm,
    sol_u, sol_v, sol_t, sol_s, qu_out, qv_out, nuv_out, eta_out, tx_out, ty_out,
    cube, stage,
    col_w, col_e, rcv_e, rcv_w, row_s, row_n, rcv_n, rcv_s, rcv_se, rcv_nw,
    kmt, nuv, sums, pk_e, pk_w, fstage, fstage_w, fstage_e, fpk_e, fpk_w,
    frame, coef, acc, result, result_in,
    table, load_sem, stage_sem, send_sem, edge_sem, row_sem, e_sem, w_sem, frow_sem, fe_sem, fw_sem, swap_sem,
):
    L = level_count
    U, V, T, S = range(4)
    sol = (sol_u, sol_v, sol_t, sol_s)
    FX, FY = 4, 5
    OWN = slice(0, 2)
    col = lax.axis_index("col")
    row = lax.axis_index("row")
    chip = row // 2
    core = row % 2
    east_col = lax.rem(col + 1, col_count)
    west_col = lax.rem(col + col_count - 1, col_count)
    peers = [lax.rem(row + d, 4) for d in (1, 2, 3)]
    lane = lanes()
    zero = jnp.zeros(TILE, F32)

    def aligned(start, size=8):
        return pl.ds(pl.multiple_of(start, 8), size)

    barrier = pltpu.get_barrier_semaphore()
    for r in peers:
        pl.semaphore_signal(barrier, inc=1, device_id={"row": r, "col": col}, device_id_type=MESH)
    for other in (east_col, west_col):
        for r in QUAD:
            pl.semaphore_signal(barrier, inc=1, device_id={"row": r, "col": other}, device_id_type=MESH)

    loads = []
    for f, src in enumerate((u_hbm, v_hbm, t_hbm, s_hbm)):
        for lt in PAIR:
            loads.append(pltpu.make_async_copy(
                src.at[:, :, :, pl.ds(LANES * lt, LANES)], cube.at[f, :, :, lt, pl.ds(PAD, ROWS), :], load_sem.at[2 * f + lt]))
            loads[-1].start()

    inv_v, ratio_v = sweep_constants(L, VISC_NUMBER)
    for n, line in enumerate((inv_v, ratio_v, [1.0 / (1.0 - r) for r in ratio_v], sweep_constants(L, DIFF_NUMBER)[0])):
        for k in range(L):
            table[n, k] = line[k]

    staged = pltpu.make_async_copy(stage_hbm.at[:, pl.ds(0, STAGED)], stage, stage_sem)
    staged.start()

    has_s, has_n = row > 0, row < 3

    @pl.when(row == 0)
    def _():
        rcv_s[...] = jnp.zeros(rcv_s.shape, F32)
        rcv_se[...] = jnp.zeros(rcv_se.shape, F32)

    @pl.when(row == 3)
    def _():
        rcv_n[...] = jnp.zeros(rcv_n.shape, F32)
        rcv_nw[...] = jnp.zeros(rcv_nw.shape, F32)

    outside = jnp.zeros((6, RING, PAD, LANES), F32)

    @pl.when(chip == 0)
    def _():
        frame[:, :, pl.ds(FPAD - PAD, PAD), :] = outside

    @pl.when(chip == 1)
    def _():
        frame[:, :, pl.ds(FPAD + SUB * TILES, PAD), :] = outside


    lane42 = lanes(4, 2)
    lane2 = lanes(M)
    empty = jnp.zeros((M, SUB, LANES), F32)
    for f in QUAD:
        for copy in loads[2 * f:2 * f + 2]:
            copy.wait()

        def pack(g, carry):
            west_pack, east_pack = carry
            for k, i in [(EDGE_BLOCK * g + j, i) for j in range(EDGE_BLOCK) for i in STRIPS]:
                slot = L * i + k
                rs = pl.ds(PAD + SUB * i, SUB)
                west_pack = jnp.where(lane2 == slot, turn(cube[f, k, :, 0, rs, :], slot), west_pack)
                east_pack = jnp.where(lane2 == slot, turn(cube[f, k, :, 1, rs, :], slot + 1), east_pack)
            for q in range(M * EDGE_BLOCK // SUB):
                rows = aligned(M * EDGE_BLOCK * g + SUB * q)
                low = high = empty
                for j in OCTET:
                    k, m = EDGE_BLOCK * g + (SUB * q + j) // M, j % M
                    low = jnp.where(sub2 == j, cube[f, k, m, OWN, pl.ds(PAD - j, SUB), :], low)
                    high = jnp.where(sub2 == j, cube[f, k, m, OWN, pl.ds(PAD + ROWS - 1 - j, SUB), :], high)
                row_n[f, :, rows, :] = high
                row_s[f if f < T else f + 1, :, rows, :] = low
                if f == S:
                    row_s[T, :, rows, :] = row_s[T + 1, :, rows, :] - (HALINE_CON / THERM_EXP) * low
            return west_pack, east_pack

        sub2 = iota((M, SUB, LANES), 1)
        col_w[f], col_e[f] = lax.fori_loop(0, L // EDGE_BLOCK, pack, (empty, empty))
    staged.wait()
    kmt[:, pl.ds(0, ROWS), :] = stage[0, KMT]
    for i in STRIPS:
        slot = 3 * L + i
        col_w[0, 0] = jnp.where(lane == slot, turn(kmt[0, pl.ds(SUB * i, SUB), :], slot), col_w[0, 0])
    row_s[U, :, pl.ds(M * L, SUB), :] = kmt[:, pl.ds(0, SUB), :]

    pl.semaphore_wait(barrier, 11)

    def send(src, dst, ssem, rsem, r, c):
        return pltpu.make_async_remote_copy(
            src_ref=src, dst_ref=dst, send_sem=send_sem.at[ssem], recv_sem=rsem, device_id={"row": r, "col": c}, device_id_type=MESH)

    def frame_rows(r, at_chip):
        return aligned(FPAD + ROWS * r - SHIFT * at_chip, ROWS)

    own_rows = frame_rows(row, chip)
    south, north = jnp.maximum(row - 1, 0), jnp.minimum(row + 1, 3)
    to_w = send(col_w, rcv_e, 0, edge_sem.at[0], row, west_col)
    to_e = send(col_e, rcv_w, 1, edge_sem.at[1], row, east_col)
    first_s, first_n = pl.ds(0, 3), pl.ds(0, 2)
    later_s, later_n = pl.ds(3, 2), pl.ds(2, 2)
    to_s = send(row_s.at[first_s], rcv_n.at[first_s], 2, edge_sem.at[2], south, col)
    to_n = send(row_n.at[first_n], rcv_s.at[first_n], 3, edge_sem.at[3], north, col)
    to_s_later = send(row_s.at[later_s], rcv_n.at[later_s], 6, edge_sem.at[6], south, col)
    to_n_later = send(row_n.at[later_n], rcv_s.at[later_n], 7, edge_sem.at[7], north, col)
    to_nw = send(col_w.at[V], rcv_se, 4, edge_sem.at[4], north, west_col)
    to_se = send(col_e.at[U], rcv_nw, 5, edge_sem.at[5], south, east_col)
    to_w.start()
    to_e.start()

    @pl.when(has_s)
    def _():
        to_s.start()
        to_se.start()
        to_s_later.start()

    @pl.when(has_n)
    def _():
        to_n.start()
        to_nw.start()
        to_n_later.start()

    def exchange(block, pack_w, pack_e, first, count, base, rsem, esem, wsem, pe, pw):
        out = []
        for d, r in enumerate(peers):
            out.append(send(block(r % 2), frame.at[pl.ds(first, count), OWN, frame_rows(row, r // 2), :], base + d, rsem.at[row], r, col))
        for r in QUAD:
            out.append(send(pack_w(r % 2), pe.at[row], base + 3 + 2 * r, esem.at[row], r, west_col))
            out.append(send(pack_e(r % 2), pw.at[row], base + 4 + 2 * r, wsem.at[row], r, east_col))
        for copy in out:
            copy.start()
        frame[pl.ds(first, count), OWN, own_rows, :] = block(core)[...]
        return out

    def collect(block, pack_w, first, count, rsem, esem, wsem, pe, pw):
        for r in peers:
            rows = frame_rows(r, chip)
            send(block(0), frame.at[pl.ds(first, count), OWN, rows, :], 0, rsem.at[r], r, col).wait_recv()
        for r in QUAD:
            send(pack_w(0), pe.at[r], 0, esem.at[r], r, east_col).wait_recv()
            send(pack_w(0), pw.at[r], 0, wsem.at[r], r, west_col).wait_recv()
        side = lax.broadcasted_iota(jnp.int32, (ROWS, 128), 1) // HALO
        for r in QUAD:
            for j in range(count):
                frame[first + j, 2, frame_rows(r, chip), :] = jnp.where(
                    side == 0, turn(pe[r], (128 - HALO * j) % 128), jnp.where(side == 3, turn(pw[r], (128 - HALO * j - HALO) % 128), 0.0))

    def stage_block(m):
        return stage.at[m, pl.ds(0, PACK)]

    def stage_w(m):
        return stage.at[m, PACK, 0]

    def stage_e(m):
        return stage.at[m, PACK, 1]

    to_w.wait_recv()
    to_e.wait_recv()

    def unpack(g, carry):
        from_e, from_w = rcv_e[...], rcv_w[...]
        for k in [EDGE_BLOCK * g + j for j in range(EDGE_BLOCK)]:
            for i in STRIPS:
                slot = L * i + k
                cube[:, k, :, 2, pl.ds(PAD + SUB * i, SUB), :] = jnp.where(
                    lane42 < 64, turn(from_w, lax.rem(128 - slot, 128)), turn(from_e, 127 - slot))
        return carry

    lax.fori_loop(0, L // EDGE_BLOCK, unpack, 0)

    def masks(i):
        rs = pl.ds(SUB * i, SUB)
        wet = kmt[:, rs, :]
        halo = turn(rcv_e[0, 0], 127 - (3 * L + i))
        nuv[0, :, rs, :] = jnp.minimum(wet, east_block(jnp.concatenate([wet, halo[None]], axis=0)))
        nuv[1, :, rs, :] = jnp.minimum(wet, kmt[:, pl.ds(8 * i + 1, 8), :])

    masks(0)
    masks(1)

    press = PRESS_SCALE / L
    pair = jnp.zeros((M, SUB, LANES), F32)

    def for_strips(body, init, strips=(0, 1, 3), levels=LEVEL_BLOCK):
        start, step, count = strips

        def strip(s, carry):
            m = s // count
            i = start + step * (s - count * m)
            rs = aligned(SUB * i)

            def get(f, k, part, d=0):
                start = PAD + 8 * i + d
                return cube[f, k, m, part, pl.ds(start if d else pl.multiple_of(start, 8), 8), :]

            state, finish = init(m, rs)

            def block(b, state):
                for j in range(levels):
                    k = b * levels + j
                    state = body(k, m, rs, get, state)
                return state

            finish(m, rs, lax.fori_loop(0, L // levels, block, state))
            return carry

        lax.fori_loop(0, M * count, strip, 0)

    def momentum_init(m, rs):
        return (pair,) * 6, momentum_finish

    def momentum_finish(m, rs, state):
        sums[0, m, :, rs, :] = state[4]
        sums[1, m, :, rs, :] = state[5]

    def momentum(k, m, rs, get, state):
        cx, cy, eu, ev, gu_sum, gv_sum = state
        level = k.astype(F32)
        both = slice(0, 3)
        u, v, un, vs = get(U, k, both), get(V, k, both), get(U, k, both, 1), get(V, k, both, -1)
        rho = (press * HALINE_CON) * get(S, k, both) - (press * THERM_EXP) * get(T, k, both)
        dx = rho[OWN] - east_block(rho)
        dy = rho[OWN] - ((press * HALINE_CON) * get(S, k, OWN, 1) - (press * THERM_EXP) * get(T, k, OWN, 1))
        vsum, usum = v + vs, u + un
        cx, cy = cx + dx, cy + dy
        gu = cx - 0.5 * (dx + u[OWN] * (east_block(u) - west_block(u))) - 0.125 * (
            (vsum[OWN] + east_block(vsum)) * (un[OWN] - get(U, k, OWN, -1)))
        gv = cy - 0.5 * (dy + v[OWN] * (get(V, k, OWN, 1) - vs[OWN])) - 0.125 * (
            (usum[OWN] + west_block(usum)) * (east_block(v) - west_block(v)))
        gu = jnp.where(nuv[0, :, rs, :] > level, gu, 0.0)
        gv = jnp.where(nuv[1, :, rs, :] > level, gv, 0.0)
        inverse = table[0, k]
        eu = (u[OWN] + gu + VISC_NUMBER * eu) * inverse
        ev = (v[OWN] + gv + VISC_NUMBER * ev) * inverse
        sol[U][k, m, :, rs, :] = eu
        sol[V][k, m, :, rs, :] = ev
        return cx, cy, eu, ev, gu_sum + gu, gv_sum + gv

    for_strips(momentum, momentum_init, strips=(1, 1, 1))

    @pl.when(has_n)
    def _():
        to_s.wait_recv()
        to_se.wait_recv()

    @pl.when(has_s)
    def _():
        to_n.wait_recv()
        to_nw.wait_recv()

    sent = exchange(stage_block, stage_w, stage_e, ETA, 4, 8, row_sem, e_sem, w_sem, pk_e, pk_w)

    def unpack_rows(g, carry):
        rows = aligned(SUB * g)
        below, above = rcv_s[:T, :, rows, :], rcv_n[:S, :, rows, :]
        for j in OCTET:
            k, m = 4 * g + j // 2, j % 2
            cube[:T, k, m, OWN, pl.ds(PAD - 1, 1), :] = below[:, :, j:j + 1, :]
            cube[:S, k, m, OWN, pl.ds(PAD + ROWS, 1), :] = above[:, :, j:j + 1, :]
            cube[S, k, m, OWN, pl.ds(PAD + ROWS, 1), :] = jnp.zeros((M, 1, LANES), F32)
            if m:
                cube[V, k, :, 2, pl.ds(0, PAD), :] = turn(rcv_se[...], 127 - 2 * L - k)
                cube[U, k, :, 2, pl.ds(PAD + ROWS, PAD), :] = turn(rcv_nw[...], lax.rem(128 - k, 128))
        return carry

    def unpack_rows_later(g, carry):
        rows = aligned(SUB * g)
        below, above = rcv_s[T:, :, rows, :], rcv_n[S:, :, rows, :]
        for j in OCTET:
            k, m = 4 * g + j // 2, j % 2
            cube[T:, k, m, OWN, pl.ds(PAD - 1, 1), :] = below[:, :, j:j + 1, :]
            cube[T:, k, m, OWN, pl.ds(PAD + ROWS, 1), :] = above[:, :, j:j + 1, :]
        return carry

    lax.fori_loop(0, L // 4, unpack_rows, 0)
    kmt[:, pl.ds(ROWS, 8), :] = rcv_n[U, :, pl.ds(M * L, SUB), :]
    masks(2)
    for_strips(momentum, momentum_init, strips=(0, 2, 2))

    collect(stage_block, stage_w, ETA, 4, row_sem, e_sem, w_sem, pk_e, pk_w)

    def coefficients(i, carry):
        rs = aligned(FPAD + SUB * i)
        depth = frame[DEPTH, :, rs, :]
        depth_e = east(depth)
        depth_n = frame[DEPTH, :, pl.ds(FPAD + SUB * i + 1, SUB), :]
        wet = depth > 0.0
        coef[0, :, rs, :] = jnp.where(wet, WAVE_COURANT, 0.0)
        coef[1, :, rs, :] = jnp.where(wet & (depth_e > 0.0), (0.5 * WAVE_COURANT) * (depth + depth_e), 0.0)
        coef[2, :, rs, :] = jnp.where(wet & (depth_n > 0.0), (0.5 * WAVE_COURANT) * (depth + depth_n), 0.0)
        return carry

    lax.fori_loop(0, TILES, coefficients, 0)

    for d in PAIR:
        scale = coef[1 + d, OWN, own_rows, :] / (jnp.maximum(nuv[d], 1.0) * (WAVE_COURANT * sub_count))
        for m in PAIR:
            fstage[m, d] = scale * sums[d, m]

    def put(m, rs, pack_w, pack_e):
        fstage_w[m, rs, :] = pack_w
        fstage_e[m, rs, :] = pack_e

    pack_2d(fstage, 2, put)
    sent += exchange(lambda m: fstage.at[m], lambda m: fstage_w.at[m], lambda m: fstage_e.at[m], FX, 2, 19, frow_sem, fe_sem, fw_sem, fpk_e, fpk_w)

    block_zero = jnp.zeros((M, ROWS, LANES), F32)

    def back(m, carry):
        def levels_back(b, state):
            x, total = list(state[:2]), list(state[2:])
            for j in range(BACK_BLOCK):
                k = L - 1 - (b * BACK_BLOCK + j)
                level = k.astype(F32)
                for d in PAIR:
                    e, n = sol[d][k, m], nuv[d]
                    x[d] = e + table[1, k] * jnp.where(n > level + 1.0, x[d], e * table[2, k])
                    sol[d][k, m] = x[d]
                    total[d] = total[d] + jnp.where(n > level, x[d], 0.0)
            return (*x, *total)

        state = lax.fori_loop(0, L // BACK_BLOCK, levels_back, (block_zero,) * 4)
        for d in PAIR:
            sums[d, m] = state[2 + d] / jnp.maximum(nuv[d], 1.0)
        return carry

    lax.fori_loop(0, M, back, 0)

    def tracer_init(m, rs):
        return pair, lambda *a: None

    def tracer(f):
        def body(k, m, rs, get, e):
            t, u = get(f, k, slice(0, 3)), get(U, k, slice(0, 3))
            fx = u * (t + jnp.concatenate([east_block(t), t[:1]], axis=0))
            t = t[OWN]
            gain = fx[OWN] - west_block(fx) + (get(V, k, OWN) * (t + get(f, k, OWN, 1)) - get(V, k, OWN, -1) * (t + get(f, k, OWN, -1)))
            e = (jnp.where(kmt[:, rs, :] > k.astype(F32), t - 0.5 * gain, 0.0) + DIFF_NUMBER * e) * table[3, k]
            sol[f][k, m, :, rs, :] = e
            return e

        return body

    @pl.when(has_n)
    def _():
        to_s_later.wait_recv()

    @pl.when(has_s)
    def _():
        to_n_later.wait_recv()

    lax.fori_loop(0, L // 4, unpack_rows_later, 0)
    for f in (T, S):
        for_strips(tracer(f), tracer_init, levels=TRACER_BLOCK)
    acc[...] = jnp.zeros(acc.shape, F32)

    collect(lambda m: fstage.at[m], lambda m: fstage_w.at[m], FX, 2, frow_sem, fe_sem, fw_sem, fpk_e, fpk_w)

    def subcycle(n, tiles, base):
        def tile_rows(t):
            return aligned(base + SUB * t)

        def eta_tile(t):
            rs = tile_rows(t)
            u, v = frame[TX, :, rs, :], frame[TY, :, rs, :]
            div = (u - west(u)) + (v - frame[TY, :, pl.ds(base + SUB * t - 1, SUB), :])
            eta = frame[ETA, :, rs, :] - coef[0, :, rs, :] * div
            frame[ETA, :, rs, :] = eta
            return eta

        last_row = iota((RING, SUB, LANES), 1) == SUB - 1
        following = eta_tile(0)
        for t in range(tiles):
            e = following
            if t + 1 < tiles:
                following = eta_tile(t + 1)
            e_n = jnp.where(last_row, pltpu.roll(following, SUB - 1, 1), pltpu.roll(e, SUB - 1, 1))
            rs = tile_rows(t)
            frame[TX, :, rs, :] += frame[FX, :, rs, :] - coef[1, :, rs, :] * (east(e) - e)
            frame[TY, :, rs, :] += frame[FY, :, rs, :] - coef[2, :, rs, :] * (e_n - e)
        chip_rows = aligned(FPAD + (M * ROWS - SHIFT) * chip, M * ROWS)
        acc[...] += stage[1, KMT, n // ROWS, pl.ds(lax.rem(n, ROWS), 1), :] * frame[pl.ds(0, RING), OWN, chip_rows, :]

    def subcycles(first, last, tiles, base):
        def block(b, carry):
            for j in range(SUB_BLOCK):
                subcycle(SUB_BLOCK * b + j, tiles, base)
            return carry

        lax.fori_loop(first // SUB_BLOCK, last // SUB_BLOCK, block, 0)

    turning = -(-max(sub_count - SHIFT, 0) // SUB_BLOCK) * SUB_BLOCK
    subcycles(0, turning, TILES, FPAD)
    subcycles(turning, sub_count, TILES - SHIFT // SUB, FPAD + SHIFT * chip)

    mine = aligned(ROWS * core, ROWS)
    theirs = aligned(ROWS * (1 - core), ROWS)
    result[...] = acc[:, :, theirs, :]
    swap = send(result, result_in, 30, swap_sem, row + 1 - 2 * core, col)
    swap.start()
    swap.wait_recv()
    for m in PAIR:
        whole = jnp.where(core == m, acc[:, :, mine, :], result_in[...])
        for lt in PAIR:
            ls = pl.ds(LANES * lt, LANES)
            eta_out[m, :, ls] = whole[ETA, lt]
            tx_out[m, :, ls] = whole[TX, lt]
            ty_out[m, :, ls] = whole[TY, lt]
            for d, out in enumerate((qu_out, qv_out)):
                depth = coef[1 + d, lt, own_rows, :]
                out[m, :, ls] = whole[TX + d, lt] / jnp.where(depth > 0.0, depth / WAVE_COURANT, 1.0) - sums[d, m, lt]
                nuv_out[d, :, ls] = nuv[d, lt]

    to_w.wait_send()
    to_e.wait_send()

    @pl.when(has_s)
    def _():
        to_s.wait_send()
        to_se.wait_send()
        to_s_later.wait_send()

    @pl.when(has_n)
    def _():
        to_n.wait_send()
        to_nw.wait_send()
        to_n_later.wait_send()

    for copy in sent:
        copy.wait_send()
    swap.wait_send()


def final_kernel(level_count, sol_u, sol_v, sol_t, sol_s, qu, qv, nuv, wet, eta_in, tx_in, ty_in,
                 eta_out, tx_out, ty_out, u_out, v_out, t_out, s_out, cubes, cube_sem, plane_sem):
    ratio = sweep_constants(level_count, DIFF_NUMBER)[1]
    strips = M * len(STRIPS)
    passed = [pltpu.make_async_copy(src, dst, plane_sem.at[n])
              for n, (src, dst) in enumerate(((eta_in, eta_out), (tx_in, tx_out), (ty_in, ty_out)))]
    for copy in passed:
        copy.start()

    def writes(s):
        m = s // 3
        rs = pl.ds(pl.multiple_of(SUB * (s - 3 * m), SUB), SUB)
        return m, rs, [pltpu.make_async_copy(cubes.at[f, s], dst.at[:, m, rs, :], cube_sem.at[f, s])
                       for f, dst in enumerate((t_out, s_out, u_out, v_out))]

    def strip(s, carry):
        m, rs, done = writes(s)
        for f, src in enumerate((sol_t, sol_s, sol_u, sol_v)):
            for lt in PAIR:
                ls = pl.ds(LANES * lt, LANES)
                if f < M:
                    n_wet = wet[rs, ls]
                    x = jnp.zeros(TILE, F32)
                    for k in reversed(range(level_count)):
                        e = src[k, m, lt, rs, :]
                        x = e + ratio[k] * jnp.where(n_wet > k + 1, x, e * (1.0 / (1.0 - ratio[k])))
                        cubes[f, s, k, :, ls] = jnp.where(n_wet > k, x, 0.0)
                else:
                    n, mean = nuv[f - M, rs, ls], (qu, qv)[f - M][m, rs, ls]
                    for k in range(level_count):
                        cubes[f, s, k, :, ls] = jnp.where(n > float(k), src[k, m, lt, rs, :] + mean, 0.0)
            done[f].start()
        return carry

    def finish(s, carry):
        for copy in writes(s)[-1]:
            copy.wait()
        return carry

    lax.fori_loop(0, strips, strip, 0)
    lax.fori_loop(0, strips, finish, 0)
    for copy in passed:
        copy.wait()


def solution(mesh):
    col_count = mesh.shape["col"]

    def local_step(vel_x, vel_y, pot_temp, salinity, surf_eta, trans_x, trans_y, col_depth, wet_levels, avg_weights):
        L = vel_x.shape[0]
        N = avg_weights.shape[0]
        hbm_spec = pl.BlockSpec(memory_space=pltpu.HBM)
        vmem_spec = pl.BlockSpec(memory_space=pltpu.VMEM)
        cube = jax.ShapeDtypeStruct(vel_x.shape, F32)
        flat = jax.ShapeDtypeStruct(surf_eta.shape, F32)
        vm = lambda *shape: pltpu.VMEM(shape, F32)
        dma = lambda n: pltpu.SemaphoreType.DMA((n,))
        stage = pl.pallas_call(
            functools.partial(stage_kernel, N),
            out_shape=jax.ShapeDtypeStruct((M, ROOM, M, ROWS, LANES), F32),
            in_specs=[vmem_spec] * 5 + [pl.BlockSpec(memory_space=pltpu.SMEM)],
            out_specs=hbm_spec,
            scratch_shapes=[vm(M, STAGED, M, ROWS, LANES), pltpu.SemaphoreType.DMA],
            name="ocean_stage",
        )(surf_eta, trans_x, trans_y, col_depth, wet_levels, avg_weights)
        *sol, qu, qv, nuv, eta_o, tx_o, ty_o = pl.pallas_call(
            functools.partial(step_kernel, col_count, L, N),
            out_shape=[jax.ShapeDtypeStruct((L, M, M, ROWS, LANES), F32)] * 4 + [flat] * 6,
            in_specs=[hbm_spec] * 5,
            out_specs=[vmem_spec] * 10,
            scratch_shapes=[
                vm(4, L, M, RING, XR, LANES), vm(M, STAGED, M, ROWS, LANES), *[vm(4, M, 8, LANES)] * 4, vm(5, M, M * L + 8, LANES), vm(4, M, M * L, LANES), vm(5, M, M * L + 8, LANES), vm(4, M, M * L, LANES),
                *[vm(M, 8, LANES)] * 2, vm(M, ROWS + 8, LANES), vm(M, M, ROWS, LANES), vm(M, M, M, ROWS, LANES),
                *[vm(4, ROWS, LANES)] * M,
                vm(M, M, M, ROWS, LANES), *[vm(M, ROWS, LANES)] * M, *[vm(4, ROWS, LANES)] * M,
                vm(6, RING, FRAME, LANES), vm(RING, RING, FRAME, LANES), vm(RING, M, M * ROWS, LANES), *[vm(RING, M, ROWS, LANES)] * M,
                pltpu.SMEM((4, L), F32), dma(8), pltpu.SemaphoreType.DMA, dma(31), dma(8), *[dma(4)] * 6, pltpu.SemaphoreType.DMA],
            compiler_params=pltpu.CompilerParams(collective_id=0, has_side_effects=True, vmem_limit_bytes=STEP_VMEM),
            name="ocean_step",
        )(vel_x, vel_y, pot_temp, salinity, stage)
        outs = pl.pallas_call(
            functools.partial(final_kernel, L),
            out_shape=[flat] * 3 + [cube] * 4,
            in_specs=[vmem_spec] * 11,
            out_specs=[hbm_spec] * 7,
            scratch_shapes=[vm(4, M * len(STRIPS), L, SUB, 256), pltpu.SemaphoreType.DMA((4, M * len(STRIPS))), dma(3)],
            name="ocean_final",
            compiler_params=pltpu.CompilerParams(vmem_limit_bytes=FINAL_VMEM),
        )(*sol, qu, qv, nuv, wet_levels, eta_o, tx_o, ty_o)
        return tuple(outs)

    spec_3d = P(None, None, "row", "col")
    spec_2d = P(None, "row", "col")
    spec_map = P("row", "col")
    return jax.shard_map(local_step, mesh=mesh, in_specs=(spec_3d,) * 4 + (spec_2d,) * 3 + (spec_map,) * 2 + (P(),),
                         out_specs=(spec_2d,) * 3 + (spec_3d,) * 4, check_vma=False)
```
